32 devices in a mesh: section: 2 (over core), ctx: 8 (over z, x), dp: 2 (over y).
Axes of the slice: x: 2, y: 2, z: 4, core: 2. Of those that a mesh axis runs over, the one named last changes fastest.
Arguments:
- hidden: bfloat16 [4, 2048, 5376], P(('section', 'dp'), 'ctx'), may hold values from -6 to 6
- frozen_query_rows: bfloat16 [4, 2048, 2048], P(('section', 'dp'), 'ctx'), may hold values from -12 to 12
- frozen_key_rows: bfloat16 [4, 2048, 1024], P(('section', 'dp'), 'ctx'), may hold values from -12 to 12
- frozen_value_rows: bfloat16 [4, 2048, 1024], P(('section', 'dp'), 'ctx'), may hold values from -6 to 6
- next_output_gradient: bfloat16 [4, 2048, 2048], P(('section', 'dp'), 'ctx'), may hold values from -0.011962891 to 0.011962891
- document_lengths: int32 [4, 16], P(('section', 'dp')), may hold values from 1 to 512, 2048 in all within a row
- document_adapter: int32 [4, 16], P(('section', 'dp')), may hold values from 0 to 3
- adapter_down_maps: bfloat16 [5376, 2, 4, 16], replicated, may hold values from -0.078125 to 0.078125
- adapter_up_maps: bfloat16 [2, 4, 16, 1024], replicated, may hold values from -1.5 to 1.5
Outputs:
- handed_on: bfloat16 [4, 2048, 2048], P(('section', 'dp'), 'ctx')
- down_map_gradient: float32 [5376, 2, 4, 16], replicated
- up_map_gradient: float32 [2, 4, 16, 1024], replicated
The draws below stay inside these ranges and needn't reach their ends.
Inputs may be any that keep to these rules, and one draw needn't show every extreme that they name: `document_lengths`: each sequence's 16 lengths sum to 2048, and the longest is exactly 512.
All inputs are finite; a program needn't handle non-finite values.
Results may differ from the reference program's by a relative error of at most 0.016.
Values may be sent and summed in bfloat16 or wider, within the bound.
No kernel may reach another device: no remote copies, remote signals or barrier semaphores. Data moves between devices by JAX's collectives and lax.ppermute only.
A program may use at most 128 MiB of HBM per device.

```python
import math
import jax
import jax.numpy as jnp
import numpy as np
from jax import lax

MODEL_WIDTH = 5376
HD = 128
HEADS = 16
KV_HEADS = 8
WINDOW = 1024
ADAPTER_RANK = 16
ADAPTER_COUNT = 4
DOCS = 16
TOK_DEV = 256
QW = 2048
KEY_VALUE_WIDTH = 1024
SEQ = 2048
SEQS = 4
N_SECTION = 2
N_DP = 2


def draw_projection(key, salt, head_count):
    array_shape = (SEQS, SEQ, head_count * HD)
    noise_key = jax.random.fold_in(key, salt)
    return jnp.clip(jax.random.normal(noise_key, array_shape, jnp.float32), -4.0, 4.0).astype(jnp.bfloat16)


def draw_frozen_query_rows(key, part):
    return draw_projection(key, 1, HEADS)


def draw_frozen_key_rows(key, part):
    return draw_projection(key, 2, KV_HEADS)


def place_ends(drawn, own_key, least, largest):
    index_at = [jax.random.randint(jax.random.fold_in(own_key, axis), (), 0, length) for axis, length in enumerate(drawn.shape)]
    widest = drawn.shape.index(max(drawn.shape))
    neighbour = index_at[:widest] + [(index_at[widest] + 1) % drawn.shape[widest]] + index_at[widest + 1:]
    return drawn.at[tuple(index_at)].set(least).at[tuple(neighbour)].set(largest)


def block_scale(rng, extent, cuts, low, high):
    def one(dim, blocks):
        draws = jax.random.uniform(jax.random.fold_in(jax.random.fold_in(rng, 6), dim), (blocks,), jnp.float32, low / len(cuts), high / len(cuts))
        return jnp.repeat(jnp.exp(draws), extent[dim] // blocks).reshape((-1,) + (1,) * (len(extent) - dim - 1))

    level = one(*cuts[0])
    for cut in cuts[1:]:
        level = level * one(*cut)
    return level


def length_profile(count, total, bound, slope):
    weights = [(1 << 20) // math.isqrt(standing ** slope) + 1 for standing in range(2, count + 1)]
    rest, counts = total - bound - (count - 1), [1] * (count - 1)
    while rest > 0:
        movable = [i for i in range(count - 1) if counts[i] < bound]
        mass, remaining = sum([weights[i] for i in movable]), rest
        for i in movable:
            more = min(bound - counts[i], max(1, remaining * weights[i] // mass), rest)
            counts[i] = counts[i] + more
            rest = rest - more
    return np.array([bound] + counts)


def ragged_sizes(own_key, amount, total, limit, skew):
    if amount == 2:
        one = jax.random.randint(own_key, (), max(1, total - limit), min(limit, total - 1) + 1)
        return jnp.stack([one, total - one])
    sizes = jnp.asarray(length_profile(amount, total, limit, skew), jnp.int32)
    twos = (amount - 1) // 2
    giver, taker = sizes[1:1 + 2 * twos:2], sizes[2:2 + 2 * twos:2]
    margin = jnp.minimum(giver - 1, limit - taker)
    moved = jax.random.randint(jax.random.fold_in(own_key, 1), (twos,), 0, 1 << 20) % (margin + 1)
    sizes = sizes.at[1:1 + 2 * twos:2].set(giver - moved).at[2:2 + 2 * twos:2].set(taker + moved)
    return sizes[jax.random.permutation(jax.random.fold_in(own_key, 2), amount)]


def noise(own_key, dims, scale, limit, pieces=(), kind=jnp.bfloat16):
    values = jax.random.normal(own_key, dims, jnp.float32) * scale
    if len(pieces) > 0:
        values = block_scale(own_key, dims, pieces, -0.22, 0.18) * values
    return jnp.clip(values, min=-limit, max=limit).astype(kind)


def setup_inputs(seed: int = 0) -> dict:
    arg_keys = jax.random.split(jax.random.key(seed), 10)
    return {
        "hidden": noise(arg_keys[0], (SEQS, SEQ, MODEL_WIDTH), 1.0, 6.0, ((0, 4), (1, 8))),
        "frozen_query_rows": draw_frozen_query_rows(jax.random.fold_in(arg_keys[9], 71), 0),
        "frozen_key_rows": draw_frozen_key_rows(jax.random.fold_in(arg_keys[9], 71), 0),
        "frozen_value_rows": noise(arg_keys[3], (SEQS, SEQ, KEY_VALUE_WIDTH), 1.0, 6.0, ((0, 4), (1, 8))),
        "next_output_gradient": noise(arg_keys[4], (SEQS, SEQ, QW), 0.002, 0.011962891, ((0, 4), (1, 8))),
        "document_lengths": jax.vmap(lambda own: ragged_sizes(own, DOCS, SEQ, SEQ // 4, 2))(jax.random.split(arg_keys[5], SEQS)).reshape((SEQS, DOCS)).astype(jnp.int32),
        "document_adapter": place_ends(jax.random.randint(arg_keys[6], (SEQS, DOCS), 0, ADAPTER_COUNT), jax.random.fold_in(arg_keys[6], 1), 0, ADAPTER_COUNT - 1).astype(jnp.int32),
        "adapter_down_maps": noise(arg_keys[7], (MODEL_WIDTH, 2, ADAPTER_COUNT, ADAPTER_RANK), MODEL_WIDTH ** -0.5, 0.078125),
        "adapter_up_maps": noise(arg_keys[8], (2, ADAPTER_COUNT, ADAPTER_RANK, KEY_VALUE_WIDTH), ADAPTER_RANK ** -0.5, 1.5),
    }


query_scale = 168.0 ** -0.5
adapter_scale = 0.5
rope_base = 10000.0
masked_score = -1.0e30


def rotate(vectors, positions, direction):
    head_dim = vectors.shape[-1]
    half_dim = head_dim // 2
    frequency = rope_base ** (-(jnp.arange(half_dim, dtype=jnp.float32) * 2.0) / head_dim)
    angles = positions[:, None] * frequency[None, :]
    cos_part = jnp.cos(angles)[:, None, :]
    sine_part = direction * jnp.sin(angles)[:, None, :]
    front_half = vectors[..., :half_dim]
    back_half = vectors[..., half_dim:]
    return jnp.concatenate([front_half * cos_part - back_half * sine_part, back_half * cos_part + front_half * sine_part], axis=-1)


def doc_index(sequence_lengths, positions):
    doc_ends = jnp.cumsum(sequence_lengths)
    return jnp.sum((doc_ends[None, :] <= positions[:, None]).astype(jnp.int32), axis=1)


def tenant_rows(sequence_lengths, adapter_bank, positions):
    doc_ids = doc_index(sequence_lengths, positions)
    picked = (doc_ids[:, None] == jnp.arange(sequence_lengths.shape[0], dtype=jnp.int32)[None, :]).astype(jnp.int32)
    return doc_ids, jnp.sum(picked * adapter_bank[None, :], axis=1)


def adapter_token_rows(hidden, frozen_key_rows, frozen_value_rows, adapter_down_maps, adapter_up_maps, adapter_choice):
    token_row_count = hidden.shape[0]
    adapter_choices = adapter_up_maps.shape[1]
    adapter_rank_size = adapter_up_maps.shape[2]
    key_value_width = adapter_up_maps.shape[3]
    adapter_onehot_mask = (adapter_choice[:, None] == jnp.arange(adapter_choices, dtype=jnp.int32)[None, :]).astype(jnp.float32)
    low_rank_rows = jnp.dot(hidden, adapter_down_maps.reshape(adapter_down_maps.shape[0], 2 * adapter_choices * adapter_rank_size), preferred_element_type=jnp.float32)
    low_rank_rows = low_rank_rows.reshape(token_row_count, 2, adapter_choices, adapter_rank_size)
    low_rank = jnp.sum(low_rank_rows * adapter_onehot_mask[:, None, :, None], axis=2).astype(jnp.bfloat16)
    adapter_spread = low_rank[:, :, None, :] * adapter_onehot_mask[:, None, :, None].astype(jnp.bfloat16)
    key_adapter_shift = jnp.dot(adapter_spread[:, 0].reshape(token_row_count, adapter_choices * adapter_rank_size), adapter_up_maps[0].reshape(adapter_choices * adapter_rank_size, key_value_width), preferred_element_type=jnp.float32)
    value_adapter_shift = jnp.dot(adapter_spread[:, 1].reshape(token_row_count, adapter_choices * adapter_rank_size), adapter_up_maps[1].reshape(adapter_choices * adapter_rank_size, key_value_width), preferred_element_type=jnp.float32)
    key_before_rotary = frozen_key_rows.astype(jnp.float32) + adapter_scale * key_adapter_shift
    value_token_rows = (frozen_value_rows.astype(jnp.float32) + adapter_scale * value_adapter_shift).astype(jnp.bfloat16)
    return adapter_onehot_mask, adapter_spread, key_before_rotary, value_token_rows


def adapter_gradients(hidden, adapter_spread, adapter_onehot_mask, key_gradient, value_gradient, adapter_up_maps):
    token_row_count = hidden.shape[0]
    adapter_choices = adapter_up_maps.shape[1]
    adapter_rank_size = adapter_up_maps.shape[2]
    key_value_width = adapter_up_maps.shape[3]
    up_gradient_parts = []
    down_parts = []
    for adapter_selector, adapter_field_gradient in ((0, key_gradient), (1, value_gradient)):
        flat_adapter_spread = adapter_spread[:, adapter_selector].reshape(token_row_count, adapter_choices * adapter_rank_size)
        up_gradient_parts.append(adapter_scale * jnp.dot(flat_adapter_spread.T, adapter_field_gradient, preferred_element_type=jnp.float32))
        low_rank_gradient = adapter_scale * jnp.dot(adapter_field_gradient, adapter_up_maps[adapter_selector].reshape(adapter_choices * adapter_rank_size, key_value_width).T, preferred_element_type=jnp.float32)
        down_parts.append((low_rank_gradient.reshape(token_row_count, adapter_choices, adapter_rank_size) * adapter_onehot_mask[:, :, None]).astype(jnp.bfloat16))
    up_map_gradient = jnp.stack(up_gradient_parts).reshape(2, adapter_choices, adapter_rank_size, key_value_width)
    low_grads = jnp.stack(down_parts, axis=1).reshape(token_row_count, 2 * adapter_choices * adapter_rank_size)
    down_map_gradient = jnp.dot(hidden.T, low_grads, preferred_element_type=jnp.float32).reshape(hidden.shape[1], 2, adapter_choices, adapter_rank_size)
    return down_map_gradient, up_map_gradient


def sequence_forward_pass(hidden, frozen_query_rows, frozen_key_rows, frozen_value_rows, returned_values, sequence_lengths, adapter_bank, adapter_down_maps, adapter_up_maps):
    seq_len = hidden.shape[0]
    query_width = frozen_query_rows.shape[1]
    key_value_width = frozen_key_rows.shape[1]
    kv_heads = key_value_width // HD
    group_size = query_width // key_value_width
    span = WINDOW + TOK_DEV
    positions = jnp.arange(seq_len, dtype=jnp.int32)
    doc_ids, adapter_choice = tenant_rows(sequence_lengths, adapter_bank, positions)
    adapter_onehot_mask, adapter_spread, key_before_rotary, value_token_rows = adapter_token_rows(hidden, frozen_key_rows, frozen_value_rows, adapter_down_maps, adapter_up_maps, adapter_choice)
    pos_float = positions.astype(jnp.float32)
    key_rows = rotate(key_before_rotary.reshape(seq_len, kv_heads, HD), pos_float, 1.0).astype(jnp.bfloat16)
    query_rows = rotate(frozen_query_rows.astype(jnp.float32).reshape(seq_len, kv_heads * group_size, HD), pos_float, 1.0).astype(jnp.bfloat16)
    query_rows = query_rows.reshape(seq_len, kv_heads, group_size, HD)
    value_token_rows = value_token_rows.reshape(seq_len, kv_heads, HD)
    grad_rows = returned_values.reshape(seq_len, kv_heads, group_size, HD)
    key_pad = jnp.concatenate([jnp.zeros((WINDOW, kv_heads, HD), jnp.bfloat16), key_rows], axis=0)
    value_pad = jnp.concatenate([jnp.zeros((WINDOW, kv_heads, HD), jnp.bfloat16), value_token_rows], axis=0)
    padded_pos = jnp.arange(-WINDOW, seq_len, dtype=jnp.int32)
    padded_docs = jnp.concatenate([jnp.full((WINDOW,), -1, jnp.int32), doc_ids], axis=0)
    block_count = seq_len // TOK_DEV

    def block_scores(row_start):
        query_pos = row_start + jnp.arange(TOK_DEV, dtype=jnp.int32)
        query_docs = lax.dynamic_slice_in_dim(doc_ids, row_start, TOK_DEV, 0)
        key_pos = lax.dynamic_slice_in_dim(padded_pos, row_start, span, 0)
        key_docs = lax.dynamic_slice_in_dim(padded_docs, row_start, span, 0)
        key_gap = query_pos[:, None] - key_pos[None, :]
        allowed = (query_docs[:, None] == key_docs[None, :]) & (key_gap >= 0) & (key_gap < WINDOW)
        query_part = lax.dynamic_slice_in_dim(query_rows, row_start, TOK_DEV, 0)
        key_part = lax.dynamic_slice_in_dim(key_pad, row_start, span, 0)
        value_part = lax.dynamic_slice_in_dim(value_pad, row_start, span, 0)
        scores = jnp.einsum("tgrd,lgd->tgrl", query_part.astype(jnp.float32), key_part.astype(jnp.float32)) * query_scale
        scores = jnp.where(allowed[:, None, None, :], scores, masked_score)
        return scores, query_part, key_part, value_part

    def forward_block(block_index):
        row_start = (block_index * TOK_DEV).astype(jnp.int32)
        scores, query_part, key_part, value_part = block_scores(row_start)
        row_max = jnp.max(scores, axis=3, keepdims=True)
        shifted = jnp.exp(scores - row_max)
        row_total = jnp.sum(shifted, axis=3, keepdims=True)
        weights = (shifted / row_total).astype(jnp.bfloat16)
        output_rows = jnp.einsum("tgrl,lgd->tgrd", weights.astype(jnp.float32), value_part.astype(jnp.float32)).astype(jnp.bfloat16)
        return output_rows, (row_max + jnp.log(row_total))[..., 0]

    out_blocks, log_blocks = lax.map(forward_block, jnp.arange(block_count, dtype=jnp.int32))
    attention_output = out_blocks.reshape(seq_len, kv_heads, group_size, HD)

    def backward_block(accum, block_index):
        key_acc, value_acc = accum
        row_start = (block_index * TOK_DEV).astype(jnp.int32)
        scores, query_part, key_part, value_part = block_scores(row_start)
        log_total = log_blocks[block_index]
        weights = jnp.exp(scores - log_total[..., None])
        weights_low = weights.astype(jnp.bfloat16)
        out_part = lax.dynamic_slice_in_dim(attention_output, row_start, TOK_DEV, 0)
        grad_part = lax.dynamic_slice_in_dim(grad_rows, row_start, TOK_DEV, 0)
        drift_rows = jnp.sum(grad_part.astype(jnp.float32) * out_part.astype(jnp.float32), axis=3)
        grad_weights = jnp.einsum("tgrd,lgd->tgrl", grad_part.astype(jnp.float32), value_part.astype(jnp.float32))
        grad_scores = (weights * (grad_weights - drift_rows[..., None])).astype(jnp.bfloat16)
        value_step = jnp.einsum("tgrl,tgrd->lgd", weights_low.astype(jnp.float32), grad_part.astype(jnp.float32))
        key_step = jnp.einsum("tgrl,tgrd->lgd", grad_scores.astype(jnp.float32), query_part.astype(jnp.float32)) * query_scale
        key_acc = lax.dynamic_update_slice_in_dim(key_acc, lax.dynamic_slice_in_dim(key_acc, row_start, span, 0) + key_step, row_start, 0)
        value_acc = lax.dynamic_update_slice_in_dim(value_acc, lax.dynamic_slice_in_dim(value_acc, row_start, span, 0) + value_step, row_start, 0)
        return (key_acc, value_acc), None

    start_acc = jnp.zeros((WINDOW + seq_len, kv_heads, HD), jnp.float32)
    (key_acc, value_acc), unused = lax.scan(backward_block, (start_acc, start_acc), jnp.arange(block_count, dtype=jnp.int32))
    key_gradient = rotate(key_acc[WINDOW:], pos_float, -1.0).astype(jnp.bfloat16).reshape(seq_len, key_value_width)
    value_gradient = value_acc[WINDOW:].astype(jnp.bfloat16).reshape(seq_len, key_value_width)
    down_map_gradient, up_map_gradient = adapter_gradients(hidden, adapter_spread, adapter_onehot_mask, key_gradient, value_gradient, adapter_up_maps)
    return attention_output.reshape(seq_len, query_width), down_map_gradient, up_map_gradient


def reference(hidden, frozen_query_rows, frozen_key_rows, frozen_value_rows, next_output_gradient, document_lengths, document_adapter, adapter_down_maps, adapter_up_maps):
    returned_values = jnp.roll(next_output_gradient, -N_DP, axis=0)
    outputs = []
    down_gradient_total = jnp.zeros(adapter_down_maps.shape, jnp.float32)
    up_gradient_total = jnp.zeros(adapter_up_maps.shape, jnp.float32)
    for sequence_index in range(N_SECTION * N_DP):
        attention_output, down_map_gradient, up_map_gradient = sequence_forward_pass(hidden[sequence_index], frozen_query_rows[sequence_index], frozen_key_rows[sequence_index], frozen_value_rows[sequence_index], returned_values[sequence_index], document_lengths[sequence_index], document_adapter[sequence_index], adapter_down_maps, adapter_up_maps)
        outputs.append(attention_output)
        down_gradient_total = down_gradient_total + down_map_gradient
        up_gradient_total = up_gradient_total + up_map_gradient
    handed_on = jnp.roll(jnp.stack(outputs), N_DP, axis=0)
    return handed_on, down_gradient_total, up_gradient_total
```

```python
from functools import partial

import jax
import jax.numpy as jnp
from jax import lax
from jax.experimental import pallas as pl
from jax.experimental.pallas import tpu as pltpu
from jax.sharding import PartitionSpec as P

HD = 128
WINDOW = 1024
SUB = 8
SPLITS = 4

query_scale = 168.0 ** (-0.5)
adapter_scale = 0.5
rope_base = 10000.0
masked_score = -1e30
f32 = jnp.float32
bf16 = jnp.bfloat16


def permute_by(value, axis, steps):
    count = lax.axis_size(axis)
    first, last = max(0, -steps), min(count, count - steps)
    return lax.ppermute(value, axis, [(i, i + steps) for i in range(first, last)])


def permute_cyclic(value, axis, by):
    count = lax.axis_size(axis)
    return lax.ppermute(value, axis, [(i, (i + by) % count) for i in range(count)])


def permute_xor(value, axis, bit):
    count = lax.axis_size(axis)
    return lax.ppermute(value, axis, [(i, i ^ bit) for i in range(count)])


def window_blocks(own, steps):
    count = lax.axis_size("ctx")
    even_to_odd = [(i, i + 1) for i in range(0, count - 1, 2)]
    odd_to_even = [(i + 1, i) for i in range(0, count - 1, 2)]
    chain = [own]
    for _ in range(steps):
        chain.append(permute_by(chain[-1], "ctx", 2))
    blocks = []
    for i in range(steps):
        blocks.append(
            [
                lax.ppermute(chain[i], "ctx", even_to_odd),
                lax.ppermute(chain[i + 1], "ctx", odd_to_even),
            ]
        )
        blocks.append([chain[i + 1]])
    return blocks


def doc_index(sequence_lengths, positions):
    doc_ends = jnp.cumsum(sequence_lengths)
    return jnp.sum((doc_ends[None, :] <= positions[:, None]).astype(jnp.int32), axis=1)


def attention_kernel(*refs, counts, tok, group):
    n_in = sum(counts)
    k_refs, v_refs = refs[:n_in], refs[n_in : 2 * n_in]
    q_ref, g_ref, spread_ref, up_ref, bias_ref, cos_ref, sin_ref = refs[2 * n_in : 2 * n_in + 7]
    out_ref, lg_ref, u_ref = refs[2 * n_in + 7 :]
    up = up_ref[0]
    spread = spread_ref[...]
    shift = adapter_scale * jnp.dot(spread, up, preferred_element_type=f32)

    def stacked(block_refs):
        rows, at = [], 0
        for n in counts:
            block = block_refs[at][...].astype(f32)
            for extra in block_refs[at + 1 : at + n]:
                block = block + extra[...].astype(f32)
            rows.append(block)
            at += n
        return jnp.concatenate(rows, axis=0)

    cos, sin = cos_ref[...], sin_ref[...]
    key = stacked(k_refs) + shift[:, :HD]
    key = (key * cos + pltpu.roll(key, HD // 2, 1) * sin).astype(bf16)
    val = (stacked(v_refs) + shift[:, HD:]).astype(bf16)
    cos_q, sin_q = cos[:tok], sin[:tok]
    queries, grads = [], []
    for h in range(group):
        q = q_ref[:, h * HD : (h + 1) * HD].astype(f32)
        queries.append((q * cos_q + pltpu.roll(q, HD // 2, 1) * sin_q).astype(bf16))
        grads.append(g_ref[:, h * HD : (h + 1) * HD])
    q = jnp.concatenate(queries, axis=0)
    g = jnp.concatenate(grads, axis=0)
    dot = partial(lax.dot_general, preferred_element_type=f32)
    last, first = (((1,), (1,)), ((), ())), (((0,), (0,)), ((), ()))
    bias = jnp.concatenate([bias_ref[...]] * group, axis=1)
    scores = dot(key, q, last) * query_scale + bias
    top = jnp.max(scores, axis=0, keepdims=True)
    probs = jnp.exp(scores - top)
    total = jnp.sum(probs, axis=0, keepdims=True)
    probs = probs * (1.0 / total)
    low_probs = probs.astype(bf16)
    out_t = dot(val, low_probs, first)
    out = out_t.T.astype(bf16)
    for h in range(group):
        out_ref[:, h * HD : (h + 1) * HD] = out[h * tok : (h + 1) * tok]
    drift = jnp.sum(out_t.astype(bf16).astype(f32) * g.astype(f32).T, axis=0, keepdims=True)
    dprob = dot(val, g, last)
    dscore = (probs * (dprob - drift)).astype(bf16)
    dkey = query_scale * jnp.dot(dscore, q, preferred_element_type=f32)
    dval = jnp.dot(low_probs, g, preferred_element_type=f32)
    dkey = dkey * cos - pltpu.roll(dkey, HD // 2, 1) * sin
    both = jnp.concatenate([dkey.astype(bf16), dval.astype(bf16)], axis=1)
    lg = dot(both, up, last)

    @pl.when(pl.program_id(0) == 0)
    def _():
        lg_ref[...] = lg

    @pl.when(pl.program_id(0) != 0)
    def _():
        lg_ref[...] += lg

    u = adapter_scale * dot(spread, both, first)
    half = spread.shape[1] // 2
    u_ref[0] = u[:half, :HD].astype(bf16)
    u_ref[1] = u[half:, HD:].astype(bf16)


def attention(blocks, start, q_rows, g_rows, spread, up_cat, bias, cos, sin):
    tok = q_rows.shape[0]
    heads = blocks[0][0].shape[1] // (2 * HD)
    kv_heads, width, _ = up_cat.shape
    group = q_rows.shape[1] // (kv_heads * HD)
    counts = tuple(len(b) for b in blocks)
    flat = [a for b in blocks for a in b]
    span = spread.shape[0]
    half = width // 2
    whole = lambda shape: pl.BlockSpec(shape, lambda h: (0,) * len(shape))
    in_specs = (
        [pl.BlockSpec((tok, HD), lambda h: (0, h))] * len(flat)
        + [pl.BlockSpec((tok, HD), lambda h: (0, h + heads))] * len(flat)
        + [pl.BlockSpec((tok, group * HD), lambda h: (0, h + start))] * 2
        + [
            whole((span, width)),
            pl.BlockSpec((1, width, 2 * HD), lambda h: (h + start, 0, 0)),
            whole((span, tok)),
            whole((span, HD)),
            whole((span, HD)),
        ]
    )
    return pl.pallas_call(
        partial(attention_kernel, counts=counts, tok=tok, group=group),
        grid=(heads,),
        in_specs=in_specs,
        out_specs=[
            pl.BlockSpec((tok, group * HD), lambda h: (0, h)),
            whole((span, width)),
            pl.BlockSpec((2, half, HD), lambda h: (0, 0, h)),
        ],
        out_shape=[
            jax.ShapeDtypeStruct((tok, heads * group * HD), bf16),
            jax.ShapeDtypeStruct((span, width), f32),
            jax.ShapeDtypeStruct((2, half, heads * HD), bf16),
        ],
        compiler_params=pltpu.CompilerParams(dimension_semantics=("arbitrary",)),
        name="attention",
    )(*flat, *flat, q_rows, g_rows, spread, up_cat, bias, cos, sin)


def product_kernel(*refs, n_recv, n_up, cols, up_cols):
    side_ref, lg_ref = refs[:2]
    recv = refs[2 : 2 + n_recv]
    mask_ref, hidden_ref = refs[2 + n_recv : 4 + n_recv]
    ups = refs[4 + n_recv : 4 + n_recv + n_up]
    keep_ref, send_ref = refs[4 + n_recv + n_up :]
    side = side_ref[0]
    total = lg_ref[...]
    for r in recv:
        total = total + r[...].astype(f32)
    total = total * mask_ref[...]
    width = total.shape[1]
    half = width // 2
    total = jnp.where(side == 0, total, pltpu.roll(total, half, 1)).astype(bf16)
    per_row = cols + up_cols
    rows = half // SUB
    step = 2 if cols % 2 == 0 else 1
    for c in range(0, cols, step):
        w = lax.dot_general(
            total,
            hidden_ref[:, c * HD : (c + step) * HD],
            (((0,), (0,)), ((), ())),
            preferred_element_type=f32,
        ).astype(bf16)
        for j in range(step):
            for r in range(rows):
                tile = w[:, j * HD : (j + 1) * HD]
                keep_ref[r * per_row + c + j] = tile[r * SUB : (r + 1) * SUB]
                send_ref[r * per_row + c + j] = tile[half + r * SUB : half + (r + 1) * SUB]
    at = cols
    for up in ups:
        for h in range(up.shape[2] // HD):
            for r in range(rows):
                where = (slice(r * SUB, (r + 1) * SUB), slice(h * HD, (h + 1) * HD))
                keep_ref[r * per_row + at] = up[(side,) + where]
                send_ref[r * per_row + at] = up[(1 - side,) + where]
            at += 1
    used = rows * per_row
    if keep_ref.shape[0] > used:
        rest = keep_ref.shape[0] - used
        keep_ref[pl.ds(used, rest)] = jnp.zeros((rest, SUB, HD), bf16)
        send_ref[pl.ds(used, rest)] = jnp.zeros((rest, SUB, HD), bf16)


def assemble_kernel(scalars_ref, ma_ref, mb_ref, ra_ref, rb_ref, w_ref, u_ref, *, cols, rows):
    side, me_a, me_b = scalars_ref[0], scalars_ref[1], scalars_ref[2]
    n_a, a = ma_ref.shape[:2]
    b = mb_ref.shape[1]
    up_cols = u_ref.shape[1] // HD
    per_row = cols + up_cols
    for r in range(rows):
        for c in range(per_row):
            t = r * per_row + c
            if t < n_a * a:
                mine, theirs, piece, off = ma_ref, ra_ref, (t // a) ^ me_a, t % a
            else:
                t -= n_a * a
                mine, theirs, piece, off = mb_ref, rb_ref, (t // b) ^ me_b, t % b
            for src, m in ((mine, side), (theirs, 1 - side)):
                at = pl.multiple_of((m * rows + r) * SUB, SUB)
                tile = src[piece, off].astype(f32)
                if c < cols:
                    w_ref[pl.ds(at, SUB), c * HD : (c + 1) * HD] = tile
                else:
                    u_ref[pl.ds(at, SUB), (c - cols) * HD : (c - cols + 1) * HD] = tile


def axis_bits(axis):
    bits, bit = [], 1
    while bit < lax.axis_size(axis):
        bits.append((axis, bit))
        bit *= 2
    return bits


def bit_of(stage):
    axis, bit = stage
    return ((lax.axis_index(axis) & bit) != 0).astype(jnp.int32)


def scatter_stage(tiles, stage):
    n = tiles.shape[0] // 2
    bit = bit_of(stage)
    send = lax.dynamic_slice_in_dim(tiles, (1 - bit) * n, n, 0)
    keep = lax.dynamic_slice_in_dim(tiles, bit * n, n, 0)
    recv = permute_xor(send, *stage)
    return (keep.astype(f32) + recv.astype(f32)).astype(bf16)


def gather_stage(tiles, stage):
    return jnp.concatenate([tiles, permute_xor(tiles, *stage)], axis=0)


def body(
    hidden,
    frozen_query_rows,
    frozen_key_rows,
    frozen_value_rows,
    next_output_gradient,
    document_lengths,
    document_adapter,
    adapter_down_maps,
    adapter_up_maps,
):
    tok, model_width = hidden.shape[1:]
    kv_width = frozen_key_rows.shape[2]
    kv_heads = kv_width // HD
    _, adapters, rank, _ = adapter_up_maps.shape
    width = 2 * adapters * rank
    half = width // 2
    ctx_index, ctx_size = lax.axis_index("ctx"), lax.axis_size("ctx")
    longest = tok * ctx_size // 4
    reach = min(-(-(min(WINDOW, longest) - 1) // tok), ctx_size - 1)
    steps = (reach + 1) // 2

    splits = SPLITS if kv_heads % SPLITS == 0 else 1
    per = kv_heads // splits
    keys, vals = frozen_key_rows[0], frozen_value_rows[0]
    parts = []
    for i in range(splits):
        cut = slice(i * per * HD, (i + 1) * per * HD)
        own = jnp.concatenate([keys[:, cut], vals[:, cut]], axis=1)
        parts.append([[own]] + window_blocks(own, steps))
    returned = permute_cyclic(next_output_gradient, "section", -1)

    block_starts = jnp.stack([(ctx_index - d) * tok for d in range(2 * steps + 1)])
    key_pos = (block_starts[:, None] + jnp.arange(tok, dtype=jnp.int32)[None, :]).reshape(-1)
    key_docs = doc_index(document_lengths[0], key_pos)
    positions, docs = key_pos[:tok], key_docs[:tok]
    picked = docs[:, None] == jnp.arange(document_lengths.shape[1], dtype=jnp.int32)[None, :]
    tenant = jnp.sum(picked.astype(jnp.int32) * document_adapter[0][None, :], axis=1)
    lane_adapter = (jnp.arange(width, dtype=jnp.int32) // rank) % adapters
    mask = (tenant[:, None] == lane_adapter[None, :]).astype(f32)
    gap = positions[None, :] - key_pos[:, None]
    allowed = (
        (key_docs[:, None] == docs[None, :])
        & (gap >= 0)
        & (gap < WINDOW)
        & (key_pos >= 0)[:, None]
    )
    bias = jnp.where(allowed, 0.0, masked_score).astype(f32)
    frequency = rope_base ** (-(jnp.arange(HD // 2, dtype=f32) * 2.0) / HD)
    angles = key_pos.astype(f32)[:, None] * frequency[None, :]
    cos_half, sin_half = jnp.cos(angles), jnp.sin(angles)
    cos = jnp.concatenate([cos_half, cos_half], axis=1)
    sin = jnp.concatenate([-sin_half, sin_half], axis=1)

    low = jnp.dot(
        hidden[0], adapter_down_maps.reshape(model_width, width), preferred_element_type=f32
    )
    spread_own = (low * mask).astype(bf16)
    spread = jnp.concatenate(
        [spread_own]
        + [sum(b[1:], b[0]) for b in window_blocks(spread_own, steps)],
        axis=0,
    )
    up_flat = adapter_up_maps.reshape(2, half, kv_heads, HD)
    zero = jnp.zeros((kv_heads, half, HD), bf16)
    up_heads = jnp.moveaxis(up_flat, 2, 1)
    up_cat = jnp.concatenate(
        [
            jnp.concatenate([up_heads[0], zero], axis=2),
            jnp.concatenate([zero, up_heads[1]], axis=2),
        ],
        axis=1,
    )

    outs, lgs, ups = [], [], []
    for i in range(splits):
        out, lg, u = attention(
            parts[i],
            i * per,
            frozen_query_rows[0],
            returned[0],
            spread,
            up_cat,
            bias,
            cos,
            sin,
        )
        outs.append(permute_cyclic(out, "section", 1))
        lgs.append(lg)
        ups.append(u)
    handed = jnp.concatenate(outs, axis=1)[None]

    lg = sum(lgs[1:], lgs[0]).reshape(2 * steps + 1, tok, width)
    received = [permute_by(lg[d].astype(bf16), "ctx", -d) for d in range(1, 2 * steps + 1)]

    other = (
        axis_bits("ctx")[:1] + axis_bits("dp"),
        axis_bits("dp") + axis_bits("ctx")[:1],
    )
    tail = axis_bits("ctx")[1:]
    group = lax.axis_size("ctx") * lax.axis_size("dp")
    cols, up_cols, rows = model_width // HD, kv_heads, half // SUB
    units = -(-(rows * (cols + up_cols)) // group)
    a = (units + 1) // 2
    b = units - a
    side = lax.axis_index("section").astype(jnp.int32)
    smem = pl.BlockSpec(memory_space=pltpu.SMEM)
    vmem = pl.BlockSpec(memory_space=pltpu.VMEM)
    keep, send = pl.pallas_call(
        partial(
            product_kernel, n_recv=len(received), n_up=len(ups), cols=cols, up_cols=up_cols
        ),
        in_specs=[smem] + [vmem] * (3 + len(received) + len(ups)),
        out_specs=[vmem, vmem],
        out_shape=[jax.ShapeDtypeStruct((units * group, SUB, HD), bf16)] * 2,
        name="product",
    )(side[None], lg[0], *received, adapter_scale * mask, hidden[0], *ups)
    recv = permute_cyclic(send, "section", 1)
    tiles = (keep.astype(f32) + recv.astype(f32)).astype(bf16)
    colours = [tiles[: a * group], tiles[a * group :]]
    ids = []
    stages = [list(other[c]) + list(tail) for c in range(2)]
    for k in range(len(stages[0])):
        colours = [scatter_stage(colours[c], stages[c][k]) for c in range(2)]
    for c in range(2):
        me = jnp.int32(0)
        for stage in stages[c]:
            me = me * 2 + bit_of(stage)
        ids.append(me)
    for k in reversed(range(len(stages[0]))):
        colours = [gather_stage(colours[c], stages[c][k]) for c in range(2)]
    theirs = [permute_cyclic(t, "section", 1) for t in colours]
    shapes = [(group, a, SUB, HD), (group, b, SUB, HD)]
    w, u = pl.pallas_call(
        partial(assemble_kernel, cols=cols, rows=rows),
        in_specs=[smem] + [vmem] * 4,
        out_specs=[vmem, vmem],
        out_shape=[
            jax.ShapeDtypeStruct((width, model_width), f32),
            jax.ShapeDtypeStruct((width, kv_width), f32),
        ],
        name="assemble",
    )(
        jnp.stack([side, ids[0], ids[1]]),
        colours[0].reshape(shapes[0]),
        colours[1].reshape(shapes[1]),
        theirs[0].reshape(shapes[0]),
        theirs[1].reshape(shapes[1]),
    )
    down_map_gradient = w.T.reshape(model_width, 2, adapters, rank)
    up_map_gradient = u.reshape(2, adapters, rank, kv_width)
    return (handed, down_map_gradient, up_map_gradient)


def solution(mesh):
    return jax.shard_map(
        body,
        mesh=mesh,
        in_specs=(
            P(("section", "dp"), "ctx", None),
            P(("section", "dp"), "ctx", None),
            P(("section", "dp"), "ctx", None),
            P(("section", "dp"), "ctx", None),
            P(("section", "dp"), "ctx", None),
            P(("section", "dp"), None),
            P(("section", "dp"), None),
            P(),
            P(),
        ),
        out_specs=(P(("section", "dp"), "ctx", None), P(), P()),
        check_vma=False,
    )
```

```python
from functools import partial

import jax
import jax.numpy as jnp
from jax import lax
from jax.experimental import pallas as pl
from jax.experimental.pallas import tpu as pltpu
from jax.sharding import PartitionSpec as P

HD = 128
WINDOW = 1024
SUB = 8
PIECES = (2, 3, 3)

query_scale = 168.0 ** (-0.5)
adapter_scale = 0.5
rope_base = 10000.0
masked_score = -1e30
f32 = jnp.float32
bf16 = jnp.bfloat16


def permute_by(value, axis, steps):
    count = lax.axis_size(axis)
    first, last = max(0, -steps), min(count, count - steps)
    return lax.ppermute(value, axis, [(i, i + steps) for i in range(first, last)])


def permute_cyclic(value, axis, by):
    count = lax.axis_size(axis)
    return lax.ppermute(value, axis, [(i, (i + by) % count) for i in range(count)])


def permute_xor(value, axis, bit):
    count = lax.axis_size(axis)
    return lax.ppermute(value, axis, [(i, i ^ bit) for i in range(count)])


def window_blocks(own, steps):
    even = lax.axis_index("ctx") % 2 == 0
    chain = [own]
    for _ in range(steps):
        chain.append(permute_by(chain[-1], "ctx", 2))
    blocks = []
    for i in range(steps):
        payload = jnp.where(even, chain[i], chain[i + 1])
        blocks.append(permute_xor(payload, "ctx", 1))
        blocks.append(chain[i + 1])
    return blocks


def doc_index(sequence_lengths, positions):
    doc_ends = jnp.cumsum(sequence_lengths)
    return jnp.sum((doc_ends[None, :] <= positions[:, None]).astype(jnp.int32), axis=1)


def attention_kernel(*refs, n_blocks, tok, group, sub, chained):
    k_refs, v_refs = refs[:n_blocks], refs[n_blocks : 2 * n_blocks]
    at = 2 * n_blocks
    q_ref, g_ref, spread_ref, up_ref, bias_ref, cos_ref, sin_ref = refs[at : at + 7]
    at += 7
    if chained:
        lg_in_ref = refs[at]
        at += 3
    out_ref, u_ref, lg_ref = refs[at : at + 3]
    lg_low_refs = refs[at + 3 :]
    step = pl.program_id(0)
    up = up_ref[0]
    spread = spread_ref[...]
    shift = adapter_scale * jnp.dot(spread, up, preferred_element_type=f32)
    cos, sin = cos_ref[...], sin_ref[...]
    key = jnp.concatenate([r[...] for r in k_refs], axis=0).astype(f32) + shift[:, :HD]
    key = (key * cos + pltpu.roll(key, HD // 2, 1) * sin).astype(bf16)
    val = jnp.concatenate([r[...] for r in v_refs], axis=0).astype(f32) + shift[:, HD:]
    val = val.astype(bf16)
    span = key.shape[0]
    cos_q, sin_q = cos[span - tok :], sin[span - tok :]
    queries, grads = [], []
    for h in range(group):
        q = q_ref[:, h * HD : (h + 1) * HD].astype(f32)
        queries.append((q * cos_q + pltpu.roll(q, HD // 2, 1) * sin_q).astype(bf16))
        grads.append(g_ref[:, h * HD : (h + 1) * HD])
    dot = partial(lax.dot_general, preferred_element_type=f32)
    last, first = (((1,), (1,)), ((), ())), (((0,), (0,)), ((), ()))
    length = span - tok + sub
    dkeys, dvals = [], []
    for i in range(tok // sub):
        cut = slice(i * sub, (i + 1) * sub)
        rows = slice(i * sub, i * sub + length)
        q = jnp.concatenate([x[cut] for x in queries], axis=0)
        g = jnp.concatenate([x[cut] for x in grads], axis=0)
        bias = jnp.concatenate([bias_ref[rows, cut]] * group, axis=1)
        scores = dot(key[rows], q, last) * query_scale + bias
        top = jnp.max(scores, axis=0, keepdims=True)
        probs = jnp.exp(scores - top)
        total = jnp.sum(probs, axis=0, keepdims=True)
        probs = probs * (1.0 / total)
        low_probs = probs.astype(bf16)
        out_t = dot(val[rows], low_probs, first).astype(bf16)
        out = out_t.T
        for h in range(group):
            out_ref[cut, h * HD : (h + 1) * HD] = out[h * sub : (h + 1) * sub]
        drift = jnp.sum(out_t.astype(f32) * g.T.astype(f32), axis=0, keepdims=True)
        dprob = dot(val[rows], g, last)
        dscore = (probs * (dprob - drift)).astype(bf16)
        dkeys.append(jnp.dot(dscore, q, preferred_element_type=f32))
        dvals.append(jnp.dot(low_probs, g, preferred_element_type=f32))

    def overlapped(parts):
        rows = []
        for j in range(span // sub):
            here = [p[(j - i) * sub : (j - i + 1) * sub] for i, p in enumerate(parts) if 0 <= j - i < length // sub]
            rows.append(sum(here[1:], here[0]))
        return jnp.concatenate(rows, axis=0)

    dkey = query_scale * overlapped(dkeys)
    dval = overlapped(dvals)
    dkey = dkey * cos - pltpu.roll(dkey, HD // 2, 1) * sin
    both = jnp.concatenate([dkey.astype(bf16), dval.astype(bf16)], axis=1)
    lg = dot(both, up, last)

    @pl.when(step == 0)
    def _():
        lg_ref[...] = lg_in_ref[...] + lg if chained else lg

    @pl.when(step != 0)
    def _():
        lg_ref[...] += lg

    if lg_low_refs:

        @pl.when(step == pl.num_programs(0) - 1)
        def _():
            for j, ref in enumerate(lg_low_refs):
                ref[...] = lg_ref[j * tok : (j + 1) * tok].astype(bf16)

    u = adapter_scale * dot(spread, both, first)
    half = spread.shape[1] // 2
    u_ref[0] = u[:half, :HD].astype(bf16)
    u_ref[1] = u[half:, HD:].astype(bf16)


def attention(blocks, start, carried, is_last, q_rows, g_rows, spread, up_cat, bias, cos, sin):
    tok = q_rows.shape[0]
    heads = blocks[0].shape[1] // (2 * HD)
    kv_heads, width, _ = up_cat.shape
    group = q_rows.shape[1] // (kv_heads * HD)
    n_blocks = len(blocks)
    span = spread.shape[0]
    half = width // 2
    sub = HD if tok % HD == 0 else tok
    whole = lambda shape: pl.BlockSpec(shape, lambda h: (0,) * len(shape))
    any_space = pl.BlockSpec(memory_space=pl.ANY)
    out_spec = pl.BlockSpec((tok, group * HD), lambda h: (0, h + start))
    u_spec = pl.BlockSpec((2, half, HD), lambda h: (0, 0, h + start))
    in_specs = (
        [pl.BlockSpec((tok, HD), lambda h: (0, h))] * n_blocks
        + [pl.BlockSpec((tok, HD), lambda h: (0, h + heads))] * n_blocks
        + [out_spec] * 2
        + [
            whole((span, width)),
            pl.BlockSpec((1, width, 2 * HD), lambda h: (h + start, 0, 0)),
            whole((span, tok)),
            whole((span, HD)),
            whole((span, HD)),
        ]
    )
    extra, aliases = [], {}
    if carried is not None:
        out, u, lg = carried
        at = len(in_specs)
        extra, aliases = [lg, out, u], {at + 1: 0, at + 2: 1}
        in_specs = in_specs + [whole((span, width)), any_space, any_space]
    low_count = n_blocks - 1 if is_last else 0
    work = heads * group * tok * (span - tok + sub) * HD * 2 * 6
    return pl.pallas_call(
        partial(
            attention_kernel,
            n_blocks=n_blocks,
            tok=tok,
            group=group,
            sub=sub,
            chained=carried is not None,
        ),
        grid=(heads,),
        in_specs=in_specs,
        out_specs=[out_spec, u_spec, whole((span, width))] + [whole((tok, width))] * low_count,
        out_shape=[
            jax.ShapeDtypeStruct(q_rows.shape, bf16),
            jax.ShapeDtypeStruct((2, half, kv_heads * HD), bf16),
            jax.ShapeDtypeStruct((span, width), f32),
        ]
        + [jax.ShapeDtypeStruct((tok, width), bf16)] * low_count,
        input_output_aliases=aliases,
        compiler_params=pltpu.CompilerParams(dimension_semantics=("arbitrary",)),
        cost_estimate=pl.CostEstimate(flops=work, transcendentals=0, bytes_accessed=heads * tok * HD * 20),
        name="attention",
    )(*blocks, *blocks, q_rows, g_rows, spread, up_cat, bias, cos, sin, *extra)


def product_kernel(*refs, n_recv, cols, up_cols):
    side_ref, lg_ref = refs[:2]
    recv = refs[2 : 2 + n_recv]
    mask_ref, hidden_ref = refs[2 + n_recv : 4 + n_recv]
    up_ref, keep_ref, send_ref = refs[4 + n_recv :]
    side = side_ref[0]
    total = lg_ref[...]
    for r in recv:
        total = total + r[...].astype(f32)
    total = total * mask_ref[...]
    width = total.shape[1]
    half = width // 2
    total = jnp.where(side == 0, total, pltpu.roll(total, half, 1)).astype(bf16)
    per_row = cols + up_cols
    rows = half // SUB
    step = 2 if cols % 2 == 0 else 1
    for c in range(0, cols, step):
        w = lax.dot_general(
            total,
            hidden_ref[:, c * HD : (c + step) * HD],
            (((0,), (0,)), ((), ())),
            preferred_element_type=f32,
        ).astype(bf16)
        for j in range(step):
            for r in range(rows):
                tile = w[:, j * HD : (j + 1) * HD]
                keep_ref[r * per_row + c + j] = tile[r * SUB : (r + 1) * SUB]
                send_ref[r * per_row + c + j] = tile[half + r * SUB : half + (r + 1) * SUB]
    for h in range(up_cols):
        for r in range(rows):
            where = (slice(r * SUB, (r + 1) * SUB), slice(h * HD, (h + 1) * HD))
            keep_ref[r * per_row + cols + h] = up_ref[(side,) + where]
            send_ref[r * per_row + cols + h] = up_ref[(1 - side,) + where]
    used = rows * per_row
    if keep_ref.shape[0] > used:
        rest = keep_ref.shape[0] - used
        keep_ref[pl.ds(used, rest)] = jnp.zeros((rest, SUB, HD), bf16)
        send_ref[pl.ds(used, rest)] = jnp.zeros((rest, SUB, HD), bf16)


def assemble_kernel(scalars_ref, ma_ref, mb_ref, ra_ref, rb_ref, w_ref, u_ref, *, cols, rows):
    side, me_a, me_b = scalars_ref[0], scalars_ref[1], scalars_ref[2]
    n_a, a = ma_ref.shape[:2]
    b = mb_ref.shape[1]
    up_cols = u_ref.shape[1] // HD
    per_row = cols + up_cols
    for r in range(rows):
        for c in range(per_row):
            t = r * per_row + c
            if t < n_a * a:
                mine, theirs, piece, off = ma_ref, ra_ref, (t // a) ^ me_a, t % a
            else:
                t -= n_a * a
                mine, theirs, piece, off = mb_ref, rb_ref, (t // b) ^ me_b, t % b
            for src, m in ((mine, side), (theirs, 1 - side)):
                at = pl.multiple_of((m * rows + r) * SUB, SUB)
                tile = src[piece, off].astype(f32)
                if c < cols:
                    w_ref[pl.ds(at, SUB), c * HD : (c + 1) * HD] = tile
                else:
                    u_ref[pl.ds(at, SUB), (c - cols) * HD : (c - cols + 1) * HD] = tile


def axis_bits(axis):
    bits, bit = [], 1
    while bit < lax.axis_size(axis):
        bits.append((axis, bit))
        bit *= 2
    return bits


def bit_of(stage):
    axis, bit = stage
    return ((lax.axis_index(axis) & bit) != 0).astype(jnp.int32)


def direct_peers(axis, bits):
    masks = [0]
    for bit in bits:
        masks = masks + [m | bit for m in masks]
    me = jnp.int32(0)
    for bit in reversed(bits):
        me = me * 2 + bit_of((axis, bit))
    return masks, me


def direct_scatter(tiles, axis, bits):
    masks, me = direct_peers(axis, bits)
    total = lax.dynamic_index_in_dim(tiles, me, 0, keepdims=False).astype(f32)
    for j in range(1, len(masks)):
        part = lax.dynamic_index_in_dim(tiles, me ^ j, 0, keepdims=False)
        total = total + permute_xor(part, axis, masks[j]).astype(f32)
    return total.astype(bf16)


def direct_gather(tiles, axis, bits):
    masks, _ = direct_peers(axis, bits)
    return jnp.stack([tiles] + [permute_xor(tiles, axis, m) for m in masks[1:]])


def scatter_stage(tiles, stage):
    n = tiles.shape[0] // 2
    bit = bit_of(stage)
    send = lax.dynamic_slice_in_dim(tiles, (1 - bit) * n, n, 0)
    keep = lax.dynamic_slice_in_dim(tiles, bit * n, n, 0)
    recv = permute_xor(send, *stage)
    return (keep.astype(f32) + recv.astype(f32)).astype(bf16)


def gather_stage(tiles, stage):
    return jnp.concatenate([tiles, permute_xor(tiles, *stage)], axis=0)


def body(
    hidden,
    frozen_query_rows,
    frozen_key_rows,
    frozen_value_rows,
    next_output_gradient,
    document_lengths,
    document_adapter,
    adapter_down_maps,
    adapter_up_maps,
):
    tok, model_width = hidden.shape[1:]
    kv_width = frozen_key_rows.shape[2]
    kv_heads = kv_width // HD
    _, adapters, rank, _ = adapter_up_maps.shape
    width = 2 * adapters * rank
    half = width // 2
    ctx_index, ctx_size = lax.axis_index("ctx"), lax.axis_size("ctx")
    longest = tok * ctx_size // 4
    reach = min(-(-(min(WINDOW, longest) - 1) // tok), ctx_size - 1)
    steps = (reach + 1) // 2

    pieces = PIECES if sum(PIECES) == kv_heads else (kv_heads,)
    starts = [sum(pieces[:i]) for i in range(len(pieces))]
    keys, vals = frozen_key_rows[0], frozen_value_rows[0]
    parts = []
    for first, count in zip(starts, pieces):
        cut = slice(first * HD, (first + count) * HD)
        own = jnp.concatenate([keys[:, cut], vals[:, cut]], axis=1)
        parts.append(window_blocks(own, steps)[::-1] + [own])
    returned = permute_cyclic(next_output_gradient, "section", -1)

    block_starts = jnp.stack([(ctx_index - d) * tok for d in range(2 * steps, -1, -1)])
    key_pos = (block_starts[:, None] + jnp.arange(tok, dtype=jnp.int32)[None, :]).reshape(-1)
    key_docs = doc_index(document_lengths[0], key_pos)
    positions, docs = key_pos[-tok:], key_docs[-tok:]
    picked = docs[:, None] == jnp.arange(document_lengths.shape[1], dtype=jnp.int32)[None, :]
    tenant = jnp.sum(picked.astype(jnp.int32) * document_adapter[0][None, :], axis=1)
    lane_adapter = (jnp.arange(width, dtype=jnp.int32) // rank) % adapters
    mask = (tenant[:, None] == lane_adapter[None, :]).astype(f32)
    gap = positions[None, :] - key_pos[:, None]
    allowed = (
        (key_docs[:, None] == docs[None, :])
        & (gap >= 0)
        & (gap < WINDOW)
        & (key_pos >= 0)[:, None]
    )
    bias = jnp.where(allowed, 0.0, masked_score).astype(f32)
    frequency = rope_base ** (-(jnp.arange(HD // 2, dtype=f32) * 2.0) / HD)
    angles = key_pos.astype(f32)[:, None] * frequency[None, :]
    cos_half, sin_half = jnp.cos(angles), jnp.sin(angles)
    cos = jnp.concatenate([cos_half, cos_half], axis=1)
    sin = jnp.concatenate([-sin_half, sin_half], axis=1)

    low = jnp.dot(
        hidden[0], adapter_down_maps.reshape(model_width, width), preferred_element_type=f32
    )
    spread_own = (low * mask).astype(bf16)
    spread = jnp.concatenate(window_blocks(spread_own, steps)[::-1] + [spread_own], axis=0)
    up_flat = adapter_up_maps.reshape(2, half, kv_heads, HD)
    zero = jnp.zeros((kv_heads, half, HD), bf16)
    up_heads = jnp.moveaxis(up_flat, 2, 1)
    up_cat = jnp.concatenate(
        [
            jnp.concatenate([up_heads[0], zero], axis=2),
            jnp.concatenate([zero, up_heads[1]], axis=2),
        ],
        axis=1,
    )

    carried = None
    for i in range(len(pieces)):
        result = attention(
            parts[i],
            starts[i],
            carried,
            i == len(pieces) - 1,
            frozen_query_rows[0],
            returned[0],
            spread,
            up_cat,
            bias,
            cos,
            sin,
        )
        carried = result[:3]
    out, ups, lg = carried
    received = [permute_by(low, "ctx", j - 2 * steps) for j, low in enumerate(result[3:])]
    handed = permute_cyclic(out, "section", 1)[None]

    other = (
        axis_bits("ctx")[:1] + axis_bits("dp"),
        axis_bits("dp") + axis_bits("ctx")[:1],
    )
    tail = [bit for _, bit in axis_bits("ctx")[1:]]
    group = lax.axis_size("ctx") * lax.axis_size("dp")
    cols, up_cols, rows = model_width // HD, kv_heads, half // SUB
    units = -(-(rows * (cols + up_cols)) // group)
    a = (units + 1) // 2
    b = units - a
    side = lax.axis_index("section").astype(jnp.int32)
    smem = pl.BlockSpec(memory_space=pltpu.SMEM)
    vmem = pl.BlockSpec(memory_space=pltpu.VMEM)
    keep, send = pl.pallas_call(
        partial(
            product_kernel, n_recv=len(received), cols=cols, up_cols=up_cols
        ),
        in_specs=[smem] + [pl.BlockSpec((tok, width), lambda i: (2 * steps, 0))] + [vmem] * (3 + len(received)),
        grid=(1,),
        out_specs=[vmem, vmem],
        out_shape=[jax.ShapeDtypeStruct((units * group, SUB, HD), bf16)] * 2,
        name="product",
    )(side[None], lg, *received, adapter_scale * mask, hidden[0], ups)
    recv = permute_cyclic(send, "section", 1)
    tiles = (keep.astype(f32) + recv.astype(f32)).astype(bf16)
    colours = [tiles[: a * group], tiles[a * group :]]
    for k in range(len(other[0])):
        colours = [scatter_stage(colours[c], other[c][k]) for c in range(2)]
    rounds = [tail[k : k + 2] for k in range(0, len(tail), 2)]
    members = group >> len(other[0])
    joined = jnp.concatenate([c.reshape(members, -1, SUB, HD) for c in colours], axis=1)
    for bits in rounds:
        joined = joined.reshape(2 ** len(bits), -1, a + b, SUB, HD)
        joined = direct_scatter(joined, "ctx", bits)
    joined = joined.reshape(a + b, SUB, HD)
    ids = []
    for c in range(2):
        me = jnp.int32(0)
        for stage in other[c]:
            me = me * 2 + bit_of(stage)
        for bits in rounds:
            me = me * 2 ** len(bits) + direct_peers("ctx", bits)[1]
        ids.append(me)
    joined = joined[None]
    for bits in reversed(rounds):
        joined = direct_gather(joined, "ctx", bits).reshape(-1, a + b, SUB, HD)
    colours = [
        joined[:, :a].reshape(-1, SUB, HD),
        joined[:, a:].reshape(-1, SUB, HD),
    ]
    for k in reversed(range(len(other[0]))):
        colours = [gather_stage(colours[c], other[c][k]) for c in range(2)]
    theirs = [permute_cyclic(t, "section", 1) for t in colours]
    shapes = [(group, a, SUB, HD), (group, b, SUB, HD)]
    w, u = pl.pallas_call(
        partial(assemble_kernel, cols=cols, rows=rows),
        in_specs=[smem] + [vmem] * 4,
        out_specs=[vmem, vmem],
        out_shape=[
            jax.ShapeDtypeStruct((width, model_width), f32),
            jax.ShapeDtypeStruct((width, kv_width), f32),
        ],
        name="assemble",
    )(
        jnp.stack([side, ids[0], ids[1]]),
        colours[0].reshape(shapes[0]),
        colours[1].reshape(shapes[1]),
        theirs[0].reshape(shapes[0]),
        theirs[1].reshape(shapes[1]),
    )
    down_map_gradient = w.T.reshape(model_width, 2, adapters, rank)
    up_map_gradient = u.reshape(2, adapters, rank, kv_width)
    return (handed, down_map_gradient, up_map_gradient)


def solution(mesh):
    return jax.shard_map(
        body,
        mesh=mesh,
        in_specs=(
            P(("section", "dp"), "ctx", None),
            P(("section", "dp"), "ctx", None),
            P(("section", "dp"), "ctx", None),
            P(("section", "dp"), "ctx", None),
            P(("section", "dp"), "ctx", None),
            P(("section", "dp"), None),
            P(("section", "dp"), None),
            P(),
            P(),
        ),
        out_specs=(P(("section", "dp"), "ctx", None), P(), P()),
        check_vma=False,
    )
```

```python
from functools import partial

import jax
import jax.numpy as jnp
from jax import lax
from jax.experimental import pallas as pl
from jax.experimental.pallas import tpu as pltpu
from jax.sharding import PartitionSpec as P

HD = 128
WINDOW = 1024
SUB = 8
PIECES = 2

query_scale = 168.0 ** (-0.5)
adapter_scale = 0.5
log2e = 1.4426950408889634
rope_base = 10000.0
masked_score = -1e30
f32 = jnp.float32
bf16 = jnp.bfloat16


def permute_by(value, axis, steps):
    count = lax.axis_size(axis)
    first, last = max(0, -steps), min(count, count - steps)
    return lax.ppermute(value, axis, [(i, i + steps) for i in range(first, last)])


def permute_cyclic(value, axis, by):
    count = lax.axis_size(axis)
    return lax.ppermute(value, axis, [(i, (i + by) % count) for i in range(count)])


def permute_xor(value, axis, bit):
    count = lax.axis_size(axis)
    return lax.ppermute(value, axis, [(i, i ^ bit) for i in range(count)])


def window_blocks(own, steps):
    even = lax.axis_index("ctx") % 2 == 0
    chain = [own]
    for _ in range(steps):
        chain.append(permute_by(chain[-1], "ctx", 2))
    blocks = []
    for i in range(steps):
        payload = jnp.where(even, chain[i], chain[i + 1])
        blocks.append(permute_xor(payload, "ctx", 1))
        blocks.append(chain[i + 1])
    return blocks


def doc_index(sequence_lengths, positions):
    doc_ends = jnp.cumsum(sequence_lengths)
    return jnp.sum((doc_ends[None, :] <= positions[:, None]).astype(jnp.int32), axis=1)


def attention_kernel(*refs, n_blocks, heads, tok, group, sub, chained, is_last):
    m_refs = refs[:n_blocks]
    q_ref, g_ref, spread_ref, up_ref, bias_ref, cos_ref, sin_ref = refs[n_blocks : n_blocks + 7]
    at = n_blocks + 7
    if is_last:
        mask_ref = refs[at]
        at += 1
    if chained:
        lg_in_ref = refs[at]
        at += 3
    out_ref, u_ref, lg_ref = refs[at : at + 3]
    lg_low_refs = refs[at + 3 :]
    spread = spread_ref[...]
    span = spread.shape[0]
    half = spread.shape[1] // 2
    cos, sin = cos_ref[...], sin_ref[...]
    dot = partial(lax.dot_general, preferred_element_type=f32)
    last, first = (((1,), (1,)), ((), ())), (((0,), (0,)), ((), ()))
    length = span - tok + sub
    subs = tok // sub

    def prepare(h):
        shift = adapter_scale * jnp.dot(spread, up_ref[h], preferred_element_type=f32)
        kc, vc = slice(h * HD, (h + 1) * HD), slice((heads + h) * HD, (heads + h + 1) * HD)
        key = jnp.concatenate([r[:, kc] for r in m_refs], axis=0).astype(f32) + shift[:, :HD]
        key = (key * cos + pltpu.roll(key, HD // 2, 1) * sin).astype(bf16)
        val = jnp.concatenate([r[:, vc] for r in m_refs], axis=0).astype(f32) + shift[:, HD:]
        return key, val.astype(bf16)

    def scored(h, i, key):
        cut = slice(i * sub, (i + 1) * sub)
        rows = slice(i * sub, i * sub + length)
        cq, sq = cos[span - tok + i * sub : span - tok + (i + 1) * sub], sin[span - tok + i * sub : span - tok + (i + 1) * sub]
        queries = []
        for j in range(group):
            q = q_ref[cut, (h * group + j) * HD : (h * group + j + 1) * HD].astype(f32)
            q = q * cq + pltpu.roll(q, HD // 2, 1) * sq
            queries.append((q * (query_scale * log2e)).astype(bf16))
        q = jnp.concatenate(queries, axis=0)
        bias = jnp.concatenate([bias_ref[rows, cut]] * group, axis=1)
        return q, dot(key[rows], q, last) + bias

    def forward(h, i, scores, val):
        cut = slice(i * sub, (i + 1) * sub)
        rows = slice(i * sub, i * sub + length)
        top = jnp.max(scores, axis=0, keepdims=True)
        probs = jnp.exp2(scores - top)
        scale = 1.0 / jnp.sum(probs, axis=0, keepdims=True)
        low_probs = probs.astype(bf16)
        out_t = (dot(val[rows], low_probs, first) * scale).astype(bf16)
        out = out_t.T
        gs = []
        for j in range(group):
            lanes = slice((h * group + j) * HD, (h * group + j + 1) * HD)
            out_ref[cut, lanes] = out[j * sub : (j + 1) * sub]
            gs.append(g_ref[cut, lanes])
        g_t = (jnp.concatenate(gs, axis=0).T.astype(f32) * scale).astype(bf16)
        drift = jnp.sum(out_t.astype(f32) * g_t.astype(f32), axis=0, keepdims=True)
        dprob = jnp.dot(val[rows], g_t, preferred_element_type=f32)
        return probs, low_probs, g_t, drift, dprob

    def backward(q, state):
        probs, low_probs, g_t, drift, dprob = state
        dscore = (probs * (dprob - drift)).astype(bf16)
        return jnp.dot(dscore, q, preferred_element_type=f32), dot(low_probs, g_t, last)

    def overlapped(parts):
        rows = []
        for j in range(span // sub):
            here = [p[(j - i) * sub : (j - i + 1) * sub] for i, p in enumerate(parts) if 0 <= j - i < length // sub]
            rows.append(sum(here[1:], here[0]))
        return jnp.concatenate(rows, axis=0)

    def finish(h, parts):
        dkey = (1.0 / log2e) * overlapped([p[0] for p in parts])
        dval = overlapped([p[1] for p in parts])
        dkey = dkey * cos - pltpu.roll(dkey, HD // 2, 1) * sin
        both = jnp.concatenate([dkey.astype(bf16), dval.astype(bf16)], axis=1)
        lg = dot(both, up_ref[h], last)
        if h > 0:
            lg_ref[...] += lg
        else:
            lg_ref[...] = lg_in_ref[...] + lg if chained else lg
        u = adapter_scale * dot(spread, both, first)
        u_ref[0, :, h * HD : (h + 1) * HD] = u[:half, :HD].astype(bf16)
        u_ref[1, :, h * HD : (h + 1) * HD] = u[half:, HD:].astype(bf16)

    units = [(h, i) for h in range(heads) for i in range(subs)]
    prepared, scores, states, grads = {}, {}, {}, {}
    for t in range(len(units) + 2):
        if t < len(units):
            h, i = units[t]
            if i == 0:
                prepared[h] = prepare(h)
            scores[h, i] = scored(h, i, prepared[h][0])
        if 0 <= t - 1 < len(units):
            h, i = units[t - 1]
            states[h, i] = forward(h, i, scores[h, i][1], prepared[h][1])
        if 0 <= t - 2 < len(units):
            h, i = units[t - 2]
            grads.setdefault(h, []).append(backward(scores[h, i][0], states[h, i]))
            if i == subs - 1:
                finish(h, grads[h])
    if is_last:
        lg_ref[...] *= mask_ref[...]
    for j, ref in enumerate(lg_low_refs):
        ref[...] = lg_ref[j * tok : (j + 1) * tok].astype(bf16)


def attention(blocks, piece, carried, mask, q_rows, g_rows, spread, up_cat, bias, cos, sin):
    tok = q_rows.shape[0]
    heads = blocks[0].shape[1] // (2 * HD)
    kv_heads, width, _ = up_cat.shape
    group = q_rows.shape[1] // (kv_heads * HD)
    n_blocks = len(blocks)
    span = spread.shape[0]
    half = width // 2
    sub = HD if tok % HD == 0 else tok
    whole = lambda shape: pl.BlockSpec(shape, lambda h: (0,) * len(shape))
    any_space = pl.BlockSpec(memory_space=pl.ANY)
    out_spec = pl.BlockSpec((tok, heads * group * HD), lambda i: (0, piece))
    u_spec = pl.BlockSpec((2, half, heads * HD), lambda i: (0, 0, piece))
    in_specs = (
        [whole((tok, 2 * heads * HD))] * n_blocks
        + [out_spec] * 2
        + [
            whole((span, width)),
            pl.BlockSpec((heads, width, 2 * HD), lambda i: (piece, 0, 0)),
            whole((span, tok)),
            whole((span, HD)),
            whole((span, HD)),
        ]
    )
    extra, aliases = [], {}
    is_last = mask is not None
    if is_last:
        extra = [mask]
        in_specs = in_specs + [whole((span, width))]
    if carried is not None:
        out, u, lg = carried
        at = len(in_specs)
        extra, aliases = extra + [lg, out, u], {at + 1: 0, at + 2: 1}
        in_specs = in_specs + [whole((span, width)), any_space, any_space]
    low_count = n_blocks - 1 if is_last else 0
    work = heads * group * tok * (span - tok + sub) * HD * 2 * 6
    return pl.pallas_call(
        partial(
            attention_kernel,
            n_blocks=n_blocks,
            heads=heads,
            tok=tok,
            group=group,
            sub=sub,
            chained=carried is not None,
            is_last=is_last,
        ),
        grid=(1,),
        in_specs=in_specs,
        out_specs=[out_spec, u_spec, whole((span, width))] + [whole((tok, width))] * low_count,
        out_shape=[
            jax.ShapeDtypeStruct(q_rows.shape, bf16),
            jax.ShapeDtypeStruct((2, half, kv_heads * HD), bf16),
            jax.ShapeDtypeStruct((span, width), f32),
        ]
        + [jax.ShapeDtypeStruct((tok, width), bf16)] * low_count,
        input_output_aliases=aliases,
        compiler_params=pltpu.CompilerParams(dimension_semantics=("arbitrary",)),
        cost_estimate=pl.CostEstimate(flops=work, transcendentals=0, bytes_accessed=heads * tok * HD * 20),
        name="attention",
    )(*blocks, q_rows, g_rows, spread, up_cat, bias, cos, sin, *extra)


def product_kernel(*refs, n_recv, cols, up_cols):
    side_ref, lg_ref = refs[:2]
    recv = refs[2 : 2 + n_recv]
    hidden_ref, up_ref, keep_ref, send_ref = refs[2 + n_recv :]
    side = side_ref[0]
    total = lg_ref[...]
    for r in recv:
        total = total + r[...].astype(f32)
    width = total.shape[1]
    half = width // 2
    total = jnp.where(side == 0, total, pltpu.roll(total, half, 1)).astype(bf16)
    per_row = cols + up_cols
    rows = half // SUB
    step = 2 if cols % 2 == 0 else 1
    for c in range(0, cols, step):
        w = lax.dot_general(
            total,
            hidden_ref[:, c * HD : (c + step) * HD],
            (((0,), (0,)), ((), ())),
            preferred_element_type=f32,
        ).astype(bf16)
        for j in range(step):
            for r in range(rows):
                tile = w[:, j * HD : (j + 1) * HD]
                keep_ref[r * per_row + c + j] = tile[r * SUB : (r + 1) * SUB]
                send_ref[r * per_row + c + j] = tile[half + r * SUB : half + (r + 1) * SUB]
    for h in range(up_cols):
        for r in range(rows):
            where = (slice(r * SUB, (r + 1) * SUB), slice(h * HD, (h + 1) * HD))
            keep_ref[r * per_row + cols + h] = up_ref[(side,) + where]
            send_ref[r * per_row + cols + h] = up_ref[(1 - side,) + where]
    used = rows * per_row
    if keep_ref.shape[0] > used:
        rest = keep_ref.shape[0] - used
        keep_ref[pl.ds(used, rest)] = jnp.zeros((rest, SUB, HD), bf16)
        send_ref[pl.ds(used, rest)] = jnp.zeros((rest, SUB, HD), bf16)


def assemble_kernel(
    scalars_ref, ma_ref, mb_ref, ra_ref, rb_ref, handed_ref, w_ref, u_ref, same_ref, *, cols, rows
):
    side, me_a, me_b = scalars_ref[0], scalars_ref[1], scalars_ref[2]
    n_a, a = ma_ref.shape[:2]
    b = mb_ref.shape[1]
    up_cols = u_ref.shape[1] // HD
    per_row = cols + up_cols
    for r in range(rows):
        for c in range(per_row):
            t = r * per_row + c
            if t < n_a * a:
                mine, theirs, piece, off = ma_ref, ra_ref, (t // a) ^ me_a, t % a
            else:
                t -= n_a * a
                mine, theirs, piece, off = mb_ref, rb_ref, (t // b) ^ me_b, t % b
            for src, m in ((mine, side), (theirs, 1 - side)):
                at = pl.multiple_of((m * rows + r) * SUB, SUB)
                tile = src[piece, off].astype(f32)
                if c < cols:
                    w_ref[pl.ds(at, SUB), c * HD : (c + 1) * HD] = tile
                else:
                    u_ref[pl.ds(at, SUB), (c - cols) * HD : (c - cols + 1) * HD] = tile


def axis_bits(axis):
    bits, bit = [], 1
    while bit < lax.axis_size(axis):
        bits.append((axis, bit))
        bit *= 2
    return bits


def bit_of(stage):
    axis, bit = stage
    return ((lax.axis_index(axis) & bit) != 0).astype(jnp.int32)


def direct_peers(axis, bits):
    masks = [0]
    for bit in bits:
        masks = masks + [m | bit for m in masks]
    me = jnp.int32(0)
    for bit in reversed(bits):
        me = me * 2 + bit_of((axis, bit))
    return masks, me


def direct_scatter(tiles, axis, bits):
    masks, me = direct_peers(axis, bits)
    total = lax.dynamic_index_in_dim(tiles, me, 0, keepdims=False).astype(f32)
    for j in range(1, len(masks)):
        part = lax.dynamic_index_in_dim(tiles, me ^ j, 0, keepdims=False)
        total = total + permute_xor(part, axis, masks[j]).astype(f32)
    return total.astype(bf16)


def direct_gather(tiles, axis, bits):
    masks, _ = direct_peers(axis, bits)
    return jnp.stack([tiles] + [permute_xor(tiles, axis, m) for m in masks[1:]])


def scatter_stage(tiles, stage):
    n = tiles.shape[0] // 2
    bit = bit_of(stage)
    send = lax.dynamic_slice_in_dim(tiles, (1 - bit) * n, n, 0)
    keep = lax.dynamic_slice_in_dim(tiles, bit * n, n, 0)
    recv = permute_xor(send, *stage)
    return (keep.astype(f32) + recv.astype(f32)).astype(bf16)


def gather_stage(tiles, stage):
    return jnp.concatenate([tiles, permute_xor(tiles, *stage)], axis=0)


def body(
    hidden,
    frozen_query_rows,
    frozen_key_rows,
    frozen_value_rows,
    next_output_gradient,
    document_lengths,
    document_adapter,
    adapter_down_maps,
    adapter_up_maps,
):
    tok, model_width = hidden.shape[1:]
    kv_width = frozen_key_rows.shape[2]
    kv_heads = kv_width // HD
    _, adapters, rank, _ = adapter_up_maps.shape
    width = 2 * adapters * rank
    half = width // 2
    ctx_index, ctx_size = lax.axis_index("ctx"), lax.axis_size("ctx")
    longest = tok * ctx_size // 4
    reach = min(-(-(min(WINDOW, longest) - 1) // tok), ctx_size - 1)
    steps = (reach + 1) // 2

    pieces = PIECES if kv_heads % PIECES == 0 else 1
    count = kv_heads // pieces
    keys, vals = frozen_key_rows[0], frozen_value_rows[0]
    parts = []
    for i in range(pieces):
        cut = slice(i * count * HD, (i + 1) * count * HD)
        own = jnp.concatenate([keys[:, cut], vals[:, cut]], axis=1)
        parts.append(window_blocks(own, steps)[::-1] + [own])
    returned = permute_cyclic(next_output_gradient, "section", -1)

    block_starts = jnp.stack([(ctx_index - d) * tok for d in range(2 * steps, -1, -1)])
    key_pos = (block_starts[:, None] + jnp.arange(tok, dtype=jnp.int32)[None, :]).reshape(-1)
    key_docs = doc_index(document_lengths[0], key_pos)
    positions, docs = key_pos[-tok:], key_docs[-tok:]
    picked = key_docs[:, None] == jnp.arange(document_lengths.shape[1], dtype=jnp.int32)[None, :]
    tenant = jnp.sum(picked.astype(jnp.int32) * document_adapter[0][None, :], axis=1)
    lane_adapter = (jnp.arange(width, dtype=jnp.int32) // rank) % adapters
    span_mask = jnp.where(tenant[:, None] == lane_adapter[None, :], adapter_scale, 0.0).astype(f32)
    mask = (tenant[-tok:, None] == lane_adapter[None, :]).astype(f32)
    gap = positions[None, :] - key_pos[:, None]
    allowed = (
        (key_docs[:, None] == docs[None, :])
        & (gap >= 0)
        & (gap < WINDOW)
        & (key_pos >= 0)[:, None]
    )
    bias = jnp.where(allowed, 0.0, masked_score).astype(f32)
    frequency = rope_base ** (-(jnp.arange(HD // 2, dtype=f32) * 2.0) / HD)
    angles = key_pos.astype(f32)[:, None] * frequency[None, :]
    cos_half, sin_half = jnp.cos(angles), jnp.sin(angles)
    cos = jnp.concatenate([cos_half, cos_half], axis=1)
    sin = jnp.concatenate([-sin_half, sin_half], axis=1)

    low = jnp.dot(
        hidden[0], adapter_down_maps.reshape(model_width, width), preferred_element_type=f32
    )
    spread_own = (low * mask).astype(bf16)
    spread = jnp.concatenate(window_blocks(spread_own, steps)[::-1] + [spread_own], axis=0)
    up_flat = adapter_up_maps.reshape(2, half, kv_heads, HD)
    zero = jnp.zeros((kv_heads, half, HD), bf16)
    up_heads = jnp.moveaxis(up_flat, 2, 1)
    up_cat = jnp.concatenate(
        [
            jnp.concatenate([up_heads[0], zero], axis=2),
            jnp.concatenate([zero, up_heads[1]], axis=2),
        ],
        axis=1,
    )

    carried = None
    for i in range(pieces):
        result = attention(
            parts[i],
            i,
            carried,
            span_mask if i == pieces - 1 else None,
            frozen_query_rows[0],
            returned[0],
            spread,
            up_cat,
            bias,
            cos,
            sin,
        )
        carried = result[:3]
    out, ups, lg = carried
    received = [permute_by(low, "ctx", j - 2 * steps) for j, low in enumerate(result[3:])]
    handed = permute_cyclic(out, "section", 1)[None]

    other = (
        axis_bits("ctx")[:1] + axis_bits("dp"),
        axis_bits("dp") + axis_bits("ctx")[:1],
    )
    tail = [bit for _, bit in axis_bits("ctx")[1:]]
    group = lax.axis_size("ctx") * lax.axis_size("dp")
    cols, up_cols, rows = model_width // HD, kv_heads, half // SUB
    units = -(-(rows * (cols + up_cols)) // group)
    a = (units + 1) // 2
    b = units - a
    side = lax.axis_index("section").astype(jnp.int32)
    smem = pl.BlockSpec(memory_space=pltpu.SMEM)
    vmem = pl.BlockSpec(memory_space=pltpu.VMEM)
    keep, send = pl.pallas_call(
        partial(
            product_kernel, n_recv=len(received), cols=cols, up_cols=up_cols
        ),
        in_specs=[smem] + [pl.BlockSpec((tok, width), lambda i: (2 * steps, 0))] + [vmem] * (2 + len(received)),
        grid=(1,),
        out_specs=[vmem, vmem],
        out_shape=[jax.ShapeDtypeStruct((units * group, SUB, HD), bf16)] * 2,
        name="product",
    )(side[None], lg, *received, hidden[0], ups)
    recv = permute_cyclic(send, "section", 1)
    tiles = (keep.astype(f32) + recv.astype(f32)).astype(bf16)
    colours = [tiles[: a * group], tiles[a * group :]]
    for k in range(len(other[0])):
        colours = [scatter_stage(colours[c], other[c][k]) for c in range(2)]
    rounds = [tail[k : k + 2] for k in range(0, len(tail), 2)]
    members = group >> len(other[0])
    joined = jnp.concatenate([c.reshape(members, -1, SUB, HD) for c in colours], axis=1)
    for bits in rounds:
        joined = joined.reshape(2 ** len(bits), -1, a + b, SUB, HD)
        joined = direct_scatter(joined, "ctx", bits)
    joined = joined.reshape(a + b, SUB, HD)
    ids = []
    for c in range(2):
        me = jnp.int32(0)
        for stage in other[c]:
            me = me * 2 + bit_of(stage)
        for bits in rounds:
            me = me * 2 ** len(bits) + direct_peers("ctx", bits)[1]
        ids.append(me)
    joined = joined[None]
    for bits in reversed(rounds):
        joined = direct_gather(joined, "ctx", bits).reshape(-1, a + b, SUB, HD)
    colours = [
        joined[:, :a].reshape(-1, SUB, HD),
        joined[:, a:].reshape(-1, SUB, HD),
    ]
    for k in reversed(range(len(other[0]))):
        colours = [gather_stage(colours[c], other[c][k]) for c in range(2)]
    theirs = [permute_cyclic(t, "section", 1) for t in colours]
    shapes = [(group, a, SUB, HD), (group, b, SUB, HD)]
    any_space = pl.BlockSpec(memory_space=pl.ANY)
    w, u, handed = pl.pallas_call(
        partial(assemble_kernel, cols=cols, rows=rows),
        in_specs=[smem] + [vmem] * 4 + [any_space],
        out_specs=[vmem, vmem, any_space],
        input_output_aliases={5: 2},
        out_shape=[
            jax.ShapeDtypeStruct((width, model_width), f32),
            jax.ShapeDtypeStruct((width, kv_width), f32),
            jax.ShapeDtypeStruct(handed.shape, bf16),
        ],
        name="assemble",
    )(
        jnp.stack([side, ids[0], ids[1]]),
        colours[0].reshape(shapes[0]),
        colours[1].reshape(shapes[1]),
        theirs[0].reshape(shapes[0]),
        theirs[1].reshape(shapes[1]),
        handed,
    )
    down_map_gradient = w.T.reshape(model_width, 2, adapters, rank)
    up_map_gradient = u.reshape(2, adapters, rank, kv_width)
    return (handed, down_map_gradient, up_map_gradient)


def solution(mesh):
    return jax.shard_map(
        body,
        mesh=mesh,
        in_specs=(
            P(("section", "dp"), "ctx", None),
            P(("section", "dp"), "ctx", None),
            P(("section", "dp"), "ctx", None),
            P(("section", "dp"), "ctx", None),
            P(("section", "dp"), "ctx", None),
            P(("section", "dp"), None),
            P(("section", "dp"), None),
            P(),
            P(),
        ),
        out_specs=(P(("section", "dp"), "ctx", None), P(), P()),
        check_vma=False,
    )
```

```python
from functools import partial

import jax
import jax.numpy as jnp
from jax import lax
from jax.experimental import pallas as pl
from jax.experimental.pallas import tpu as pltpu
from jax.sharding import PartitionSpec as P

HD = 128
WINDOW = 1024
SUB = 8
PIECES = 2

query_scale = 168.0 ** (-0.5)
adapter_scale = 0.5
log2e = 1.4426950408889634
rope_base = 10000.0
masked_score = -1e30
f32 = jnp.float32
bf16 = jnp.bfloat16


def permute_by(value, axis, steps):
    count = lax.axis_size(axis)
    first, last = max(0, -steps), min(count, count - steps)
    return lax.ppermute(value, axis, [(i, i + steps) for i in range(first, last)])


def permute_cyclic(value, axis, by):
    count = lax.axis_size(axis)
    return lax.ppermute(value, axis, [(i, (i + by) % count) for i in range(count)])


def permute_xor(value, axis, bit):
    count = lax.axis_size(axis)
    return lax.ppermute(value, axis, [(i, i ^ bit) for i in range(count)])


def window_blocks(own, steps):
    even = lax.axis_index("ctx") % 2 == 0
    chain = [own]
    for _ in range(steps):
        chain.append(permute_by(chain[-1], "ctx", 2))
    blocks = []
    for i in range(steps):
        payload = jnp.where(even, chain[i], chain[i + 1])
        blocks.append(permute_xor(payload, "ctx", 1))
        blocks.append(chain[i + 1])
    return blocks


def doc_index(sequence_lengths, positions):
    doc_ends = jnp.cumsum(sequence_lengths)
    return jnp.sum((doc_ends[None, :] <= positions[:, None]).astype(jnp.int32), axis=1)


def in_vmem(value):
    return pltpu.with_memory_space_constraint(value, pltpu.VMEM)


def attention_kernel(*refs, n_blocks, piece, heads, tok, group, sub, chained, is_last):
    m_refs = refs[:n_blocks]
    q_ref, g_ref, spread_ref, up_ref, bias_ref, cos_ref, sin_ref = refs[n_blocks : n_blocks + 7]
    at = n_blocks + 7
    if is_last:
        mask_ref = refs[at]
        at += 1
    if chained:
        lg_in_ref = refs[at]
        at += 3
    out_ref, u_ref, lg_ref = refs[at : at + 3]
    lg_low_refs = refs[at + 3 :]
    first_head = piece * heads
    spread = spread_ref[...]
    span = spread.shape[0]
    half = spread.shape[1] // 2
    cos, sin = cos_ref[...], sin_ref[...]
    dot = partial(lax.dot_general, preferred_element_type=f32)
    last, first = (((1,), (1,)), ((), ())), (((0,), (0,)), ((), ()))
    length = span - tok + sub
    subs = tok // sub

    def lanes_of(query_head):
        at = first_head * group + query_head
        return slice(at * HD, (at + 1) * HD)

    def prepare(h):
        shift = adapter_scale * jnp.dot(spread, up_ref[first_head + h], preferred_element_type=f32)
        kc, vc = slice(h * HD, (h + 1) * HD), slice((heads + h) * HD, (heads + h + 1) * HD)
        key = jnp.concatenate([r[:, kc] for r in m_refs], axis=0).astype(f32) + shift[:, :HD]
        key = (key * cos + pltpu.roll(key, HD // 2, 1) * sin).astype(bf16)
        val = jnp.concatenate([r[:, vc] for r in m_refs], axis=0).astype(f32) + shift[:, HD:]
        return key, val.astype(bf16)

    def scored(h, i, key):
        cut = slice(i * sub, (i + 1) * sub)
        rows = slice(i * sub, i * sub + length)
        cq, sq = cos[span - tok + i * sub : span - tok + (i + 1) * sub], sin[span - tok + i * sub : span - tok + (i + 1) * sub]
        queries = []
        for j in range(group):
            q = q_ref[cut, lanes_of(h * group + j)].astype(f32)
            q = q * cq + pltpu.roll(q, HD // 2, 1) * sq
            queries.append((q * (query_scale * log2e)).astype(bf16))
        q = jnp.concatenate(queries, axis=0)
        bias = jnp.concatenate([bias_ref[rows, cut]] * group, axis=1)
        return q, dot(key[rows], q, last) + bias

    def forward(h, i, scores, val):
        cut = slice(i * sub, (i + 1) * sub)
        rows = slice(i * sub, i * sub + length)
        top = jnp.max(scores, axis=0, keepdims=True)
        probs = jnp.exp2(scores - top)
        scale = 1.0 / jnp.sum(probs, axis=0, keepdims=True)
        low_probs = probs.astype(bf16)
        out_t = (dot(val[rows], low_probs, first) * scale).astype(bf16)
        out = out_t.T
        gs = []
        for j in range(group):
            lanes = lanes_of(h * group + j)
            out_ref[cut, lanes] = out[j * sub : (j + 1) * sub]
            gs.append(g_ref[cut, lanes])
        g_t = (jnp.concatenate(gs, axis=0).T.astype(f32) * scale).astype(bf16)
        drift = jnp.sum(out_t.astype(f32) * g_t.astype(f32), axis=0, keepdims=True)
        dprob = jnp.dot(val[rows], g_t, preferred_element_type=f32)
        return probs, low_probs, g_t, drift, dprob

    def backward(q, state):
        probs, low_probs, g_t, drift, dprob = state
        dscore = (probs * (dprob - drift)).astype(bf16)
        return jnp.dot(dscore, q, preferred_element_type=f32), dot(low_probs, g_t, last)

    def overlapped(parts):
        rows = []
        for j in range(span // sub):
            here = [p[(j - i) * sub : (j - i + 1) * sub] for i, p in enumerate(parts) if 0 <= j - i < length // sub]
            rows.append(sum(here[1:], here[0]))
        return jnp.concatenate(rows, axis=0)

    def finish(h, parts):
        dkey = (1.0 / log2e) * overlapped([p[0] for p in parts])
        dval = overlapped([p[1] for p in parts])
        dkey = dkey * cos - pltpu.roll(dkey, HD // 2, 1) * sin
        both = jnp.concatenate([dkey.astype(bf16), dval.astype(bf16)], axis=1)
        lg = dot(both, up_ref[first_head + h], last)
        if h > 0:
            lg_ref[...] += lg
        else:
            lg_ref[...] = lg_in_ref[...] + lg if chained else lg
        u = adapter_scale * dot(spread, both, first)
        head_lanes = slice((first_head + h) * HD, (first_head + h + 1) * HD)
        u_ref[0, :, head_lanes] = u[:half, :HD].astype(bf16)
        u_ref[1, :, head_lanes] = u[half:, HD:].astype(bf16)

    units = [(h, i) for h in range(heads) for i in range(subs)]
    prepared, scores, states, grads = {}, {}, {}, {}
    for t in range(len(units) + 2):
        if t < len(units):
            h, i = units[t]
            if i == 0:
                prepared[h] = prepare(h)
            scores[h, i] = scored(h, i, prepared[h][0])
        if 0 <= t - 1 < len(units):
            h, i = units[t - 1]
            states[h, i] = forward(h, i, scores[h, i][1], prepared[h][1])
        if 0 <= t - 2 < len(units):
            h, i = units[t - 2]
            grads.setdefault(h, []).append(backward(scores[h, i][0], states[h, i]))
            if i == subs - 1:
                finish(h, grads[h])
    if is_last:
        lg_ref[...] *= mask_ref[...]
    for j, ref in enumerate(lg_low_refs):
        ref[...] = lg_ref[j * tok : (j + 1) * tok].astype(bf16)


def attention(blocks, piece, carried, mask, q_rows, g_rows, spread, up_cat, bias, cos, sin):
    tok = q_rows.shape[0]
    heads = blocks[0].shape[1] // (2 * HD)
    kv_heads, width, _ = up_cat.shape
    group = q_rows.shape[1] // (kv_heads * HD)
    n_blocks = len(blocks)
    span = spread.shape[0]
    half = width // 2
    sub = HD if tok % HD == 0 else tok
    operands = [*blocks, q_rows, g_rows, spread, up_cat, bias, cos, sin]
    aliases = {}
    is_last = mask is not None
    if is_last:
        operands.append(mask)
    if carried is not None:
        out, u, lg = carried
        at = len(operands)
        operands += [lg, out, u]
        aliases = {at: 2, at + 1: 0, at + 2: 1}
    low_count = n_blocks - 1 if is_last else 0
    work = heads * group * tok * (span - tok + sub) * HD * 2 * 6
    return pl.pallas_call(
        partial(
            attention_kernel,
            n_blocks=n_blocks,
            piece=piece,
            heads=heads,
            tok=tok,
            group=group,
            sub=sub,
            chained=carried is not None,
            is_last=is_last,
        ),
        in_specs=[pl.BlockSpec(memory_space=pltpu.VMEM)] * len(operands),
        out_specs=[pl.BlockSpec(memory_space=pltpu.VMEM)] * (3 + low_count),
        out_shape=[
            pltpu.VMEM(q_rows.shape, bf16),
            pltpu.VMEM((2, half, kv_heads * HD), bf16),
            pltpu.VMEM((span, width), f32),
        ]
        + [pltpu.VMEM((tok, width), bf16)] * low_count,
        input_output_aliases=aliases,
        compiler_params=pltpu.CompilerParams(vmem_limit_bytes=28 << 20),
        cost_estimate=pl.CostEstimate(flops=work, transcendentals=0, bytes_accessed=heads * tok * HD * 20),
        name="attention",
    )(*[in_vmem(x) for x in operands])


def product_kernel(*refs, n_recv, tok, cols, up_cols, chunk):
    side_ref, lg_ref = refs[:2]
    recv = refs[2 : 2 + n_recv]
    up_ref, hidden_hbm, handed_hbm, keep_ref, send_ref, handed_out, hidden_ref, sems = refs[2 + n_recv :]
    loads = []
    for k, c in enumerate(range(0, cols, chunk)):
        lanes = slice(c * HD, min(c + chunk, cols) * HD)
        loads.append(pltpu.make_async_copy(hidden_hbm.at[:, lanes], hidden_ref.at[:, lanes], sems.at[k]))
    handing = pltpu.make_async_copy(handed_hbm, handed_out, sems.at[len(loads)])
    for load in loads:
        load.start()
    handing.start()
    side = side_ref[0]
    total = lg_ref[lg_ref.shape[0] - tok :]
    for r in recv:
        total = total + r[...].astype(f32)
    width = total.shape[1]
    half = width // 2
    total = jnp.where(side == 0, total, pltpu.roll(total, half, 1)).astype(bf16)
    per_row = cols + up_cols
    rows = half // SUB
    for h in range(up_cols):
        for r in range(rows):
            where = (slice(r * SUB, (r + 1) * SUB), slice(h * HD, (h + 1) * HD))
            keep_ref[r * per_row + cols + h] = up_ref[(side,) + where]
            send_ref[r * per_row + cols + h] = up_ref[(1 - side,) + where]
    used = rows * per_row
    if keep_ref.shape[0] > used:
        rest = keep_ref.shape[0] - used
        keep_ref[pl.ds(used, rest)] = jnp.zeros((rest, SUB, HD), bf16)
        send_ref[pl.ds(used, rest)] = jnp.zeros((rest, SUB, HD), bf16)
    step = 2 if cols % 2 == 0 and chunk % 2 == 0 else 1
    for c in range(0, cols, step):
        if c % chunk == 0:
            loads[c // chunk].wait()
        w = lax.dot_general(
            total,
            hidden_ref[:, c * HD : (c + step) * HD],
            (((0,), (0,)), ((), ())),
            preferred_element_type=f32,
        ).astype(bf16)
        for j in range(step):
            for r in range(rows):
                tile = w[:, j * HD : (j + 1) * HD]
                keep_ref[r * per_row + c + j] = tile[r * SUB : (r + 1) * SUB]
                send_ref[r * per_row + c + j] = tile[half + r * SUB : half + (r + 1) * SUB]
    handing.wait()


def assemble_kernel(
    scalars_ref, ma_ref, mb_ref, ra_ref, rb_ref, w_hbm, u_hbm, w_ref, u_ref, sems, *, cols, rows
):
    side, me_a, me_b = scalars_ref[0], scalars_ref[1], scalars_ref[2]
    n_a, a = ma_ref.shape[:2]
    b = mb_ref.shape[1]
    up_cols = u_ref.shape[1] // HD
    per_row = cols + up_cols
    stores = []
    for r in range(rows):
        starts = [pl.multiple_of((m * rows + r) * SUB, SUB) for m in (side, 1 - side)]
        for c in range(per_row):
            t = r * per_row + c
            if t < n_a * a:
                mine, theirs, piece, off = ma_ref, ra_ref, (t // a) ^ me_a, t % a
            else:
                t -= n_a * a
                mine, theirs, piece, off = mb_ref, rb_ref, (t // b) ^ me_b, t % b
            for src, at in zip((mine, theirs), starts):
                tile = src[piece, off].astype(f32)
                if c < cols:
                    w_ref[pl.ds(at, SUB), c * HD : (c + 1) * HD] = tile
                else:
                    u_ref[pl.ds(at, SUB), (c - cols) * HD : (c - cols + 1) * HD] = tile
        for at in starts:
            band = pl.ds(at, SUB)
            stores.append(pltpu.make_async_copy(w_ref.at[band], w_hbm.at[band], sems.at[len(stores)]))
            stores[-1].start()
    stores.append(pltpu.make_async_copy(u_ref, u_hbm, sems.at[len(stores)]))
    stores[-1].start()
    for store in stores:
        store.wait()


def axis_bits(axis):
    bits, bit = [], 1
    while bit < lax.axis_size(axis):
        bits.append((axis, bit))
        bit *= 2
    return bits


def bit_of(stage):
    axis, bit = stage
    return ((lax.axis_index(axis) & bit) != 0).astype(jnp.int32)


def direct_peers(axis, bits):
    masks = [0]
    for bit in bits:
        masks = masks + [m | bit for m in masks]
    me = jnp.int32(0)
    for bit in reversed(bits):
        me = me * 2 + bit_of((axis, bit))
    return masks, me


def direct_scatter(tiles, axis, bits):
    masks, me = direct_peers(axis, bits)
    total = lax.dynamic_index_in_dim(tiles, me, 0, keepdims=False).astype(f32)
    for j in range(1, len(masks)):
        part = lax.dynamic_index_in_dim(tiles, me ^ j, 0, keepdims=False)
        total = total + permute_xor(part, axis, masks[j]).astype(f32)
    return total.astype(bf16)


def direct_gather(tiles, axis, bits):
    masks, _ = direct_peers(axis, bits)
    return jnp.stack([tiles] + [permute_xor(tiles, axis, m) for m in masks[1:]])


def scatter_stage(tiles, stage):
    n = tiles.shape[0] // 2
    bit = bit_of(stage)
    send = lax.dynamic_slice_in_dim(tiles, (1 - bit) * n, n, 0)
    keep = lax.dynamic_slice_in_dim(tiles, bit * n, n, 0)
    recv = permute_xor(send, *stage)
    return (keep.astype(f32) + recv.astype(f32)).astype(bf16)


def gather_stage(tiles, stage):
    return jnp.concatenate([tiles, permute_xor(tiles, *stage)], axis=0)


def step(
    hidden,
    frozen_query_rows,
    frozen_key_rows,
    frozen_value_rows,
    next_output_gradient,
    document_lengths,
    document_adapter,
    adapter_down_maps,
    adapter_up_maps,
):
    tok, model_width = hidden.shape[1:]
    kv_width = frozen_key_rows.shape[2]
    kv_heads = kv_width // HD
    _, adapters, rank, _ = adapter_up_maps.shape
    width = 2 * adapters * rank
    half = width // 2
    ctx_index, ctx_size = lax.axis_index("ctx"), lax.axis_size("ctx")
    longest = tok * ctx_size // 4
    reach = min(-(-(min(WINDOW, longest) - 1) // tok), ctx_size - 1)
    steps = (reach + 1) // 2

    pieces = PIECES if kv_heads % PIECES == 0 else 1
    count = kv_heads // pieces
    keys, vals = frozen_key_rows[0], frozen_value_rows[0]
    parts = []
    for i in range(pieces):
        cut = slice(i * count * HD, (i + 1) * count * HD)
        own = jnp.concatenate([keys[:, cut], vals[:, cut]], axis=1)
        parts.append(window_blocks(own, steps)[::-1] + [own])
    returned = permute_cyclic(next_output_gradient, "section", -1)

    block_starts = jnp.stack([(ctx_index - d) * tok for d in range(2 * steps, -1, -1)])
    key_pos = (block_starts[:, None] + jnp.arange(tok, dtype=jnp.int32)[None, :]).reshape(-1)
    key_docs = doc_index(document_lengths[0], key_pos)
    positions, docs = key_pos[-tok:], key_docs[-tok:]
    picked = key_docs[:, None] == jnp.arange(document_lengths.shape[1], dtype=jnp.int32)[None, :]
    tenant = jnp.sum(picked.astype(jnp.int32) * document_adapter[0][None, :], axis=1)
    lane_adapter = (jnp.arange(width, dtype=jnp.int32) // rank) % adapters
    span_mask = jnp.where(tenant[:, None] == lane_adapter[None, :], adapter_scale, 0.0).astype(f32)
    mask = (tenant[-tok:, None] == lane_adapter[None, :]).astype(f32)
    gap = positions[None, :] - key_pos[:, None]
    allowed = (
        (key_docs[:, None] == docs[None, :])
        & (gap >= 0)
        & (gap < WINDOW)
        & (key_pos >= 0)[:, None]
    )
    bias = jnp.where(allowed, 0.0, masked_score).astype(f32)
    frequency = rope_base ** (-(jnp.arange(HD // 2, dtype=f32) * 2.0) / HD)
    angles = key_pos.astype(f32)[:, None] * frequency[None, :]
    cos_half, sin_half = jnp.cos(angles), jnp.sin(angles)
    cos = jnp.concatenate([cos_half, cos_half], axis=1)
    sin = jnp.concatenate([-sin_half, sin_half], axis=1)

    low = jnp.dot(
        hidden[0], adapter_down_maps.reshape(model_width, width), preferred_element_type=f32
    )
    spread_own = (low * mask).astype(bf16)
    spread = jnp.concatenate(window_blocks(spread_own, steps)[::-1] + [spread_own], axis=0)
    up_flat = adapter_up_maps.reshape(2, half, kv_heads, HD)
    zero = jnp.zeros((kv_heads, half, HD), bf16)
    up_heads = jnp.moveaxis(up_flat, 2, 1)
    up_cat = jnp.concatenate(
        [
            jnp.concatenate([up_heads[0], zero], axis=2),
            jnp.concatenate([zero, up_heads[1]], axis=2),
        ],
        axis=1,
    )

    carried = None
    for i in range(pieces):
        result = attention(
            parts[i],
            i,
            carried,
            span_mask if i == pieces - 1 else None,
            frozen_query_rows[0],
            returned[0],
            spread,
            up_cat,
            bias,
            cos,
            sin,
        )
        carried = result[:3]
    out, ups, lg = carried
    received = [permute_by(low, "ctx", j - 2 * steps) for j, low in enumerate(result[3:])]
    handed = permute_cyclic(out, "section", 1)[None]

    other = (
        axis_bits("ctx")[:1] + axis_bits("dp"),
        axis_bits("dp") + axis_bits("ctx")[:1],
    )
    tail = [bit for _, bit in axis_bits("ctx")[1:]]
    group = lax.axis_size("ctx") * lax.axis_size("dp")
    cols, up_cols, rows = model_width // HD, kv_heads, half // SUB
    units = -(-(rows * (cols + up_cols)) // group)
    a = (units + 1) // 2
    b = units - a
    side = lax.axis_index("section").astype(jnp.int32)
    smem = pl.BlockSpec(memory_space=pltpu.SMEM)
    vmem = pl.BlockSpec(memory_space=pltpu.VMEM)
    any_space = pl.BlockSpec(memory_space=pl.ANY)
    chunk = -(-cols // 6)
    chunk += chunk % 2
    tile_shape = (units * group, SUB, HD)
    keep, send, handed = pl.pallas_call(
        partial(
            product_kernel, n_recv=len(received), tok=tok, cols=cols, up_cols=up_cols, chunk=chunk
        ),
        in_specs=[smem] + [vmem] * (2 + len(received)) + [any_space] * 2,
        out_specs=[vmem, vmem, any_space],
        out_shape=[
            pltpu.VMEM(tile_shape, bf16),
            pltpu.VMEM(tile_shape, bf16),
            jax.ShapeDtypeStruct(handed.shape, bf16),
        ],
        scratch_shapes=[
            pltpu.VMEM((tok, model_width), bf16),
            pltpu.SemaphoreType.DMA((-(-cols // chunk) + 1,)),
        ],
        compiler_params=pltpu.CompilerParams(vmem_limit_bytes=16 << 20),
        name="product",
    )(side[None], in_vmem(lg), *[in_vmem(r) for r in received], in_vmem(ups), hidden[0], handed)
    recv = permute_cyclic(send, "section", 1)
    tiles = (keep.astype(f32) + recv.astype(f32)).astype(bf16)
    colours = [tiles[: a * group], tiles[a * group :]]
    for k in range(len(other[0])):
        colours = [scatter_stage(colours[c], other[c][k]) for c in range(2)]
    rounds = [tail[k : k + 2] for k in range(0, len(tail), 2)]
    members = group >> len(other[0])
    joined = jnp.concatenate([c.reshape(members, -1, SUB, HD) for c in colours], axis=1)
    for bits in rounds:
        joined = joined.reshape(2 ** len(bits), -1, a + b, SUB, HD)
        joined = direct_scatter(joined, "ctx", bits)
    joined = joined.reshape(a + b, SUB, HD)
    ids = []
    for c in range(2):
        me = jnp.int32(0)
        for stage in other[c]:
            me = me * 2 + bit_of(stage)
        for bits in rounds:
            me = me * 2 ** len(bits) + direct_peers("ctx", bits)[1]
        ids.append(me)
    joined = joined[None]
    for bits in reversed(rounds):
        joined = direct_gather(joined, "ctx", bits).reshape(-1, a + b, SUB, HD)
    colours = [
        joined[:, :a].reshape(-1, SUB, HD),
        joined[:, a:].reshape(-1, SUB, HD),
    ]
    for k in reversed(range(len(other[0]))):
        colours = [gather_stage(colours[c], other[c][k]) for c in range(2)]
    theirs = [permute_cyclic(t, "section", 1) for t in colours]
    shapes = [(group, a, SUB, HD), (group, b, SUB, HD)]
    w, u = pl.pallas_call(
        partial(assemble_kernel, cols=cols, rows=rows),
        in_specs=[smem] + [vmem] * 4,
        out_specs=[any_space, any_space],
        out_shape=[
            jax.ShapeDtypeStruct((width, model_width), f32),
            jax.ShapeDtypeStruct((width, kv_width), f32),
        ],
        scratch_shapes=[
            pltpu.VMEM((width, model_width), f32),
            pltpu.VMEM((width, kv_width), f32),
            pltpu.SemaphoreType.DMA((2 * rows + 1,)),
        ],
        compiler_params=pltpu.CompilerParams(vmem_limit_bytes=16 << 20),
        name="assemble",
    )(
        jnp.stack([side, ids[0], ids[1]]),
        in_vmem(colours[0].reshape(shapes[0])),
        in_vmem(colours[1].reshape(shapes[1])),
        in_vmem(theirs[0].reshape(shapes[0])),
        in_vmem(theirs[1].reshape(shapes[1])),
    )
    down_map_gradient = w.T.reshape(model_width, 2, adapters, rank)
    up_map_gradient = u.reshape(2, adapters, rank, kv_width)
    return (handed, down_map_gradient, up_map_gradient)


def solution(mesh):
    return jax.shard_map(
        step,
        mesh=mesh,
        in_specs=(
            P(("section", "dp"), "ctx", None),
            P(("section", "dp"), "ctx", None),
            P(("section", "dp"), "ctx", None),
            P(("section", "dp"), "ctx", None),
            P(("section", "dp"), "ctx", None),
            P(("section", "dp"), None),
            P(("section", "dp"), None),
            P(),
            P(),
        ),
        out_specs=(P(("section", "dp"), "ctx", None), P(), P()),
        check_vma=False,
    )
```

```python
from functools import partial

import jax
import jax.numpy as jnp
from jax import lax
from jax.experimental import pallas as pl
from jax.experimental.pallas import tpu as pltpu
from jax.sharding import PartitionSpec as P

HD = 128
WINDOW = 1024
SUB = 16
PIECES = 4

query_scale = 168.0 ** (-0.5)
adapter_scale = 0.5
log2e = 1.4426950408889634
rope_base = 10000.0
masked_score = -1e30
f32 = jnp.float32
bf16 = jnp.bfloat16


def permute_by(value, axis, steps):
    count = lax.axis_size(axis)
    first, last = max(0, -steps), min(count, count - steps)
    return lax.ppermute(value, axis, [(i, i + steps) for i in range(first, last)])


def permute_cyclic(value, axis, by):
    count = lax.axis_size(axis)
    return lax.ppermute(value, axis, [(i, (i + by) % count) for i in range(count)])


def permute_xor(value, axis, bit):
    count = lax.axis_size(axis)
    return lax.ppermute(value, axis, [(i, i ^ bit) for i in range(count)])


def window_blocks(own, steps):
    even = lax.axis_index("ctx") % 2 == 0
    chain = [own]
    for _ in range(steps):
        chain.append(permute_by(chain[-1], "ctx", 2))
    blocks = []
    for i in range(steps):
        payload = jnp.where(even, chain[i], chain[i + 1])
        blocks.append(permute_xor(payload, "ctx", 1))
        blocks.append(chain[i + 1])
    return blocks


def doc_index(sequence_lengths, positions):
    doc_ends = jnp.cumsum(sequence_lengths)
    return jnp.sum((doc_ends[None, :] <= positions[:, None]).astype(jnp.int32), axis=1)


def in_hbm(value):
    return pltpu.with_memory_space_constraint(value, pltpu.HBM)


def chunks_of(cols):
    chunk = -(-cols // 6)
    chunk += chunk % 2
    return [slice(c * HD, min(c + chunk, cols) * HD) for c in range(0, cols, chunk)]


def pack_kernel(hidden_hbm, down_hbm, key_hbm, val_hbm, *refs, pieces, heads, lanes):
    messages = refs[:pieces]
    hidden_ref, down_ref, sems = refs[pieces:]
    loads, packs = [], []
    for k, cut in enumerate(lanes):
        loads.append(
            [
                pltpu.make_async_copy(hidden_hbm.at[:, cut], hidden_ref.at[:, cut], sems.at[2 * k]),
                pltpu.make_async_copy(down_hbm.at[:, cut], down_ref.at[:, cut], sems.at[2 * k + 1]),
            ]
        )
    at = 2 * len(lanes)
    for i, message in enumerate(messages):
        cut = slice(i * heads * HD, (i + 1) * heads * HD)
        for j, rows in enumerate((key_hbm, val_hbm)):
            target = message.at[:, j * heads * HD : (j + 1) * heads * HD]
            packs.append(pltpu.make_async_copy(rows.at[:, cut], target, sems.at[at]))
            at += 1
    for pair in loads:
        for load in pair:
            load.start()
    for pack in packs:
        pack.start()
    low = None
    for pair, cut in zip(loads, lanes):
        for load in pair:
            load.wait()
        part = lax.dot_general(
            hidden_ref[:, cut],
            down_ref[:, cut],
            (((1,), (1,)), ((), ())),
            preferred_element_type=f32,
        )
        low = part if low is None else low + part
    messages[0][:, 2 * heads * HD :] = low.astype(bf16)
    for pack in packs:
        pack.wait()


def pack(hidden, down, keys, vals, pieces):
    tok, model_width = hidden.shape
    width = down.shape[0]
    heads = keys.shape[1] // HD // pieces
    lanes = chunks_of(model_width // HD)
    return pl.pallas_call(
        partial(pack_kernel, pieces=pieces, heads=heads, lanes=lanes),
        in_specs=[pl.BlockSpec(memory_space=pltpu.HBM)] * 4,
        out_specs=[pl.BlockSpec(memory_space=pltpu.VMEM)] * pieces,
        out_shape=[
            pltpu.VMEM((tok, 2 * heads * HD + (width if i == 0 else 0)), bf16)
            for i in range(pieces)
        ],
        scratch_shapes=[
            pltpu.VMEM((tok, model_width), bf16),
            pltpu.VMEM((width, model_width), bf16),
            pltpu.SemaphoreType.DMA((2 * len(lanes) + 2 * pieces,)),
        ],
        compiler_params=pltpu.CompilerParams(vmem_limit_bytes=16 << 20),
        name="pack",
    )(in_hbm(hidden), in_hbm(down), in_hbm(keys), in_hbm(vals))


def in_vmem(value):
    return pltpu.with_memory_space_constraint(value, pltpu.VMEM)


def attention_kernel(*refs, n_blocks, piece, heads, tok, group, sub, rank, chained, is_last):
    m_refs = refs[:n_blocks]
    q_ref, up_ref, bias_ref, cos_ref, sin_ref, mask_ref, g_hbm = refs[n_blocks : n_blocks + 7]
    at = n_blocks + 7
    if chained:
        spread_ref, lg_in_ref = refs[at : at + 2]
        at += 4
    out_ref, u_ref = refs[at : at + 2]
    at += 2
    if not is_last:
        lg_ref = refs[at]
        at += 1
    else:
        low_refs = refs[at : at + n_blocks]
        at += n_blocks
    if not chained:
        spread_ref = refs[at]
        at += 1
    if is_last:
        lg_ref = refs[at]
        at += 1
    g_ref, g_sem = refs[at:]
    first_head = piece * heads
    g_lanes = slice(first_head * group * HD, (first_head + heads) * group * HD)
    g_load = pltpu.make_async_copy(g_hbm.at[:, g_lanes], g_ref, g_sem)
    g_load.start()
    if not chained:
        low_lanes = slice(2 * heads * HD, None)
        low = jnp.concatenate([r[:, low_lanes] for r in m_refs], axis=0).astype(f32)
        spread_ref[...] = (low * mask_ref[...]).astype(bf16)
    spread = spread_ref[...]
    span = spread.shape[0]
    half = spread.shape[1] // 2
    cos, sin = cos_ref[...], sin_ref[...]
    dot = partial(lax.dot_general, preferred_element_type=f32)
    last, first = (((1,), (1,)), ((), ())), (((0,), (0,)), ((), ()))
    length = span - tok + sub
    subs = tok // sub

    def lanes_of(query_head):
        at = first_head * group + query_head
        return slice(at * HD, (at + 1) * HD)

    def prepare(h):
        shift = adapter_scale * jnp.dot(spread, up_ref[first_head + h], preferred_element_type=f32)
        kc, vc = slice(h * HD, (h + 1) * HD), slice((heads + h) * HD, (heads + h + 1) * HD)
        key = jnp.concatenate([r[:, kc] for r in m_refs], axis=0).astype(f32) + shift[:, :HD]
        key = (key * cos + pltpu.roll(key, HD // 2, 1) * sin).astype(bf16)
        val = jnp.concatenate([r[:, vc] for r in m_refs], axis=0).astype(f32) + shift[:, HD:]
        return key, val.astype(bf16)

    def scored(h, i, key):
        cut = slice(i * sub, (i + 1) * sub)
        rows = slice(i * sub, i * sub + length)
        cq, sq = cos[span - tok + i * sub : span - tok + (i + 1) * sub], sin[span - tok + i * sub : span - tok + (i + 1) * sub]
        queries = []
        for j in range(group):
            q = q_ref[cut, lanes_of(h * group + j)].astype(f32)
            q = q * cq + pltpu.roll(q, HD // 2, 1) * sq
            queries.append((q * (query_scale * log2e)).astype(bf16))
        q = jnp.concatenate(queries, axis=0)
        bias = jnp.concatenate([bias_ref[rows, cut]] * group, axis=1)
        return q, dot(key[rows], q, last) + bias

    def forward(h, i, scores, val):
        cut = slice(i * sub, (i + 1) * sub)
        rows = slice(i * sub, i * sub + length)
        top = jnp.max(scores, axis=0, keepdims=True)
        probs = jnp.exp2(scores - top)
        scale = 1.0 / jnp.sum(probs, axis=0, keepdims=True)
        low_probs = probs.astype(bf16)
        out_t = (dot(val[rows], low_probs, first) * scale).astype(bf16)
        out = out_t.T
        gs = []
        for j in range(group):
            lanes = lanes_of(h * group + j)
            out_ref[cut, lanes] = out[j * sub : (j + 1) * sub]
            gs.append(g_ref[cut, (h * group + j) * HD : (h * group + j + 1) * HD])
        g_t = (jnp.concatenate(gs, axis=0).T.astype(f32) * scale).astype(bf16)
        drift = jnp.sum(out_t.astype(f32) * g_t.astype(f32), axis=0, keepdims=True)
        dprob = jnp.dot(val[rows], g_t, preferred_element_type=f32)
        return probs, low_probs, g_t, drift, dprob

    def backward(q, state):
        probs, low_probs, g_t, drift, dprob = state
        dscore = (probs * (dprob - drift)).astype(bf16)
        return jnp.dot(dscore, q, preferred_element_type=f32), dot(low_probs, g_t, last)

    def overlapped(parts):
        rows = []
        for j in range(span // sub):
            here = [p[(j - i) * sub : (j - i + 1) * sub] for i, p in enumerate(parts) if 0 <= j - i < length // sub]
            rows.append(sum(here[1:], here[0]))
        return jnp.concatenate(rows, axis=0)

    def finish(h, parts):
        dkey = (1.0 / log2e) * overlapped([p[0] for p in parts])
        dval = overlapped([p[1] for p in parts])
        dkey = dkey * cos - pltpu.roll(dkey, HD // 2, 1) * sin
        both = jnp.concatenate([dkey.astype(bf16), dval.astype(bf16)], axis=1)
        lg = dot(both, up_ref[first_head + h], last)
        if h > 0:
            lg_ref[...] += lg
        else:
            lg_ref[...] = lg_in_ref[...] + lg if chained else lg
        u = adapter_scale * dot(spread, both, first)
        head_lanes = slice((first_head + h) * HD, (first_head + h + 1) * HD)
        u_ref[0, :, head_lanes] = u[:half, :HD].astype(bf16)
        u_ref[1, :, head_lanes] = u[half:, HD:].astype(bf16)

    units = [(h, i) for h in range(heads) for i in range(subs)]
    prepared, scores, states, grads = {}, {}, {}, {}
    for t in range(len(units) + 2):
        if t < len(units):
            h, i = units[t]
            if i == 0:
                prepared[h] = prepare(h)
            scores[h, i] = scored(h, i, prepared[h][0])
        if t == 1:
            g_load.wait()
        if 0 <= t - 1 < len(units):
            h, i = units[t - 1]
            states[h, i] = forward(h, i, scores[h, i][1], prepared[h][1])
        if 0 <= t - 2 < len(units):
            h, i = units[t - 2]
            grads.setdefault(h, []).append(backward(scores[h, i][0], states[h, i]))
            if i == subs - 1:
                finish(h, grads[h])
    if is_last:
        masked = (adapter_scale * lg_ref[...] * mask_ref[...]).astype(bf16)
        compact = dot(picks(2 * half, rank), masked, last)
        for j, ref in enumerate(low_refs):
            ref[...] = compact[:, j * tok : (j + 1) * tok].astype(bf16)


def picks(width, rank):
    row = lax.broadcasted_iota(jnp.int32, (2 * rank, width), 0)
    col = lax.broadcasted_iota(jnp.int32, (2 * rank, width), 1)
    hit = (row // rank == col // (width // 2)) & (row % rank == col % rank)
    return hit.astype(f32).astype(bf16)


def attention(blocks, piece, pieces, carried, mask, q_rows, g_rows, up_cat, bias, cos, sin, rank):
    tok = q_rows.shape[0]
    kv_heads, width, _ = up_cat.shape
    heads = kv_heads // pieces
    group = q_rows.shape[1] // (kv_heads * HD)
    n_blocks = len(blocks)
    span = bias.shape[0]
    half = width // 2
    sub = HD if tok % HD == 0 else tok
    operands = [in_vmem(x) for x in (*blocks, q_rows, up_cat, bias, cos, sin, mask)]
    operands.append(in_hbm(g_rows))
    aliases = {}
    is_last = piece == pieces - 1
    resident = [pl.BlockSpec(memory_space=pltpu.VMEM)]
    in_specs = resident * (len(operands) - 1) + [pl.BlockSpec(memory_space=pltpu.HBM)]
    if carried is not None:
        at = len(operands)
        aliases = {at + 2: 0, at + 3: 1}
        if not is_last:
            aliases[at + 1] = 2
        out, u, lg, spread = carried
        operands += [in_vmem(x) for x in (spread, lg, out, u)]
        in_specs = in_specs + resident * 4
    out_shape = [pltpu.VMEM(q_rows.shape, bf16), pltpu.VMEM((2, half, kv_heads * HD), bf16)]
    scratch = []
    if is_last:
        out_shape += [pltpu.VMEM((2 * rank, tok), bf16)] * n_blocks
        scratch = [pltpu.VMEM((span, width), f32)]
    else:
        out_shape.append(pltpu.VMEM((span, width), f32))
    if carried is None:
        out_shape.append(pltpu.VMEM((span, width), bf16))
    work = heads * group * tok * (span - tok + sub) * HD * 2 * 6
    result = pl.pallas_call(
        partial(
            attention_kernel,
            n_blocks=n_blocks,
            piece=piece,
            heads=heads,
            tok=tok,
            group=group,
            sub=sub,
            rank=rank,
            chained=carried is not None,
            is_last=is_last,
        ),
        in_specs=in_specs,
        out_specs=resident * len(out_shape),
        out_shape=out_shape,
        scratch_shapes=scratch
        + [pltpu.VMEM((tok, heads * group * HD), bf16), pltpu.SemaphoreType.DMA(())],
        input_output_aliases=aliases,
        compiler_params=pltpu.CompilerParams(vmem_limit_bytes=28 << 20),
        cost_estimate=pl.CostEstimate(flops=work, transcendentals=0, bytes_accessed=heads * tok * HD * 20),
        name="attention",
    )(*operands)
    if is_last:
        return result
    return (*result[:3], result[3] if carried is None else spread)


def product_kernel(*refs, n_recv, lanes, up_cols):
    side_ref, own_ref = refs[:2]
    recv = refs[2 : 2 + n_recv]
    mask_ref, up_ref, hidden_hbm, handed_hbm = refs[2 + n_recv : 6 + n_recv]
    keep_ref, send_ref, handed_out, hidden_ref, sems = refs[6 + n_recv :]
    loads = [
        pltpu.make_async_copy(hidden_hbm.at[:, cut], hidden_ref.at[:, cut], sems.at[k])
        for k, cut in enumerate(lanes)
    ]
    handing = pltpu.make_async_copy(handed_hbm, handed_out, sems.at[len(loads)])
    for load in loads:
        load.start()
    handing.start()
    side = side_ref[0]
    total = own_ref[...].astype(f32)
    for r in recv:
        total = total + r[...].astype(f32)
    width = mask_ref.shape[0]
    half = width // 2
    cols = hidden_ref.shape[1] // HD
    total = lax.dot_general(
        picks(width, total.shape[0] // 2),
        total.astype(bf16),
        (((0,), (0,)), ((), ())),
        preferred_element_type=f32,
    )
    total = total * mask_ref[...]
    swapped = jnp.concatenate([total[half:], total[:half]], axis=0)
    total = jnp.where(side == 0, total, swapped).astype(bf16)
    per_row = cols + up_cols
    rows = half // SUB
    for h in range(up_cols):
        for r in range(rows):
            where = (slice(r * SUB, (r + 1) * SUB), slice(h * HD, (h + 1) * HD))
            keep_ref[r * per_row + cols + h] = up_ref[(side,) + where]
            send_ref[r * per_row + cols + h] = up_ref[(1 - side,) + where]
    used = rows * per_row
    if keep_ref.shape[0] > used:
        rest = keep_ref.shape[0] - used
        keep_ref[pl.ds(used, rest)] = jnp.zeros((rest, SUB, HD), bf16)
        send_ref[pl.ds(used, rest)] = jnp.zeros((rest, SUB, HD), bf16)
    step = 2 if cols % 2 == 0 else 1
    starts = [cut.start // HD for cut in lanes]
    for c in range(0, cols, step):
        if c in starts:
            loads[starts.index(c)].wait()
        w = jnp.dot(
            total, hidden_ref[:, c * HD : (c + step) * HD], preferred_element_type=f32
        ).astype(bf16)
        for j in range(step):
            for r in range(rows):
                tile = w[:, j * HD : (j + 1) * HD]
                keep_ref[r * per_row + c + j] = tile[r * SUB : (r + 1) * SUB]
                send_ref[r * per_row + c + j] = tile[half + r * SUB : half + (r + 1) * SUB]
    handing.wait()


def merge_kernel(keep_ref, recv_ref, *out_refs):
    at = 0
    for ref in out_refs:
        rows = slice(at, at + ref.shape[0])
        ref[...] = (keep_ref[rows].astype(f32) + recv_ref[rows].astype(f32)).astype(bf16)
        at += ref.shape[0]


def assemble_kernel(
    scalars_ref, ma_ref, mb_ref, ra_ref, rb_ref, w_hbm, u_hbm, w_ref, u_ref, sems, *, cols, rows
):
    side, me_a, me_b = scalars_ref[0], scalars_ref[1], scalars_ref[2]
    n_a, a = ma_ref.shape[:2]
    b = mb_ref.shape[1]
    up_cols = u_ref.shape[1] // HD
    per_row = cols + up_cols
    stores = []
    for r in range(rows):
        starts = [pl.multiple_of((m * rows + r) * SUB, SUB) for m in (side, 1 - side)]
        for c in range(per_row):
            t = r * per_row + c
            if t < n_a * a:
                mine, theirs, piece, off = ma_ref, ra_ref, (t // a) ^ me_a, t % a
            else:
                t -= n_a * a
                mine, theirs, piece, off = mb_ref, rb_ref, (t // b) ^ me_b, t % b
            for src, at in zip((mine, theirs), starts):
                tile = src[piece, off].astype(f32)
                if c < cols:
                    w_ref[pl.ds(at, SUB), c * HD : (c + 1) * HD] = tile
                else:
                    u_ref[pl.ds(at, SUB), (c - cols) * HD : (c - cols + 1) * HD] = tile
        for at in starts:
            band = pl.ds(at, SUB)
            stores.append(pltpu.make_async_copy(w_ref.at[band], w_hbm.at[band], sems.at[len(stores)]))
            stores[-1].start()
    stores.append(pltpu.make_async_copy(u_ref, u_hbm, sems.at[len(stores)]))
    stores[-1].start()
    for store in stores:
        store.wait()


def axis_bits(axis):
    bits, bit = [], 1
    while bit < lax.axis_size(axis):
        bits.append((axis, bit))
        bit *= 2
    return bits


def bit_of(stage):
    axis, bit = stage
    return ((lax.axis_index(axis) & bit) != 0).astype(jnp.int32)


def direct_peers(axis, bits):
    masks = [0]
    for bit in bits:
        masks = masks + [m | bit for m in masks]
    me = jnp.int32(0)
    for bit in reversed(bits):
        me = me * 2 + bit_of((axis, bit))
    return masks, me


def direct_scatter(tiles, axis, bits):
    masks, me = direct_peers(axis, bits)
    total = lax.dynamic_index_in_dim(tiles, me, 0, keepdims=False).astype(f32)
    for j in range(1, len(masks)):
        part = lax.dynamic_index_in_dim(tiles, me ^ j, 0, keepdims=False)
        total = total + permute_xor(part, axis, masks[j]).astype(f32)
    return total.astype(bf16)


def direct_gather(tiles, axis, bits):
    masks, _ = direct_peers(axis, bits)
    return jnp.stack([tiles] + [permute_xor(tiles, axis, m) for m in masks[1:]])


def scatter_stage(tiles, stage):
    n = tiles.shape[0] // 2
    bit = bit_of(stage)
    send = lax.dynamic_slice_in_dim(tiles, (1 - bit) * n, n, 0)
    keep = lax.dynamic_slice_in_dim(tiles, bit * n, n, 0)
    recv = permute_xor(send, *stage)
    return (keep.astype(f32) + recv.astype(f32)).astype(bf16)


def gather_stage(tiles, stage):
    return jnp.concatenate([tiles, permute_xor(tiles, *stage)], axis=0)


def step(
    hidden,
    frozen_query_rows,
    frozen_key_rows,
    frozen_value_rows,
    next_output_gradient,
    document_lengths,
    document_adapter,
    adapter_down_maps,
    adapter_up_maps,
):
    tok, model_width = hidden.shape[1:]
    kv_width = frozen_key_rows.shape[2]
    kv_heads = kv_width // HD
    _, adapters, rank, _ = adapter_up_maps.shape
    width = 2 * adapters * rank
    half = width // 2
    ctx_index, ctx_size = lax.axis_index("ctx"), lax.axis_size("ctx")
    longest = tok * ctx_size // 4
    reach = min(-(-(min(WINDOW, longest) - 1) // tok), ctx_size - 1)
    steps = (reach + 1) // 2

    pieces = PIECES if kv_heads % PIECES == 0 else 1
    down = adapter_down_maps.reshape(model_width, width).T
    messages = pack(hidden[0], down, frozen_key_rows[0], frozen_value_rows[0], pieces)
    parts = [window_blocks(m, steps)[::-1] + [m] for m in messages]
    returned = permute_cyclic(next_output_gradient, "section", -1)

    block_starts = jnp.stack([(ctx_index - d) * tok for d in range(2 * steps, -1, -1)])
    key_pos = (block_starts[:, None] + jnp.arange(tok, dtype=jnp.int32)[None, :]).reshape(-1)
    key_docs = doc_index(document_lengths[0], key_pos)
    positions, docs = key_pos[-tok:], key_docs[-tok:]
    picked = key_docs[:, None] == jnp.arange(document_lengths.shape[1], dtype=jnp.int32)[None, :]
    tenant = jnp.sum(picked.astype(jnp.int32) * document_adapter[0][None, :], axis=1)
    lane_adapter = (jnp.arange(width, dtype=jnp.int32) // rank) % adapters
    mask = (tenant[:, None] == lane_adapter[None, :]).astype(f32)
    own_mask = (lane_adapter[:, None] == tenant[None, -tok:]).astype(f32)
    gap = positions[None, :] - key_pos[:, None]
    allowed = (
        (key_docs[:, None] == docs[None, :])
        & (gap >= 0)
        & (gap < WINDOW)
        & (key_pos >= 0)[:, None]
    )
    bias = jnp.where(allowed, 0.0, masked_score).astype(f32)
    frequency = rope_base ** (-(jnp.arange(HD // 2, dtype=f32) * 2.0) / HD)
    angles = key_pos.astype(f32)[:, None] * frequency[None, :]
    cos_half, sin_half = jnp.cos(angles), jnp.sin(angles)
    cos = jnp.concatenate([cos_half, cos_half], axis=1)
    sin = jnp.concatenate([-sin_half, sin_half], axis=1)
    up_flat = adapter_up_maps.reshape(2, half, kv_heads, HD)
    zero = jnp.zeros((kv_heads, half, HD), bf16)
    up_heads = jnp.moveaxis(up_flat, 2, 1)
    up_cat = jnp.concatenate(
        [
            jnp.concatenate([up_heads[0], zero], axis=2),
            jnp.concatenate([zero, up_heads[1]], axis=2),
        ],
        axis=1,
    )

    carried = None
    for i in range(pieces):
        carried = attention(
            parts[i],
            i,
            pieces,
            carried,
            mask,
            frozen_query_rows[0],
            returned[0],
            up_cat,
            bias,
            cos,
            sin,
            rank,
        )
    out, ups = carried[:2]
    lows = carried[2:]
    received = [permute_by(low, "ctx", j - 2 * steps) for j, low in enumerate(lows[:-1])]
    handed = permute_cyclic(out, "section", 1)[None]

    other = (
        axis_bits("ctx")[:1] + axis_bits("dp"),
        axis_bits("dp") + axis_bits("ctx")[:1],
    )
    tail = [bit for _, bit in axis_bits("ctx")[1:]]
    group = lax.axis_size("ctx") * lax.axis_size("dp")
    cols, up_cols, rows = model_width // HD, kv_heads, half // SUB
    units = -(-(rows * (cols + up_cols)) // group)
    a = (units + 1) // 2
    b = units - a
    side = lax.axis_index("section").astype(jnp.int32)
    smem = pl.BlockSpec(memory_space=pltpu.SMEM)
    vmem = pl.BlockSpec(memory_space=pltpu.VMEM)
    any_space = pl.BlockSpec(memory_space=pl.ANY)
    lanes = chunks_of(cols)
    tile_shape = (units * group, SUB, HD)
    keep, send, handed = pl.pallas_call(
        partial(product_kernel, n_recv=len(received), lanes=lanes, up_cols=up_cols),
        in_specs=[smem] + [vmem] * (3 + len(received)) + [pl.BlockSpec(memory_space=pltpu.HBM)] * 2,
        out_specs=[vmem, vmem, any_space],
        out_shape=[
            pltpu.VMEM(tile_shape, bf16),
            pltpu.VMEM(tile_shape, bf16),
            jax.ShapeDtypeStruct(handed.shape, bf16),
        ],
        scratch_shapes=[
            pltpu.VMEM((tok, model_width), bf16),
            pltpu.SemaphoreType.DMA((len(lanes) + 1,)),
        ],
        compiler_params=pltpu.CompilerParams(vmem_limit_bytes=16 << 20),
        name="product",
    )(
        side[None],
        *[in_vmem(x) for x in (lows[-1], *received, own_mask, ups)],
        in_hbm(hidden[0]),
        in_hbm(handed),
    )
    recv = permute_cyclic(send, "section", 1)
    colours = pl.pallas_call(
        merge_kernel,
        in_specs=[vmem, vmem],
        out_specs=[vmem, vmem],
        out_shape=[pltpu.VMEM((n * group, SUB, HD), bf16) for n in (a, b)],
        compiler_params=pltpu.CompilerParams(vmem_limit_bytes=8 << 20),
        name="merge",
    )(in_vmem(keep), in_vmem(recv))
    for k in range(len(other[0])):
        colours = [scatter_stage(colours[c], other[c][k]) for c in range(2)]
    rounds = [tail[k : k + 2] for k in range(0, len(tail), 2)]
    members = group >> len(other[0])
    joined = jnp.concatenate([c.reshape(members, -1, SUB, HD) for c in colours], axis=1)
    for bits in rounds:
        joined = joined.reshape(2 ** len(bits), -1, a + b, SUB, HD)
        joined = direct_scatter(joined, "ctx", bits)
    joined = joined.reshape(a + b, SUB, HD)
    ids = []
    for c in range(2):
        me = jnp.int32(0)
        for stage in other[c]:
            me = me * 2 + bit_of(stage)
        for bits in rounds:
            me = me * 2 ** len(bits) + direct_peers("ctx", bits)[1]
        ids.append(me)
    joined = joined[None]
    for bits in reversed(rounds):
        joined = direct_gather(joined, "ctx", bits).reshape(-1, a + b, SUB, HD)
    colours = [
        joined[:, :a].reshape(-1, SUB, HD),
        joined[:, a:].reshape(-1, SUB, HD),
    ]
    for k in reversed(range(len(other[0]))):
        colours = [gather_stage(colours[c], other[c][k]) for c in range(2)]
    theirs = [permute_cyclic(t, "section", 1) for t in colours]
    shapes = [(group, a, SUB, HD), (group, b, SUB, HD)]
    w, u = pl.pallas_call(
        partial(assemble_kernel, cols=cols, rows=rows),
        in_specs=[smem] + [vmem] * 4,
        out_specs=[any_space, any_space],
        out_shape=[
            jax.ShapeDtypeStruct((width, model_width), f32),
            jax.ShapeDtypeStruct((width, kv_width), f32),
        ],
        scratch_shapes=[
            pltpu.VMEM((width, model_width), f32),
            pltpu.VMEM((width, kv_width), f32),
            pltpu.SemaphoreType.DMA((2 * rows + 1,)),
        ],
        compiler_params=pltpu.CompilerParams(vmem_limit_bytes=16 << 20),
        name="assemble",
    )(
        jnp.stack([side, ids[0], ids[1]]),
        in_vmem(colours[0].reshape(shapes[0])),
        in_vmem(colours[1].reshape(shapes[1])),
        in_vmem(theirs[0].reshape(shapes[0])),
        in_vmem(theirs[1].reshape(shapes[1])),
    )
    down_map_gradient = w.T.reshape(model_width, 2, adapters, rank)
    up_map_gradient = u.reshape(2, adapters, rank, kv_width)
    return (handed, down_map_gradient, up_map_gradient)


def solution(mesh):
    return jax.shard_map(
        step,
        mesh=mesh,
        in_specs=(
            P(("section", "dp"), "ctx", None),
            P(("section", "dp"), "ctx", None),
            P(("section", "dp"), "ctx", None),
            P(("section", "dp"), "ctx", None),
            P(("section", "dp"), "ctx", None),
            P(("section", "dp"), None),
            P(("section", "dp"), None),
            P(),
            P(),
        ),
        out_specs=(P(("section", "dp"), "ctx", None), P(), P()),
        check_vma=False,
    )
```

```python
from functools import partial

import jax
import jax.numpy as jnp
from jax import lax
from jax.experimental import pallas as pl
from jax.experimental.pallas import tpu as pltpu
from jax.sharding import PartitionSpec as P

HD = 128
WINDOW = 1024
SUB = 16
PIECES = 4

query_scale = 168.0 ** (-0.5)
adapter_scale = 0.5
log2e = 1.4426950408889634
rope_base = 10000.0
masked_score = -1e30
f32 = jnp.float32
bf16 = jnp.bfloat16


def permute_by(value, axis, steps):
    count = lax.axis_size(axis)
    first, last = max(0, -steps), min(count, count - steps)
    return lax.ppermute(value, axis, [(i, i + steps) for i in range(first, last)])


def permute_cyclic(value, axis, by):
    count = lax.axis_size(axis)
    return lax.ppermute(value, axis, [(i, (i + by) % count) for i in range(count)])


def permute_xor(value, axis, bit):
    count = lax.axis_size(axis)
    return lax.ppermute(value, axis, [(i, i ^ bit) for i in range(count)])


def window_blocks(own, steps):
    even = lax.axis_index("ctx") % 2 == 0
    chain = [own]
    for _ in range(steps):
        chain.append(permute_by(chain[-1], "ctx", 2))
    blocks = []
    for i in range(steps):
        payload = jnp.where(even, chain[i], chain[i + 1])
        blocks.append(permute_xor(payload, "ctx", 1))
        blocks.append(chain[i + 1])
    return blocks


def doc_index(sequence_lengths, positions):
    doc_ends = jnp.cumsum(sequence_lengths)
    return jnp.sum((doc_ends[None, :] <= positions[:, None]).astype(jnp.int32), axis=1)


def in_hbm(value):
    return pltpu.with_memory_space_constraint(value, pltpu.HBM)


def chunks_of(cols):
    chunk = -(-cols // 6)
    chunk += chunk % 2
    return [slice(c * HD, min(c + chunk, cols) * HD) for c in range(0, cols, chunk)]


def pack_kernel(hidden_hbm, down_hbm, key_hbm, val_hbm, *refs, pieces, heads, lanes):
    messages = refs[:pieces]
    hidden_ref, down_ref, sems = refs[pieces:]
    loads, packs = [], []
    for k, cut in enumerate(lanes):
        loads.append(
            [
                pltpu.make_async_copy(hidden_hbm.at[:, cut], hidden_ref.at[:, cut], sems.at[2 * k]),
                pltpu.make_async_copy(down_hbm.at[:, cut], down_ref.at[:, cut], sems.at[2 * k + 1]),
            ]
        )
    at = 2 * len(lanes)
    for i, message in enumerate(messages):
        cut = slice(i * heads * HD, (i + 1) * heads * HD)
        for j, rows in enumerate((key_hbm, val_hbm)):
            target = message.at[:, j * heads * HD : (j + 1) * heads * HD]
            packs.append(pltpu.make_async_copy(rows.at[:, cut], target, sems.at[at]))
            at += 1
    for pair in loads:
        for load in pair:
            load.start()
    for pack in packs:
        pack.start()
    low = None
    for pair, cut in zip(loads, lanes):
        for load in pair:
            load.wait()
        part = lax.dot_general(
            hidden_ref[:, cut],
            down_ref[:, cut],
            (((1,), (1,)), ((), ())),
            preferred_element_type=f32,
        )
        low = part if low is None else low + part
    messages[0][:, 2 * heads * HD :] = low.astype(bf16)
    for pack in packs:
        pack.wait()


def pack(hidden, down, keys, vals, pieces):
    tok, model_width = hidden.shape
    width = down.shape[0]
    heads = keys.shape[1] // HD // pieces
    lanes = chunks_of(model_width // HD)
    return pl.pallas_call(
        partial(pack_kernel, pieces=pieces, heads=heads, lanes=lanes),
        in_specs=[pl.BlockSpec(memory_space=pltpu.HBM)] * 4,
        out_specs=[pl.BlockSpec(memory_space=pltpu.VMEM)] * pieces,
        out_shape=[
            pltpu.VMEM((tok, 2 * heads * HD + (width if i == 0 else 0)), bf16)
            for i in range(pieces)
        ],
        scratch_shapes=[
            pltpu.VMEM((tok, model_width), bf16),
            pltpu.VMEM((width, model_width), bf16),
            pltpu.SemaphoreType.DMA((2 * len(lanes) + 2 * pieces,)),
        ],
        compiler_params=pltpu.CompilerParams(vmem_limit_bytes=16 << 20),
        name="pack",
    )(in_hbm(hidden), in_hbm(down), in_hbm(keys), in_hbm(vals))


def in_vmem(value):
    return pltpu.with_memory_space_constraint(value, pltpu.VMEM)


def attention_kernel(*refs, n_blocks, piece, heads, tok, group, sub, rank, chained, is_last):
    m_refs = refs[:n_blocks]
    q_ref, up_ref, bias_ref, cos_ref, sin_ref, mask_ref, g_hbm = refs[n_blocks : n_blocks + 7]
    at = n_blocks + 7
    if chained:
        spread_ref, lg_in_ref = refs[at : at + 2]
        at += 4
    out_ref, u_ref = refs[at : at + 2]
    at += 2
    if not is_last:
        lg_ref = refs[at]
        at += 1
    else:
        low_refs = refs[at : at + n_blocks]
        at += n_blocks
    if not chained:
        spread_ref = refs[at]
        at += 1
    if is_last:
        lg_ref = refs[at]
        at += 1
    g_ref, g_sem = refs[at:]
    first_head = piece * heads
    g_lanes = slice(first_head * group * HD, (first_head + heads) * group * HD)
    g_load = pltpu.make_async_copy(g_hbm.at[:, g_lanes], g_ref, g_sem)
    g_load.start()
    if not chained:
        low_lanes = slice(2 * heads * HD, None)
        low = jnp.concatenate([r[:, low_lanes] for r in m_refs], axis=0).astype(f32)
        spread_ref[...] = (low * mask_ref[...]).astype(bf16)
    spread = spread_ref[...]
    span = spread.shape[0]
    half = spread.shape[1] // 2
    cos, sin = cos_ref[...], sin_ref[...]
    dot = partial(lax.dot_general, preferred_element_type=f32)
    last, first = (((1,), (1,)), ((), ())), (((0,), (0,)), ((), ()))
    length = span - tok + sub
    subs = tok // sub

    def lanes_of(query_head):
        at = first_head * group + query_head
        return slice(at * HD, (at + 1) * HD)

    def prepare(h):
        shift = adapter_scale * jnp.dot(spread, up_ref[first_head + h], preferred_element_type=f32)
        kc, vc = slice(h * HD, (h + 1) * HD), slice((heads + h) * HD, (heads + h + 1) * HD)
        key = jnp.concatenate([r[:, kc] for r in m_refs], axis=0).astype(f32) + shift[:, :HD]
        key = (key * cos + pltpu.roll(key, HD // 2, 1) * sin).astype(bf16)
        val = jnp.concatenate([r[:, vc] for r in m_refs], axis=0).astype(f32) + shift[:, HD:]
        return key, val.astype(bf16)

    def scored(h, i, key):
        cut = slice(i * sub, (i + 1) * sub)
        rows = slice(i * sub, i * sub + length)
        cq, sq = cos[span - tok + i * sub : span - tok + (i + 1) * sub], sin[span - tok + i * sub : span - tok + (i + 1) * sub]
        queries = []
        for j in range(group):
            q = q_ref[cut, lanes_of(h * group + j)].astype(f32)
            q = q * cq + pltpu.roll(q, HD // 2, 1) * sq
            queries.append((q * (query_scale * log2e)).astype(bf16))
        q = jnp.concatenate(queries, axis=0)
        bias = jnp.concatenate([bias_ref[rows, cut]] * group, axis=1)
        return q, dot(key[rows], q, last) + bias

    def forward(h, i, scores, val):
        cut = slice(i * sub, (i + 1) * sub)
        rows = slice(i * sub, i * sub + length)
        top = jnp.max(scores, axis=0, keepdims=True)
        probs = jnp.exp2(scores - top)
        scale = 1.0 / jnp.sum(probs, axis=0, keepdims=True)
        low_probs = probs.astype(bf16)
        out_t = (dot(val[rows], low_probs, first) * scale).astype(bf16)
        out = out_t.T
        gs = []
        for j in range(group):
            lanes = lanes_of(h * group + j)
            out_ref[cut, lanes] = out[j * sub : (j + 1) * sub]
            gs.append(g_ref[cut, (h * group + j) * HD : (h * group + j + 1) * HD])
        g_t = (jnp.concatenate(gs, axis=0).T.astype(f32) * scale).astype(bf16)
        drift = jnp.sum(out_t.astype(f32) * g_t.astype(f32), axis=0, keepdims=True)
        dprob = jnp.dot(val[rows], g_t, preferred_element_type=f32)
        return probs, low_probs, g_t, drift, dprob

    def backward(q, state):
        probs, low_probs, g_t, drift, dprob = state
        dscore = (probs * (dprob - drift)).astype(bf16)
        return jnp.dot(dscore, q, preferred_element_type=f32), dot(low_probs, g_t, last)

    def overlapped(parts):
        rows = []
        for j in range(span // sub):
            here = [p[(j - i) * sub : (j - i + 1) * sub] for i, p in enumerate(parts) if 0 <= j - i < length // sub]
            rows.append(sum(here[1:], here[0]))
        return jnp.concatenate(rows, axis=0)

    def finish(h, parts):
        dkey = (1.0 / log2e) * overlapped([p[0] for p in parts])
        dval = overlapped([p[1] for p in parts])
        dkey = dkey * cos - pltpu.roll(dkey, HD // 2, 1) * sin
        both = jnp.concatenate([dkey.astype(bf16), dval.astype(bf16)], axis=1)
        lg = dot(both, up_ref[first_head + h], last)
        if h > 0:
            lg_ref[...] += lg
        else:
            lg_ref[...] = lg_in_ref[...] + lg if chained else lg
        u = adapter_scale * dot(spread, both, first)
        head_lanes = slice((first_head + h) * HD, (first_head + h + 1) * HD)
        u_ref[0, :, head_lanes] = u[:half, :HD].astype(bf16)
        u_ref[1, :, head_lanes] = u[half:, HD:].astype(bf16)

    units = [(h, i) for h in range(heads) for i in range(subs)]
    prepared, scores, states, grads = {}, {}, {}, {}
    for t in range(len(units) + 2):
        if t < len(units):
            h, i = units[t]
            if i == 0:
                prepared[h] = prepare(h)
            scores[h, i] = scored(h, i, prepared[h][0])
        if t == 1:
            g_load.wait()
        if 0 <= t - 1 < len(units):
            h, i = units[t - 1]
            states[h, i] = forward(h, i, scores[h, i][1], prepared[h][1])
        if 0 <= t - 2 < len(units):
            h, i = units[t - 2]
            grads.setdefault(h, []).append(backward(scores[h, i][0], states[h, i]))
            if i == subs - 1:
                finish(h, grads[h])
    if is_last:
        masked = (adapter_scale * lg_ref[...] * mask_ref[...]).astype(bf16)
        compact = dot(picks(2 * half, rank), masked, last)
        for j, ref in enumerate(low_refs):
            ref[...] = compact[:, j * tok : (j + 1) * tok].astype(bf16)


def picks(width, rank):
    row = lax.broadcasted_iota(jnp.int32, (2 * rank, width), 0)
    col = lax.broadcasted_iota(jnp.int32, (2 * rank, width), 1)
    hit = (row // rank == col // (width // 2)) & (row % rank == col % rank)
    return hit.astype(f32).astype(bf16)


def attention(blocks, piece, pieces, carried, mask, q_rows, g_rows, up_cat, bias, cos, sin, rank):
    tok = q_rows.shape[0]
    kv_heads, width, _ = up_cat.shape
    heads = kv_heads // pieces
    group = q_rows.shape[1] // (kv_heads * HD)
    n_blocks = len(blocks)
    span = bias.shape[0]
    half = width // 2
    sub = HD if tok % HD == 0 else tok
    operands = [in_vmem(x) for x in (*blocks, q_rows, up_cat, bias, cos, sin, mask)]
    operands.append(in_hbm(g_rows))
    aliases = {}
    is_last = piece == pieces - 1
    resident = [pl.BlockSpec(memory_space=pltpu.VMEM)]
    in_specs = resident * (len(operands) - 1) + [pl.BlockSpec(memory_space=pltpu.HBM)]
    if carried is not None:
        at = len(operands)
        aliases = {at + 2: 0, at + 3: 1}
        if not is_last:
            aliases[at + 1] = 2
        out, u, lg, spread = carried
        operands += [in_vmem(x) for x in (spread, lg, out, u)]
        in_specs = in_specs + resident * 4
    out_shape = [pltpu.VMEM(q_rows.shape, bf16), pltpu.VMEM((2, half, kv_heads * HD), bf16)]
    scratch = []
    if is_last:
        out_shape += [pltpu.VMEM((2 * rank, tok), bf16)] * n_blocks
        scratch = [pltpu.VMEM((span, width), f32)]
    else:
        out_shape.append(pltpu.VMEM((span, width), f32))
    if carried is None:
        out_shape.append(pltpu.VMEM((span, width), bf16))
    work = heads * group * tok * (span - tok + sub) * HD * 2 * 6
    result = pl.pallas_call(
        partial(
            attention_kernel,
            n_blocks=n_blocks,
            piece=piece,
            heads=heads,
            tok=tok,
            group=group,
            sub=sub,
            rank=rank,
            chained=carried is not None,
            is_last=is_last,
        ),
        in_specs=in_specs,
        out_specs=resident * len(out_shape),
        out_shape=out_shape,
        scratch_shapes=scratch
        + [pltpu.VMEM((tok, heads * group * HD), bf16), pltpu.SemaphoreType.DMA(())],
        input_output_aliases=aliases,
        compiler_params=pltpu.CompilerParams(vmem_limit_bytes=28 << 20),
        cost_estimate=pl.CostEstimate(flops=work, transcendentals=0, bytes_accessed=heads * tok * HD * 20),
        name="attention",
    )(*operands)
    if is_last:
        return result
    return (*result[:3], result[3] if carried is None else spread)


def product_kernel(*refs, n_recv, lanes, up_cols):
    side_ref, own_ref = refs[:2]
    recv = refs[2 : 2 + n_recv]
    mask_ref, up_ref, handed_ref, hidden_hbm = refs[2 + n_recv : 6 + n_recv]
    keep_ref, send_ref, handed_out, hidden_ref, sems = refs[6 + n_recv :]
    loads = [
        pltpu.make_async_copy(hidden_hbm.at[:, cut], hidden_ref.at[:, cut], sems.at[k])
        for k, cut in enumerate(lanes)
    ]
    handing = pltpu.make_async_copy(handed_ref, handed_out, sems.at[len(loads)])
    for load in loads:
        load.start()
    handing.start()
    side = side_ref[0]
    total = own_ref[...].astype(f32)
    for r in recv:
        total = total + r[...].astype(f32)
    width = mask_ref.shape[0]
    half = width // 2
    cols = hidden_ref.shape[1] // HD
    total = lax.dot_general(
        picks(width, total.shape[0] // 2),
        total.astype(bf16),
        (((0,), (0,)), ((), ())),
        preferred_element_type=f32,
    )
    total = total * mask_ref[...]
    swapped = jnp.concatenate([total[half:], total[:half]], axis=0)
    total = jnp.where(side == 0, total, swapped).astype(bf16)
    per_row = cols + up_cols
    rows = half // SUB
    for h in range(up_cols):
        for r in range(rows):
            where = (slice(r * SUB, (r + 1) * SUB), slice(h * HD, (h + 1) * HD))
            keep_ref[r * per_row + cols + h] = up_ref[(side,) + where]
            send_ref[r * per_row + cols + h] = up_ref[(1 - side,) + where]
    used = rows * per_row
    if keep_ref.shape[0] > used:
        rest = keep_ref.shape[0] - used
        keep_ref[pl.ds(used, rest)] = jnp.zeros((rest, SUB, HD), bf16)
        send_ref[pl.ds(used, rest)] = jnp.zeros((rest, SUB, HD), bf16)
    step = 2 if cols % 2 == 0 else 1
    starts = [cut.start // HD for cut in lanes]
    for c in range(0, cols, step):
        if c in starts:
            loads[starts.index(c)].wait()
        w = jnp.dot(
            total, hidden_ref[:, c * HD : (c + step) * HD], preferred_element_type=f32
        ).astype(bf16)
        for j in range(step):
            for r in range(rows):
                tile = w[:, j * HD : (j + 1) * HD]
                keep_ref[r * per_row + c + j] = tile[r * SUB : (r + 1) * SUB]
                send_ref[r * per_row + c + j] = tile[half + r * SUB : half + (r + 1) * SUB]
    handing.wait()


def merge_kernel(keep_ref, recv_ref, *out_refs):
    at = 0
    for ref in out_refs:
        rows = slice(at, at + ref.shape[0])
        ref[...] = (keep_ref[rows].astype(f32) + recv_ref[rows].astype(f32)).astype(bf16)
        at += ref.shape[0]


def assemble_kernel(
    scalars_ref, ma_ref, mb_ref, ra_ref, rb_ref, w_hbm, u_hbm, w_ref, u_ref, sems, *, cols, rows
):
    side, me_a, me_b = scalars_ref[0], scalars_ref[1], scalars_ref[2]
    n_a, a = ma_ref.shape[:2]
    b = mb_ref.shape[1]
    up_cols = u_ref.shape[1] // HD
    per_row = cols + up_cols
    stores = []
    for r in range(rows):
        starts = [pl.multiple_of((m * rows + r) * SUB, SUB) for m in (side, 1 - side)]
        for c in range(per_row):
            t = r * per_row + c
            if t < n_a * a:
                mine, theirs, piece, off = ma_ref, ra_ref, (t // a) ^ me_a, t % a
            else:
                t -= n_a * a
                mine, theirs, piece, off = mb_ref, rb_ref, (t // b) ^ me_b, t % b
            for src, at in zip((mine, theirs), starts):
                tile = src[piece, off].astype(f32)
                if c < cols:
                    w_ref[pl.ds(at, SUB), c * HD : (c + 1) * HD] = tile
                else:
                    u_ref[pl.ds(at, SUB), (c - cols) * HD : (c - cols + 1) * HD] = tile
        for at in starts:
            band = pl.ds(at, SUB)
            stores.append(pltpu.make_async_copy(w_ref.at[band], w_hbm.at[band], sems.at[len(stores)]))
            stores[-1].start()
    stores.append(pltpu.make_async_copy(u_ref, u_hbm, sems.at[len(stores)]))
    stores[-1].start()
    for store in stores:
        store.wait()


def axis_bits(axis):
    bits, bit = [], 1
    while bit < lax.axis_size(axis):
        bits.append((axis, bit))
        bit *= 2
    return bits


def bit_of(stage):
    axis, bit = stage
    return ((lax.axis_index(axis) & bit) != 0).astype(jnp.int32)


def direct_peers(axis, bits):
    masks = [0]
    for bit in bits:
        masks = masks + [m | bit for m in masks]
    me = jnp.int32(0)
    for bit in reversed(bits):
        me = me * 2 + bit_of((axis, bit))
    return masks, me


def direct_scatter(tiles, axis, bits):
    masks, me = direct_peers(axis, bits)
    total = lax.dynamic_index_in_dim(tiles, me, 0, keepdims=False).astype(f32)
    for j in range(1, len(masks)):
        part = lax.dynamic_index_in_dim(tiles, me ^ j, 0, keepdims=False)
        total = total + permute_xor(part, axis, masks[j]).astype(f32)
    return total.astype(bf16)


def direct_gather(tiles, axis, bits):
    masks, _ = direct_peers(axis, bits)
    return jnp.stack([tiles] + [permute_xor(tiles, axis, m) for m in masks[1:]])


def scatter_stage(tiles, stage):
    n = tiles.shape[0] // 2
    bit = bit_of(stage)
    send = lax.dynamic_slice_in_dim(tiles, (1 - bit) * n, n, 0)
    keep = lax.dynamic_slice_in_dim(tiles, bit * n, n, 0)
    recv = permute_xor(send, *stage)
    return (keep.astype(f32) + recv.astype(f32)).astype(bf16)


def gather_stage(tiles, stage):
    return jnp.concatenate([tiles, permute_xor(tiles, *stage)], axis=0)


def step(
    hidden,
    frozen_query_rows,
    frozen_key_rows,
    frozen_value_rows,
    next_output_gradient,
    document_lengths,
    document_adapter,
    adapter_down_maps,
    adapter_up_maps,
):
    tok, model_width = hidden.shape[1:]
    kv_width = frozen_key_rows.shape[2]
    kv_heads = kv_width // HD
    _, adapters, rank, _ = adapter_up_maps.shape
    width = 2 * adapters * rank
    half = width // 2
    ctx_index, ctx_size = lax.axis_index("ctx"), lax.axis_size("ctx")
    longest = tok * ctx_size // 4
    reach = min(-(-(min(WINDOW, longest) - 1) // tok), ctx_size - 1)
    steps = (reach + 1) // 2

    pieces = PIECES if kv_heads % PIECES == 0 else 1
    down = adapter_down_maps.reshape(model_width, width).T
    messages = pack(hidden[0], down, frozen_key_rows[0], frozen_value_rows[0], pieces)
    parts = [window_blocks(m, steps)[::-1] + [m] for m in messages]
    returned = permute_cyclic(next_output_gradient, "section", -1)

    block_starts = jnp.stack([(ctx_index - d) * tok for d in range(2 * steps, -1, -1)])
    key_pos = (block_starts[:, None] + jnp.arange(tok, dtype=jnp.int32)[None, :]).reshape(-1)
    key_docs = doc_index(document_lengths[0], key_pos)
    positions, docs = key_pos[-tok:], key_docs[-tok:]
    picked = key_docs[:, None] == jnp.arange(document_lengths.shape[1], dtype=jnp.int32)[None, :]
    tenant = jnp.sum(picked.astype(jnp.int32) * document_adapter[0][None, :], axis=1)
    lane_adapter = (jnp.arange(width, dtype=jnp.int32) // rank) % adapters
    mask = (tenant[:, None] == lane_adapter[None, :]).astype(f32)
    own_mask = (lane_adapter[:, None] == tenant[None, -tok:]).astype(f32)
    gap = positions[None, :] - key_pos[:, None]
    allowed = (
        (key_docs[:, None] == docs[None, :])
        & (gap >= 0)
        & (gap < WINDOW)
        & (key_pos >= 0)[:, None]
    )
    bias = jnp.where(allowed, 0.0, masked_score).astype(f32)
    frequency = rope_base ** (-(jnp.arange(HD // 2, dtype=f32) * 2.0) / HD)
    angles = key_pos.astype(f32)[:, None] * frequency[None, :]
    cos_half, sin_half = jnp.cos(angles), jnp.sin(angles)
    cos = jnp.concatenate([cos_half, cos_half], axis=1)
    sin = jnp.concatenate([-sin_half, sin_half], axis=1)
    up_flat = adapter_up_maps.reshape(2, half, kv_heads, HD)
    zero = jnp.zeros((kv_heads, half, HD), bf16)
    up_heads = jnp.moveaxis(up_flat, 2, 1)
    up_cat = jnp.concatenate(
        [
            jnp.concatenate([up_heads[0], zero], axis=2),
            jnp.concatenate([zero, up_heads[1]], axis=2),
        ],
        axis=1,
    )

    carried = None
    for i in range(pieces):
        carried = attention(
            parts[i],
            i,
            pieces,
            carried,
            mask,
            frozen_query_rows[0],
            returned[0],
            up_cat,
            bias,
            cos,
            sin,
            rank,
        )
    out, ups = carried[:2]
    lows = carried[2:]
    received = [permute_by(low, "ctx", j - 2 * steps) for j, low in enumerate(lows[:-1])]
    handed = permute_cyclic(out, "section", 1)[None]

    other = (
        axis_bits("ctx")[:1] + axis_bits("dp"),
        axis_bits("dp") + axis_bits("ctx")[:1],
    )
    tail = [bit for _, bit in axis_bits("ctx")[1:]]
    group = lax.axis_size("ctx") * lax.axis_size("dp")
    cols, up_cols, rows = model_width // HD, kv_heads, half // SUB
    units = -(-(rows * (cols + up_cols)) // group)
    a = (units + 1) // 2
    b = units - a
    side = lax.axis_index("section").astype(jnp.int32)
    smem = pl.BlockSpec(memory_space=pltpu.SMEM)
    vmem = pl.BlockSpec(memory_space=pltpu.VMEM)
    any_space = pl.BlockSpec(memory_space=pl.ANY)
    lanes = chunks_of(cols)
    tile_shape = (units * group, SUB, HD)
    keep, send, handed = pl.pallas_call(
        partial(product_kernel, n_recv=len(received), lanes=lanes, up_cols=up_cols),
        in_specs=[smem] + [vmem] * (4 + len(received)) + [pl.BlockSpec(memory_space=pltpu.HBM)],
        out_specs=[vmem, vmem, any_space],
        out_shape=[
            pltpu.VMEM(tile_shape, bf16),
            pltpu.VMEM(tile_shape, bf16),
            jax.ShapeDtypeStruct(handed.shape, bf16),
        ],
        scratch_shapes=[
            pltpu.VMEM((tok, model_width), bf16),
            pltpu.SemaphoreType.DMA((len(lanes) + 1,)),
        ],
        compiler_params=pltpu.CompilerParams(vmem_limit_bytes=16 << 20),
        name="product",
    )(
        side[None],
        *[in_vmem(x) for x in (lows[-1], *received, own_mask, ups, handed)],
        in_hbm(hidden[0]),
    )
    recv = permute_cyclic(send, "section", 1)
    colours = pl.pallas_call(
        merge_kernel,
        in_specs=[vmem, vmem],
        out_specs=[vmem, vmem],
        out_shape=[pltpu.VMEM((n * group, SUB, HD), bf16) for n in (a, b)],
        compiler_params=pltpu.CompilerParams(vmem_limit_bytes=8 << 20),
        name="merge",
    )(in_vmem(keep), in_vmem(recv))
    for k in range(len(other[0])):
        colours = [scatter_stage(colours[c], other[c][k]) for c in range(2)]
    rounds = [tail[k : k + 2] for k in range(0, len(tail), 2)]
    members = group >> len(other[0])
    joined = jnp.concatenate([c.reshape(members, -1, SUB, HD) for c in colours], axis=1)
    for bits in rounds:
        joined = joined.reshape(2 ** len(bits), -1, a + b, SUB, HD)
        joined = direct_scatter(joined, "ctx", bits)
    joined = joined.reshape(a + b, SUB, HD)
    ids = []
    for c in range(2):
        me = jnp.int32(0)
        for stage in other[c]:
            me = me * 2 + bit_of(stage)
        for bits in rounds:
            me = me * 2 ** len(bits) + direct_peers("ctx", bits)[1]
        ids.append(me)
    joined = joined[None]
    for bits in reversed(rounds):
        joined = direct_gather(joined, "ctx", bits).reshape(-1, a + b, SUB, HD)
    colours = [
        joined[:, :a].reshape(-1, SUB, HD),
        joined[:, a:].reshape(-1, SUB, HD),
    ]
    for k in reversed(range(len(other[0]))):
        colours = [gather_stage(colours[c], other[c][k]) for c in range(2)]
    theirs = [permute_cyclic(t, "section", 1) for t in colours]
    shapes = [(group, a, SUB, HD), (group, b, SUB, HD)]
    w, u = pl.pallas_call(
        partial(assemble_kernel, cols=cols, rows=rows),
        in_specs=[smem] + [vmem] * 4,
        out_specs=[any_space, any_space],
        out_shape=[
            jax.ShapeDtypeStruct((width, model_width), f32),
            jax.ShapeDtypeStruct((width, kv_width), f32),
        ],
        scratch_shapes=[
            pltpu.VMEM((width, model_width), f32),
            pltpu.VMEM((width, kv_width), f32),
            pltpu.SemaphoreType.DMA((2 * rows + 1,)),
        ],
        compiler_params=pltpu.CompilerParams(vmem_limit_bytes=16 << 20),
        name="assemble",
    )(
        jnp.stack([side, ids[0], ids[1]]),
        in_vmem(colours[0].reshape(shapes[0])),
        in_vmem(colours[1].reshape(shapes[1])),
        in_vmem(theirs[0].reshape(shapes[0])),
        in_vmem(theirs[1].reshape(shapes[1])),
    )
    down_map_gradient = w.T.reshape(model_width, 2, adapters, rank)
    up_map_gradient = u.reshape(2, adapters, rank, kv_width)
    return (handed, down_map_gradient, up_map_gradient)


def solution(mesh):
    return jax.shard_map(
        step,
        mesh=mesh,
        in_specs=(
            P(("section", "dp"), "ctx", None),
            P(("section", "dp"), "ctx", None),
            P(("section", "dp"), "ctx", None),
            P(("section", "dp"), "ctx", None),
            P(("section", "dp"), "ctx", None),
            P(("section", "dp"), None),
            P(("section", "dp"), None),
            P(),
            P(),
        ),
        out_specs=(P(("section", "dp"), "ctx", None), P(), P()),
        check_vma=False,
    )
```

```python
from functools import partial

import jax
import jax.numpy as jnp
import numpy as np
from jax import lax
from jax.experimental import pallas as pl
from jax.experimental.pallas import tpu as pltpu
from jax.sharding import PartitionSpec as P

HD = 128
WINDOW = 1024
SUB = 16
PIECES = (2, 2, 2, 2)

query_scale = 168.0 ** (-0.5)
adapter_scale = 0.5
log2e = 1.4426950408889634
rope_base = 10000.0
masked_score = -1e30
f32 = jnp.float32
bf16 = jnp.bfloat16


def permute_by(value, axis, steps):
    count = lax.axis_size(axis)
    first, last = max(0, -steps), min(count, count - steps)
    return lax.ppermute(value, axis, [(i, i + steps) for i in range(first, last)])


def permute_cyclic(value, axis, by):
    count = lax.axis_size(axis)
    return lax.ppermute(value, axis, [(i, (i + by) % count) for i in range(count)])


def permute_xor(value, axis, bit):
    count = lax.axis_size(axis)
    return lax.ppermute(value, axis, [(i, i ^ bit) for i in range(count)])


def window_blocks(own, steps, odd):
    chain = [own]
    for _ in range(steps):
        chain.append(permute_by(chain[-1], "ctx", 2))
    blocks = []
    for i in range(steps):
        payload = chosen(odd, chain[i], chain[i + 1])
        blocks.append(permute_xor(payload, "ctx", 1))
        blocks.append(chain[i + 1])
    return blocks


def choose_kernel(second_ref, a_ref, b_ref, out_ref):
    out_ref[...] = jnp.where(second_ref[0] == 0, a_ref[...], b_ref[...])


def chosen(second, a, b):
    resident = pl.BlockSpec(memory_space=pltpu.VMEM)
    return pl.pallas_call(
        choose_kernel,
        in_specs=[pl.BlockSpec(memory_space=pltpu.SMEM), resident, resident],
        out_specs=resident,
        out_shape=pltpu.VMEM(a.shape, a.dtype),
        compiler_params=pltpu.CompilerParams(vmem_limit_bytes=4 << 20),
        name="choose",
    )(second, in_vmem(a), in_vmem(b))


def tables_kernel(
    place_ref, lengths_ref, adapter_ref, freq_ref,
    mask_ref, own_mask_ref, bias_ref, cos_ref, sin_ref, *, adapters, rank,
):
    span, width = mask_ref.shape
    tok = bias_ref.shape[1]
    first = place_ref[1]

    def labels(position):
        docs = jnp.zeros(position.shape, jnp.int32)
        tenants = jnp.full(position.shape, adapter_ref[0, 0], jnp.int32)
        end = jnp.int32(0)
        for i in range(lengths_ref.shape[1]):
            end = end + lengths_ref[0, i]
            past = end <= position
            docs = docs + past.astype(jnp.int32)
            if i + 1 < lengths_ref.shape[1]:
                tenants = jnp.where(past, adapter_ref[0, i + 1], tenants)
        return docs, tenants

    key_pos = first + lax.broadcasted_iota(jnp.int32, (span, HD), 0)
    key_docs, key_tenants = labels(key_pos)
    lane = lax.broadcasted_iota(jnp.int32, (span, HD), 1)
    mask_ref[...] = ((lane // rank) % adapters == key_tenants).astype(f32).astype(bf16)
    pos = first + (span - tok) + lax.broadcasted_iota(jnp.int32, (SUB, tok), 1)
    docs, tenants = labels(pos)
    row = lax.broadcasted_iota(jnp.int32, (width, tok), 0)
    own_mask_ref[...] = ((row // rank) % adapters == tenants[:1]).astype(f32)
    for c in range(0, tok, HD):
        lanes = slice(c, c + HD)
        gap = pos[:1, lanes] - key_pos
        allowed = (key_docs == docs[:1, lanes]) & (gap >= 0) & (gap < WINDOW) & (key_pos >= 0)
        bias_ref[:, lanes] = jnp.where(allowed, 0.0, masked_score)
    angle = key_pos.astype(f32) * freq_ref[...]
    cos_ref[...] = jnp.cos(angle)
    sin = jnp.sin(angle)
    sin_ref[...] = jnp.where(lane < HD // 2, -sin, sin)


def tables(place, lengths, adapter, span, tok, adapters, rank):
    width = 2 * adapters * rank
    half = np.arange(HD // 2, dtype=np.float64) * 2.0 / HD
    freq = np.tile((rope_base ** -half).astype(np.float32), 2)[None]
    smem = pl.BlockSpec(memory_space=pltpu.SMEM)
    resident = pl.BlockSpec(memory_space=pltpu.VMEM)
    return pl.pallas_call(
        partial(tables_kernel, adapters=adapters, rank=rank),
        in_specs=[smem, smem, smem, resident],
        out_specs=[resident] * 5,
        out_shape=[
            pltpu.VMEM((span, width), bf16),
            pltpu.VMEM((width, tok), f32),
            pltpu.VMEM((span, tok), f32),
            pltpu.VMEM((span, HD), f32),
            pltpu.VMEM((span, HD), f32),
        ],
        compiler_params=pltpu.CompilerParams(vmem_limit_bytes=8 << 20),
        name="tables",
    )(place, lengths, adapter, jnp.asarray(freq))


def in_hbm(value):
    return pltpu.with_memory_space_constraint(value, pltpu.HBM)


def chunks_of(cols, parts):
    chunk = -(-cols // parts)
    chunk += chunk % 2
    return [slice(c * HD, min(c + chunk, cols) * HD) for c in range(0, cols, chunk)]


def pack_kernel(place_ref, hidden_hbm, down_hbm, key_hbm, val_hbm, *refs, pieces, lanes):
    messages = refs[: len(pieces)]
    place_out, hidden_ref, down_ref, sems = refs[len(pieces) :]
    place_out[0] = place_ref[0]
    place_out[1] = place_ref[1]
    loads, packs = [], []
    for k, cut in enumerate(lanes):
        loads.append(
            [
                pltpu.make_async_copy(hidden_hbm.at[:, cut], hidden_ref.at[:, cut], sems.at[2 * k]),
                pltpu.make_async_copy(down_hbm.at[:, cut], down_ref.at[:, cut], sems.at[2 * k + 1]),
            ]
        )
    at = 2 * len(lanes)
    begin = 0
    for heads, message in zip(pieces, messages):
        cut = slice(begin * HD, (begin + heads) * HD)
        begin += heads
        for j, rows in enumerate((key_hbm, val_hbm)):
            target = message.at[:, j * heads * HD : (j + 1) * heads * HD]
            packs.append(pltpu.make_async_copy(rows.at[:, cut], target, sems.at[at]))
            at += 1
    for pair in loads:
        for load in pair:
            load.start()
    for pack in packs:
        pack.start()
    low = None
    for pair, cut in zip(loads, lanes):
        for load in pair:
            load.wait()
        part = lax.dot_general(
            hidden_ref[:, cut],
            down_ref[:, cut],
            (((1,), (1,)), ((), ())),
            preferred_element_type=f32,
        )
        low = part if low is None else low + part
    messages[0][:, 2 * pieces[0] * HD :] = low.astype(bf16)
    for pack in packs:
        pack.wait()


def pack(place, hidden, down, keys, vals, pieces):
    tok, model_width = hidden.shape
    width = down.shape[0]
    lanes = chunks_of(model_width // HD, 6)
    *messages, place = pl.pallas_call(
        partial(pack_kernel, pieces=pieces, lanes=lanes),
        in_specs=[pl.BlockSpec(memory_space=pltpu.SMEM)] + [pl.BlockSpec(memory_space=pltpu.HBM)] * 4,
        out_specs=[pl.BlockSpec(memory_space=pltpu.VMEM)] * len(pieces)
        + [pl.BlockSpec(memory_space=pltpu.SMEM)],
        out_shape=[
            pltpu.VMEM((tok, 2 * heads * HD + (width if i == 0 else 0)), bf16)
            for i, heads in enumerate(pieces)
        ]
        + [pltpu.SMEM((2,), jnp.int32)],
        scratch_shapes=[
            pltpu.VMEM((tok, model_width), bf16),
            pltpu.VMEM((width, model_width), bf16),
            pltpu.SemaphoreType.DMA((2 * len(lanes) + 2 * len(pieces),)),
        ],
        compiler_params=pltpu.CompilerParams(vmem_limit_bytes=16 << 20),
        name="pack",
    )(place, in_hbm(hidden), in_hbm(down), in_hbm(keys), in_hbm(vals))
    return messages, place


def in_vmem(value):
    return pltpu.with_memory_space_constraint(value, pltpu.VMEM)


def attention_kernel(*refs, n_blocks, first_head, heads, tok, group, sub, rank, chained, is_last):
    m_refs = refs[:n_blocks]
    q_ref, up_ref, bias_ref, cos_ref, sin_ref, mask_ref, g_hbm = refs[n_blocks : n_blocks + 7]
    at = n_blocks + 7
    if chained:
        spread_ref, lg_in_ref = refs[at : at + 2]
        at += 4
    out_ref, u_ref = refs[at : at + 2]
    at += 2
    if not is_last:
        lg_ref = refs[at]
        at += 1
    else:
        low_refs = refs[at : at + n_blocks]
        at += n_blocks
    if not chained:
        spread_ref = refs[at]
        at += 1
    if is_last:
        lg_ref = refs[at]
        at += 1
    g_ref, g_sem = refs[at:]
    g_lanes = slice(first_head * group * HD, (first_head + heads) * group * HD)
    g_load = pltpu.make_async_copy(g_hbm.at[:, g_lanes], g_ref, g_sem)
    g_load.start()
    if not chained:
        low_lanes = slice(2 * heads * HD, None)
        low = jnp.concatenate([r[:, low_lanes] for r in m_refs], axis=0).astype(f32)
        spread_ref[...] = (low * mask_ref[...].astype(f32)).astype(bf16)
    spread = spread_ref[...]
    span = spread.shape[0]
    half = spread.shape[1] // 2
    cos, sin = cos_ref[...], sin_ref[...]
    dot = partial(lax.dot_general, preferred_element_type=f32)
    last, first = (((1,), (1,)), ((), ())), (((0,), (0,)), ((), ()))
    length = span - tok + sub
    subs = tok // sub

    def lanes_of(query_head):
        at = first_head * group + query_head
        return slice(at * HD, (at + 1) * HD)

    def up_of(h):
        lanes = slice((first_head + h) * HD, (first_head + h + 1) * HD)
        zero = jnp.zeros((up_ref.shape[1], HD), bf16)
        keys = jnp.concatenate([up_ref[0, :, lanes], zero], axis=1)
        vals = jnp.concatenate([zero, up_ref[1, :, lanes]], axis=1)
        return jnp.concatenate([keys, vals], axis=0)

    def prepare(h):
        shift = adapter_scale * jnp.dot(spread, up_of(h), preferred_element_type=f32)
        kc, vc = slice(h * HD, (h + 1) * HD), slice((heads + h) * HD, (heads + h + 1) * HD)
        key = jnp.concatenate([r[:, kc] for r in m_refs], axis=0).astype(f32) + shift[:, :HD]
        key = (key * cos + pltpu.roll(key, HD // 2, 1) * sin).astype(bf16)
        val = jnp.concatenate([r[:, vc] for r in m_refs], axis=0).astype(f32) + shift[:, HD:]
        return key, val.astype(bf16)

    def scored(h, i, key):
        cut = slice(i * sub, (i + 1) * sub)
        rows = slice(i * sub, i * sub + length)
        cq, sq = cos[span - tok + i * sub : span - tok + (i + 1) * sub], sin[span - tok + i * sub : span - tok + (i + 1) * sub]
        queries = []
        for j in range(group):
            q = q_ref[cut, lanes_of(h * group + j)].astype(f32)
            q = q * cq + pltpu.roll(q, HD // 2, 1) * sq
            queries.append((q * (query_scale * log2e)).astype(bf16))
        q = jnp.concatenate(queries, axis=0)
        bias = jnp.concatenate([bias_ref[rows, cut]] * group, axis=1)
        return q, dot(key[rows], q, last) + bias

    def forward(h, i, scores, val):
        cut = slice(i * sub, (i + 1) * sub)
        rows = slice(i * sub, i * sub + length)
        top = jnp.max(scores, axis=0, keepdims=True)
        probs = jnp.exp2(scores - top)
        scale = 1.0 / jnp.sum(probs, axis=0, keepdims=True)
        low_probs = probs.astype(bf16)
        out_t = (dot(val[rows], low_probs, first) * scale).astype(bf16)
        out = out_t.T
        gs = []
        for j in range(group):
            lanes = lanes_of(h * group + j)
            out_ref[cut, lanes] = out[j * sub : (j + 1) * sub]
            gs.append(g_ref[cut, (h * group + j) * HD : (h * group + j + 1) * HD])
        g_t = (jnp.concatenate(gs, axis=0).T.astype(f32) * scale).astype(bf16)
        drift = jnp.sum(out_t.astype(f32) * g_t.astype(f32), axis=0, keepdims=True)
        dprob = jnp.dot(val[rows], g_t, preferred_element_type=f32)
        return probs, low_probs, g_t, drift, dprob

    def backward(q, state):
        probs, low_probs, g_t, drift, dprob = state
        dscore = (probs * (dprob - drift)).astype(bf16)
        return jnp.dot(dscore, q, preferred_element_type=f32), dot(low_probs, g_t, last)

    def overlapped(parts):
        rows = []
        for j in range(span // sub):
            here = [p[(j - i) * sub : (j - i + 1) * sub] for i, p in enumerate(parts) if 0 <= j - i < length // sub]
            rows.append(sum(here[1:], here[0]))
        return jnp.concatenate(rows, axis=0)

    def finish(h, parts):
        dkey = (1.0 / log2e) * overlapped([p[0] for p in parts])
        dval = overlapped([p[1] for p in parts])
        dkey = dkey * cos - pltpu.roll(dkey, HD // 2, 1) * sin
        both = jnp.concatenate([dkey.astype(bf16), dval.astype(bf16)], axis=1)
        lg = dot(both, up_of(h), last)
        if h > 0:
            lg_ref[...] += lg
        else:
            lg_ref[...] = lg_in_ref[...] + lg if chained else lg
        u = adapter_scale * dot(spread, both, first)
        head_lanes = slice((first_head + h) * HD, (first_head + h + 1) * HD)
        u_ref[0, :, head_lanes] = u[:half, :HD].astype(bf16)
        u_ref[1, :, head_lanes] = u[half:, HD:].astype(bf16)

    units = [(h, i) for h in range(heads) for i in range(subs)]
    prepared, scores, states, grads = {}, {}, {}, {}
    for t in range(len(units) + 2):
        if t < len(units):
            h, i = units[t]
            if i == 0:
                prepared[h] = prepare(h)
            scores[h, i] = scored(h, i, prepared[h][0])
        if t == 1:
            g_load.wait()
        if 0 <= t - 1 < len(units):
            h, i = units[t - 1]
            states[h, i] = forward(h, i, scores[h, i][1], prepared[h][1])
        if 0 <= t - 2 < len(units):
            h, i = units[t - 2]
            grads.setdefault(h, []).append(backward(scores[h, i][0], states[h, i]))
            if i == subs - 1:
                finish(h, grads[h])
    if is_last:
        masked = (adapter_scale * lg_ref[...] * mask_ref[...].astype(f32)).astype(bf16)
        compact = dot(picks(2 * half, rank), masked, last)
        for j, ref in enumerate(low_refs):
            ref[...] = compact[:, j * tok : (j + 1) * tok].astype(bf16)


def picks(width, rank):
    row = lax.broadcasted_iota(jnp.int32, (2 * rank, width), 0)
    col = lax.broadcasted_iota(jnp.int32, (2 * rank, width), 1)
    hit = (row // rank == col // (width // 2)) & (row % rank == col % rank)
    return hit.astype(f32).astype(bf16)


def attention(blocks, first_head, heads, carried, is_last, mask, q_rows, g_rows, ups, bias, cos, sin, rank):
    tok = q_rows.shape[0]
    _, half, kv_width = ups.shape
    kv_heads, width = kv_width // HD, 2 * half
    group = q_rows.shape[1] // (kv_heads * HD)
    n_blocks = len(blocks)
    span = bias.shape[0]
    sub = HD if tok % HD == 0 else tok
    operands = [in_vmem(x) for x in (*blocks, q_rows, ups, bias, cos, sin, mask)]
    operands.append(in_hbm(g_rows))
    aliases = {}
    resident = [pl.BlockSpec(memory_space=pltpu.VMEM)]
    in_specs = resident * (len(operands) - 1) + [pl.BlockSpec(memory_space=pltpu.HBM)]
    if carried is not None:
        at = len(operands)
        aliases = {at + 2: 0, at + 3: 1}
        if not is_last:
            aliases[at + 1] = 2
        out, u, lg, spread = carried
        operands += [in_vmem(x) for x in (spread, lg, out, u)]
        in_specs = in_specs + resident * 4
    out_shape = [pltpu.VMEM(q_rows.shape, bf16), pltpu.VMEM((2, half, kv_heads * HD), bf16)]
    scratch = []
    if is_last:
        out_shape += [pltpu.VMEM((2 * rank, tok), bf16)] * n_blocks
        scratch = [pltpu.VMEM((span, width), f32)]
    else:
        out_shape.append(pltpu.VMEM((span, width), f32))
    if carried is None:
        out_shape.append(pltpu.VMEM((span, width), bf16))
    work = heads * group * tok * (span - tok + sub) * HD * 2 * 6
    result = pl.pallas_call(
        partial(
            attention_kernel,
            n_blocks=n_blocks,
            first_head=first_head,
            heads=heads,
            tok=tok,
            group=group,
            sub=sub,
            rank=rank,
            chained=carried is not None,
            is_last=is_last,
        ),
        in_specs=in_specs,
        out_specs=resident * len(out_shape),
        out_shape=out_shape,
        scratch_shapes=scratch
        + [pltpu.VMEM((tok, heads * group * HD), bf16), pltpu.SemaphoreType.DMA(())],
        input_output_aliases=aliases,
        compiler_params=pltpu.CompilerParams(vmem_limit_bytes=28 << 20),
        cost_estimate=pl.CostEstimate(flops=work, transcendentals=0, bytes_accessed=heads * tok * HD * 20),
        name="attention",
    )(*operands)
    if is_last:
        return result
    return (*result[:3], result[3] if carried is None else spread)


def product_kernel(*refs, n_recv, lanes, up_cols):
    side_ref, own_ref = refs[:2]
    recv = refs[2 : 2 + n_recv]
    mask_ref, up_ref, handed_ref, hidden_hbm = refs[2 + n_recv : 6 + n_recv]
    keep_ref, send_ref, handed_out, hidden_ref, sems = refs[6 + n_recv :]
    loads = [
        pltpu.make_async_copy(hidden_hbm.at[:, cut], hidden_ref.at[:, cut], sems.at[k])
        for k, cut in enumerate(lanes)
    ]
    handing = pltpu.make_async_copy(handed_ref, handed_out, sems.at[len(loads)])
    for load in loads:
        load.start()
    handing.start()
    side = side_ref[0]
    total = own_ref[...].astype(f32)
    for r in recv:
        total = total + r[...].astype(f32)
    width = mask_ref.shape[0]
    half = width // 2
    cols = hidden_ref.shape[1] // HD
    total = lax.dot_general(
        picks(width, total.shape[0] // 2),
        total.astype(bf16),
        (((0,), (0,)), ((), ())),
        preferred_element_type=f32,
    )
    total = total * mask_ref[...]
    swapped = jnp.concatenate([total[half:], total[:half]], axis=0)
    total = jnp.where(side == 0, total, swapped).astype(bf16)
    per_row = cols + up_cols
    rows = half // SUB
    for h in range(up_cols):
        for r in range(rows):
            where = (slice(r * SUB, (r + 1) * SUB), slice(h * HD, (h + 1) * HD))
            keep_ref[r * per_row + cols + h] = up_ref[(side,) + where]
            send_ref[r * per_row + cols + h] = up_ref[(1 - side,) + where]
    used = rows * per_row
    if keep_ref.shape[0] > used:
        rest = keep_ref.shape[0] - used
        keep_ref[pl.ds(used, rest)] = jnp.zeros((rest, SUB, HD), bf16)
        send_ref[pl.ds(used, rest)] = jnp.zeros((rest, SUB, HD), bf16)
    step = 2 if cols % 2 == 0 else 1
    starts = [cut.start // HD for cut in lanes]
    for c in range(0, cols, step):
        if c in starts:
            loads[starts.index(c)].wait()
        w = jnp.dot(
            total, hidden_ref[:, c * HD : (c + step) * HD], preferred_element_type=f32
        ).astype(bf16)
        for j in range(step):
            for r in range(rows):
                tile = w[:, j * HD : (j + 1) * HD]
                keep_ref[r * per_row + c + j] = tile[r * SUB : (r + 1) * SUB]
                send_ref[r * per_row + c + j] = tile[half + r * SUB : half + (r + 1) * SUB]
    handing.wait()


def merge_kernel(keep_ref, recv_ref, *out_refs):
    at = 0
    for ref in out_refs:
        rows = slice(at, at + ref.shape[0])
        ref[...] = (keep_ref[rows].astype(f32) + recv_ref[rows].astype(f32)).astype(bf16)
        at += ref.shape[0]


def assemble_kernel(
    scalars_ref, ma_ref, mb_ref, ra_ref, rb_ref, w_hbm, u_hbm, w_ref, u_ref, sems, *, cols, rows
):
    side, me_a, me_b = scalars_ref[0], scalars_ref[1], scalars_ref[2]
    n_a, a = ma_ref.shape[:2]
    b = mb_ref.shape[1]
    up_cols = u_ref.shape[1] // HD
    per_row = cols + up_cols
    stores = []
    for r in range(rows):
        starts = [pl.multiple_of((m * rows + r) * SUB, SUB) for m in (side, 1 - side)]
        for c in range(per_row):
            t = r * per_row + c
            if t < n_a * a:
                mine, theirs, piece, off = ma_ref, ra_ref, (t // a) ^ me_a, t % a
            else:
                t -= n_a * a
                mine, theirs, piece, off = mb_ref, rb_ref, (t // b) ^ me_b, t % b
            for src, at in zip((mine, theirs), starts):
                tile = src[piece, off].astype(f32)
                if c < cols:
                    w_ref[pl.ds(at, SUB), c * HD : (c + 1) * HD] = tile
                else:
                    u_ref[pl.ds(at, SUB), (c - cols) * HD : (c - cols + 1) * HD] = tile
        for at in starts:
            band = pl.ds(at, SUB)
            stores.append(pltpu.make_async_copy(w_ref.at[band], w_hbm.at[band], sems.at[len(stores)]))
            stores[-1].start()
    stores.append(pltpu.make_async_copy(u_ref, u_hbm, sems.at[len(stores)]))
    stores[-1].start()
    for store in stores:
        store.wait()


def axis_bits(axis):
    bits, bit = [], 1
    while bit < lax.axis_size(axis):
        bits.append((axis, bit))
        bit *= 2
    return bits


def bit_of(stage):
    axis, bit = stage
    return ((lax.axis_index(axis) & bit) != 0).astype(jnp.int32)


def direct_peers(axis, bits):
    masks = [0]
    for bit in bits:
        masks = masks + [m | bit for m in masks]
    me = jnp.int32(0)
    for bit in reversed(bits):
        me = me * 2 + bit_of((axis, bit))
    return masks, me


def direct_scatter(tiles, axis, bits):
    masks, me = direct_peers(axis, bits)
    total = lax.dynamic_index_in_dim(tiles, me, 0, keepdims=False).astype(f32)
    for j in range(1, len(masks)):
        part = lax.dynamic_index_in_dim(tiles, me ^ j, 0, keepdims=False)
        total = total + permute_xor(part, axis, masks[j]).astype(f32)
    return total.astype(bf16)


def direct_gather(tiles, axis, bits):
    masks, _ = direct_peers(axis, bits)
    return jnp.stack([tiles] + [permute_xor(tiles, axis, m) for m in masks[1:]])


def scatter_stage(tiles, stage):
    n = tiles.shape[0] // 2
    bit = bit_of(stage)
    send = lax.dynamic_slice_in_dim(tiles, (1 - bit) * n, n, 0)
    keep = lax.dynamic_slice_in_dim(tiles, bit * n, n, 0)
    recv = permute_xor(send, *stage)
    return (keep.astype(f32) + recv.astype(f32)).astype(bf16)


def gather_stage(tiles, stage):
    return jnp.concatenate([tiles, permute_xor(tiles, *stage)], axis=0)


def step(
    hidden,
    frozen_query_rows,
    frozen_key_rows,
    frozen_value_rows,
    next_output_gradient,
    document_lengths,
    document_adapter,
    adapter_down_maps,
    adapter_up_maps,
):
    tok, model_width = hidden.shape[1:]
    kv_width = frozen_key_rows.shape[2]
    kv_heads = kv_width // HD
    _, adapters, rank, _ = adapter_up_maps.shape
    width = 2 * adapters * rank
    half = width // 2
    ctx_index, ctx_size = lax.axis_index("ctx"), lax.axis_size("ctx")
    longest = tok * ctx_size // 4
    reach = min(-(-(min(WINDOW, longest) - 1) // tok), ctx_size - 1)
    steps = (reach + 1) // 2

    pieces = PIECES if sum(PIECES) == kv_heads else (kv_heads,)
    down = adapter_down_maps.reshape(model_width, width).T
    place = jnp.stack([ctx_index % 2, (ctx_index - 2 * steps) * tok]).astype(jnp.int32)
    messages, place = pack(place, hidden[0], down, frozen_key_rows[0], frozen_value_rows[0], pieces)
    parts = [window_blocks(m, steps, place)[::-1] + [m] for m in messages]
    returned = permute_cyclic(next_output_gradient, "section", -1)

    span = (2 * steps + 1) * tok
    mask, own_mask, bias, cos, sin = tables(
        place, document_lengths, document_adapter, span, tok, adapters, rank
    )
    up_rows = adapter_up_maps.reshape(2, half, kv_width)
    carried = None
    for i, heads in enumerate(pieces):
        carried = attention(
            parts[i],
            sum(pieces[:i]),
            heads,
            carried,
            i == len(pieces) - 1,
            mask,
            frozen_query_rows[0],
            returned[0],
            up_rows,
            bias,
            cos,
            sin,
            rank,
        )
    out, ups = carried[:2]
    lows = carried[2:]
    received = [permute_by(low, "ctx", j - 2 * steps) for j, low in enumerate(lows[:-1])]
    handed = permute_cyclic(out, "section", 1)[None]

    other = (
        axis_bits("ctx")[:1] + axis_bits("dp"),
        axis_bits("dp") + axis_bits("ctx")[:1],
    )
    tail = [bit for _, bit in axis_bits("ctx")[1:]]
    group = lax.axis_size("ctx") * lax.axis_size("dp")
    cols, up_cols, rows = model_width // HD, kv_heads, half // SUB
    units = -(-(rows * (cols + up_cols)) // group)
    a = (units + 1) // 2
    b = units - a
    side = lax.axis_index("section").astype(jnp.int32)
    smem = pl.BlockSpec(memory_space=pltpu.SMEM)
    vmem = pl.BlockSpec(memory_space=pltpu.VMEM)
    any_space = pl.BlockSpec(memory_space=pl.ANY)
    lanes = chunks_of(cols, 3)
    tile_shape = (units * group, SUB, HD)
    keep, send, handed = pl.pallas_call(
        partial(product_kernel, n_recv=len(received), lanes=lanes, up_cols=up_cols),
        in_specs=[smem] + [vmem] * (4 + len(received)) + [pl.BlockSpec(memory_space=pltpu.HBM)],
        out_specs=[vmem, vmem, any_space],
        out_shape=[
            pltpu.VMEM(tile_shape, bf16),
            pltpu.VMEM(tile_shape, bf16),
            jax.ShapeDtypeStruct(handed.shape, bf16),
        ],
        scratch_shapes=[
            pltpu.VMEM((tok, model_width), bf16),
            pltpu.SemaphoreType.DMA((len(lanes) + 1,)),
        ],
        compiler_params=pltpu.CompilerParams(vmem_limit_bytes=16 << 20),
        name="product",
    )(
        side[None],
        *[in_vmem(x) for x in (lows[-1], *received, own_mask, ups, handed)],
        in_hbm(hidden[0]),
    )
    recv = permute_cyclic(send, "section", 1)
    colours = pl.pallas_call(
        merge_kernel,
        in_specs=[vmem, vmem],
        out_specs=[vmem, vmem],
        out_shape=[pltpu.VMEM((n * group, SUB, HD), bf16) for n in (a, b)],
        compiler_params=pltpu.CompilerParams(vmem_limit_bytes=8 << 20),
        name="merge",
    )(in_vmem(keep), in_vmem(recv))
    for k in range(len(other[0])):
        colours = [scatter_stage(colours[c], other[c][k]) for c in range(2)]
    rounds = [tail[k : k + 2] for k in range(0, len(tail), 2)]
    members = group >> len(other[0])
    joined = jnp.concatenate([c.reshape(members, -1, SUB, HD) for c in colours], axis=1)
    for bits in rounds:
        joined = joined.reshape(2 ** len(bits), -1, a + b, SUB, HD)
        joined = direct_scatter(joined, "ctx", bits)
    joined = joined.reshape(a + b, SUB, HD)
    ids = []
    for c in range(2):
        me = jnp.int32(0)
        for stage in other[c]:
            me = me * 2 + bit_of(stage)
        for bits in rounds:
            me = me * 2 ** len(bits) + direct_peers("ctx", bits)[1]
        ids.append(me)
    joined = joined[None]
    for bits in reversed(rounds):
        joined = direct_gather(joined, "ctx", bits).reshape(-1, a + b, SUB, HD)
    colours = [
        joined[:, :a].reshape(-1, SUB, HD),
        joined[:, a:].reshape(-1, SUB, HD),
    ]
    for k in reversed(range(len(other[0]))):
        colours = [gather_stage(colours[c], other[c][k]) for c in range(2)]
    theirs = [permute_cyclic(t, "section", 1) for t in colours]
    shapes = [(group, a, SUB, HD), (group, b, SUB, HD)]
    w, u = pl.pallas_call(
        partial(assemble_kernel, cols=cols, rows=rows),
        in_specs=[smem] + [vmem] * 4,
        out_specs=[any_space, any_space],
        out_shape=[
            jax.ShapeDtypeStruct((width, model_width), f32),
            jax.ShapeDtypeStruct((width, kv_width), f32),
        ],
        scratch_shapes=[
            pltpu.VMEM((width, model_width), f32),
            pltpu.VMEM((width, kv_width), f32),
            pltpu.SemaphoreType.DMA((2 * rows + 1,)),
        ],
        compiler_params=pltpu.CompilerParams(vmem_limit_bytes=16 << 20),
        name="assemble",
    )(
        jnp.stack([side, ids[0], ids[1]]),
        in_vmem(colours[0].reshape(shapes[0])),
        in_vmem(colours[1].reshape(shapes[1])),
        in_vmem(theirs[0].reshape(shapes[0])),
        in_vmem(theirs[1].reshape(shapes[1])),
    )
    down_map_gradient = w.T.reshape(model_width, 2, adapters, rank)
    up_map_gradient = u.reshape(2, adapters, rank, kv_width)
    return (handed, down_map_gradient, up_map_gradient)


def solution(mesh):
    return jax.shard_map(
        step,
        mesh=mesh,
        in_specs=(
            P(("section", "dp"), "ctx", None),
            P(("section", "dp"), "ctx", None),
            P(("section", "dp"), "ctx", None),
            P(("section", "dp"), "ctx", None),
            P(("section", "dp"), "ctx", None),
            P(("section", "dp"), None),
            P(("section", "dp"), None),
            P(),
            P(),
        ),
        out_specs=(P(("section", "dp"), "ctx", None), P(), P()),
        check_vma=False,
    )
```

```python
from functools import partial

import jax
import jax.numpy as jnp
import numpy as np
from jax import lax
from jax.experimental import pallas as pl
from jax.experimental.pallas import tpu as pltpu
from jax.sharding import PartitionSpec as P

HD = 128
WINDOW = 1024
SUB = 16
PIECES = (2, 2, 2, 2)

query_scale = 168.0 ** (-0.5)
adapter_scale = 0.5
log2e = 1.4426950408889634
rope_base = 10000.0
masked_score = -1e30
f32 = jnp.float32
bf16 = jnp.bfloat16


def permute_by(value, axis, steps):
    count = lax.axis_size(axis)
    first, last = max(0, -steps), min(count, count - steps)
    return lax.ppermute(value, axis, [(i, i + steps) for i in range(first, last)])


def permute_cyclic(value, axis, by):
    count = lax.axis_size(axis)
    return lax.ppermute(value, axis, [(i, (i + by) % count) for i in range(count)])


def permute_xor(value, axis, bit):
    count = lax.axis_size(axis)
    return lax.ppermute(value, axis, [(i, i ^ bit) for i in range(count)])


def window_blocks(own, steps, odd):
    chain = [own]
    for _ in range(steps):
        chain.append(permute_by(chain[-1], "ctx", 2))
    blocks = []
    for i in range(steps):
        payload = chosen(odd, chain[i], chain[i + 1])
        blocks.append(permute_xor(payload, "ctx", 1))
        blocks.append(chain[i + 1])
    return blocks


def choose_kernel(second_ref, a_ref, b_ref, out_ref):
    out_ref[...] = jnp.where(second_ref[0] == 0, a_ref[...], b_ref[...])


def chosen(second, a, b):
    resident = pl.BlockSpec(memory_space=pltpu.VMEM)
    return pl.pallas_call(
        choose_kernel,
        in_specs=[pl.BlockSpec(memory_space=pltpu.SMEM), resident, resident],
        out_specs=resident,
        out_shape=pltpu.VMEM(a.shape, a.dtype),
        compiler_params=pltpu.CompilerParams(vmem_limit_bytes=4 << 20),
        name="choose",
    )(second, in_vmem(a), in_vmem(b))


def tables_kernel(
    place_ref, lengths_ref, adapter_ref, freq_ref,
    mask_ref, own_mask_ref, bias_ref, cos_ref, sin_ref, *, adapters, rank,
):
    span, width = mask_ref.shape
    tok = bias_ref.shape[1]
    first = place_ref[1]

    def labels(position):
        docs = jnp.zeros(position.shape, jnp.int32)
        tenants = jnp.full(position.shape, adapter_ref[0, 0], jnp.int32)
        end = jnp.int32(0)
        for i in range(lengths_ref.shape[1]):
            end = end + lengths_ref[0, i]
            past = end <= position
            docs = docs + past.astype(jnp.int32)
            if i + 1 < lengths_ref.shape[1]:
                tenants = jnp.where(past, adapter_ref[0, i + 1], tenants)
        return docs, tenants

    key_pos = first + lax.broadcasted_iota(jnp.int32, (span, HD), 0)
    key_docs, key_tenants = labels(key_pos)
    lane = lax.broadcasted_iota(jnp.int32, (span, HD), 1)
    mask_ref[...] = ((lane // rank) % adapters == key_tenants).astype(f32).astype(bf16)
    pos = first + (span - tok) + lax.broadcasted_iota(jnp.int32, (SUB, tok), 1)
    docs, tenants = labels(pos)
    row = lax.broadcasted_iota(jnp.int32, (width, tok), 0)
    own_mask_ref[...] = ((row // rank) % adapters == tenants[:1]).astype(f32)
    for c in range(0, tok, HD):
        lanes = slice(c, c + HD)
        gap = pos[:1, lanes] - key_pos
        allowed = (key_docs == docs[:1, lanes]) & (gap >= 0) & (gap < WINDOW) & (key_pos >= 0)
        bias_ref[:, lanes] = jnp.where(allowed, 0.0, masked_score)
    angle = key_pos.astype(f32) * freq_ref[...]
    cos_ref[...] = jnp.cos(angle)
    sin = jnp.sin(angle)
    sin_ref[...] = jnp.where(lane < HD // 2, -sin, sin)


def tables(place, lengths, adapter, span, tok, adapters, rank):
    width = 2 * adapters * rank
    half = np.arange(HD // 2, dtype=np.float64) * 2.0 / HD
    freq = np.tile((rope_base ** -half).astype(np.float32), 2)[None]
    smem = pl.BlockSpec(memory_space=pltpu.SMEM)
    resident = pl.BlockSpec(memory_space=pltpu.VMEM)
    return pl.pallas_call(
        partial(tables_kernel, adapters=adapters, rank=rank),
        in_specs=[smem, smem, smem, resident],
        out_specs=[resident] * 5,
        out_shape=[
            pltpu.VMEM((span, width), bf16),
            pltpu.VMEM((width, tok), f32),
            pltpu.VMEM((span, tok), f32),
            pltpu.VMEM((span, HD), f32),
            pltpu.VMEM((span, HD), f32),
        ],
        compiler_params=pltpu.CompilerParams(vmem_limit_bytes=8 << 20),
        name="tables",
    )(place, lengths, adapter, jnp.asarray(freq))


def in_hbm(value):
    return pltpu.with_memory_space_constraint(value, pltpu.HBM)


def chunks_of(cols, parts):
    chunk = -(-cols // parts)
    chunk += chunk % 2
    return [slice(c * HD, min(c + chunk, cols) * HD) for c in range(0, cols, chunk)]


def pack_kernel(place_ref, hidden_hbm, down_hbm, key_hbm, val_hbm, *refs, pieces, lanes):
    messages = refs[: len(pieces)]
    place_out, hidden_ref, down_ref, sems = refs[len(pieces) :]
    place_out[0] = place_ref[0]
    place_out[1] = place_ref[1]
    loads, packs = [], []
    for k, cut in enumerate(lanes):
        loads.append(
            [
                pltpu.make_async_copy(hidden_hbm.at[:, cut], hidden_ref.at[:, cut], sems.at[2 * k]),
                pltpu.make_async_copy(down_hbm.at[:, cut], down_ref.at[:, cut], sems.at[2 * k + 1]),
            ]
        )
    at = 2 * len(lanes)
    begin = 0
    for heads, message in zip(pieces, messages):
        cut = slice(begin * HD, (begin + heads) * HD)
        begin += heads
        for j, rows in enumerate((key_hbm, val_hbm)):
            target = message.at[:, j * heads * HD : (j + 1) * heads * HD]
            packs.append(pltpu.make_async_copy(rows.at[:, cut], target, sems.at[at]))
            at += 1
    for pair in loads:
        for load in pair:
            load.start()
    for pack in packs:
        pack.start()
    low = None
    for pair, cut in zip(loads, lanes):
        for load in pair:
            load.wait()
        part = lax.dot_general(
            hidden_ref[:, cut],
            down_ref[:, cut],
            (((1,), (1,)), ((), ())),
            preferred_element_type=f32,
        )
        low = part if low is None else low + part
    messages[0][:, 2 * pieces[0] * HD :] = low.astype(bf16)
    for pack in packs:
        pack.wait()


def pack(place, hidden, down, keys, vals, pieces):
    tok, model_width = hidden.shape
    width = down.shape[0]
    lanes = chunks_of(model_width // HD, 6)
    *messages, place = pl.pallas_call(
        partial(pack_kernel, pieces=pieces, lanes=lanes),
        in_specs=[pl.BlockSpec(memory_space=pltpu.SMEM)] + [pl.BlockSpec(memory_space=pltpu.HBM)] * 4,
        out_specs=[pl.BlockSpec(memory_space=pltpu.VMEM)] * len(pieces)
        + [pl.BlockSpec(memory_space=pltpu.SMEM)],
        out_shape=[
            pltpu.VMEM((tok, 2 * heads * HD + (width if i == 0 else 0)), bf16)
            for i, heads in enumerate(pieces)
        ]
        + [pltpu.SMEM((2,), jnp.int32)],
        scratch_shapes=[
            pltpu.VMEM((tok, model_width), bf16),
            pltpu.VMEM((width, model_width), bf16),
            pltpu.SemaphoreType.DMA((2 * len(lanes) + 2 * len(pieces),)),
        ],
        compiler_params=pltpu.CompilerParams(vmem_limit_bytes=16 << 20),
        name="pack",
    )(place, in_hbm(hidden), in_hbm(down), in_hbm(keys), in_hbm(vals))
    return messages, place


def in_vmem(value):
    return pltpu.with_memory_space_constraint(value, pltpu.VMEM)


def attention_kernel(*refs, n_blocks, first_head, heads, tok, group, sub, rank, chained, is_last):
    m_refs = refs[:n_blocks]
    q_ref, up_ref, bias_ref, cos_ref, sin_ref, mask_ref, g_hbm = refs[n_blocks : n_blocks + 7]
    at = n_blocks + 7
    if chained:
        spread_ref, lg_in_ref = refs[at : at + 2]
        at += 4
    out_ref, u_ref = refs[at : at + 2]
    at += 2
    if not is_last:
        lg_ref = refs[at]
        at += 1
    else:
        low_refs = refs[at : at + n_blocks]
        at += n_blocks
    if not chained:
        spread_ref = refs[at]
        at += 1
    if is_last:
        lg_ref = refs[at]
        at += 1
    g_ref, g_sem = refs[at:]
    g_lanes = slice(first_head * group * HD, (first_head + heads) * group * HD)
    g_load = pltpu.make_async_copy(g_hbm.at[:, g_lanes], g_ref, g_sem)
    g_load.start()
    if not chained:
        low_lanes = slice(2 * heads * HD, None)
        low = jnp.concatenate([r[:, low_lanes] for r in m_refs], axis=0).astype(f32)
        spread_ref[...] = (low * mask_ref[...].astype(f32)).astype(bf16)
    spread = spread_ref[...]
    span = spread.shape[0]
    half = spread.shape[1] // 2
    cos, sin = cos_ref[...], sin_ref[...]
    dot = partial(lax.dot_general, preferred_element_type=f32)
    last, first = (((1,), (1,)), ((), ())), (((0,), (0,)), ((), ()))
    length = span - tok + sub
    subs = tok // sub

    def lanes_of(query_head):
        at = first_head * group + query_head
        return slice(at * HD, (at + 1) * HD)

    def up_of(h):
        lanes = slice((first_head + h) * HD, (first_head + h + 1) * HD)
        zero = jnp.zeros((up_ref.shape[1], HD), bf16)
        keys = jnp.concatenate([up_ref[0, :, lanes], zero], axis=1)
        vals = jnp.concatenate([zero, up_ref[1, :, lanes]], axis=1)
        return jnp.concatenate([keys, vals], axis=0)

    def prepare(h):
        shift = adapter_scale * jnp.dot(spread, up_of(h), preferred_element_type=f32)
        kc, vc = slice(h * HD, (h + 1) * HD), slice((heads + h) * HD, (heads + h + 1) * HD)
        key = jnp.concatenate([r[:, kc] for r in m_refs], axis=0).astype(f32) + shift[:, :HD]
        key = (key * cos + pltpu.roll(key, HD // 2, 1) * sin).astype(bf16)
        val = jnp.concatenate([r[:, vc] for r in m_refs], axis=0).astype(f32) + shift[:, HD:]
        return key, val.astype(bf16)

    def scored(h, i, key):
        cut = slice(i * sub, (i + 1) * sub)
        rows = slice(i * sub, i * sub + length)
        cq, sq = cos[span - tok + i * sub : span - tok + (i + 1) * sub], sin[span - tok + i * sub : span - tok + (i + 1) * sub]
        queries = []
        for j in range(group):
            q = q_ref[cut, lanes_of(h * group + j)].astype(f32)
            q = q * cq + pltpu.roll(q, HD // 2, 1) * sq
            queries.append((q * (query_scale * log2e)).astype(bf16))
        q = jnp.concatenate(queries, axis=0)
        bias = jnp.concatenate([bias_ref[rows, cut]] * group, axis=1)
        return q, dot(key[rows], q, last) + bias

    def forward(h, i, scores, val):
        cut = slice(i * sub, (i + 1) * sub)
        rows = slice(i * sub, i * sub + length)
        top = jnp.max(scores, axis=0, keepdims=True)
        probs = jnp.exp2(scores - top)
        scale = 1.0 / jnp.sum(probs, axis=0, keepdims=True)
        low_probs = probs.astype(bf16)
        out_t = (dot(val[rows], low_probs, first) * scale).astype(bf16)
        out = out_t.T
        gs = []
        for j in range(group):
            lanes = lanes_of(h * group + j)
            out_ref[cut, lanes] = out[j * sub : (j + 1) * sub]
            gs.append(g_ref[cut, (h * group + j) * HD : (h * group + j + 1) * HD])
        g_t = (jnp.concatenate(gs, axis=0).T.astype(f32) * scale).astype(bf16)
        drift = jnp.sum(out_t.astype(f32) * g_t.astype(f32), axis=0, keepdims=True)
        dprob = jnp.dot(val[rows], g_t, preferred_element_type=f32)
        return probs, low_probs, g_t, drift, dprob

    def backward(q, state):
        probs, low_probs, g_t, drift, dprob = state
        dscore = (probs * (dprob - drift)).astype(bf16)
        return jnp.dot(dscore, q, preferred_element_type=f32), dot(low_probs, g_t, last)

    def overlapped(parts):
        rows = []
        for j in range(span // sub):
            here = [p[(j - i) * sub : (j - i + 1) * sub] for i, p in enumerate(parts) if 0 <= j - i < length // sub]
            rows.append(sum(here[1:], here[0]))
        return jnp.concatenate(rows, axis=0)

    def finish(h, parts):
        dkey = (1.0 / log2e) * overlapped([p[0] for p in parts])
        dval = overlapped([p[1] for p in parts])
        dkey = dkey * cos - pltpu.roll(dkey, HD // 2, 1) * sin
        both = jnp.concatenate([dkey.astype(bf16), dval.astype(bf16)], axis=1)
        lg = dot(both, up_of(h), last)
        if h > 0:
            lg_ref[...] += lg
        else:
            lg_ref[...] = lg_in_ref[...] + lg if chained else lg
        u = adapter_scale * dot(spread, both, first)
        head_lanes = slice((first_head + h) * HD, (first_head + h + 1) * HD)
        u_ref[0, :, head_lanes] = u[:half, :HD].astype(bf16)
        u_ref[1, :, head_lanes] = u[half:, HD:].astype(bf16)

    units = [(h, i) for h in range(heads) for i in range(subs)]
    prepared, scores, states, grads = {}, {}, {}, {}
    for t in range(len(units) + 2):
        if t < len(units):
            h, i = units[t]
            if i == 0:
                prepared[h] = prepare(h)
            scores[h, i] = scored(h, i, prepared[h][0])
        if t == 1:
            g_load.wait()
        if 0 <= t - 1 < len(units):
            h, i = units[t - 1]
            states[h, i] = forward(h, i, scores[h, i][1], prepared[h][1])
        if 0 <= t - 2 < len(units):
            h, i = units[t - 2]
            grads.setdefault(h, []).append(backward(scores[h, i][0], states[h, i]))
            if i == subs - 1:
                finish(h, grads[h])
    if is_last:
        masked = (adapter_scale * lg_ref[...] * mask_ref[...].astype(f32)).astype(bf16)
        compact = dot(picks(2 * half, rank), masked, last)
        for j, ref in enumerate(low_refs):
            ref[...] = compact[:, j * tok : (j + 1) * tok].astype(bf16)


def picks(width, rank):
    row = lax.broadcasted_iota(jnp.int32, (2 * rank, width), 0)
    col = lax.broadcasted_iota(jnp.int32, (2 * rank, width), 1)
    hit = (row // rank == col // (width // 2)) & (row % rank == col % rank)
    return hit.astype(f32).astype(bf16)


def attention(blocks, first_head, heads, carried, is_last, mask, q_rows, g_rows, ups, bias, cos, sin, rank):
    tok = q_rows.shape[0]
    _, half, kv_width = ups.shape
    kv_heads, width = kv_width // HD, 2 * half
    group = q_rows.shape[1] // (kv_heads * HD)
    n_blocks = len(blocks)
    span = bias.shape[0]
    sub = HD if tok % HD == 0 else tok
    operands = [in_vmem(x) for x in (*blocks, q_rows, ups, bias, cos, sin, mask)]
    operands.append(in_hbm(g_rows))
    aliases = {}
    resident = [pl.BlockSpec(memory_space=pltpu.VMEM)]
    in_specs = resident * (len(operands) - 1) + [pl.BlockSpec(memory_space=pltpu.HBM)]
    if carried is not None:
        at = len(operands)
        aliases = {at + 2: 0, at + 3: 1}
        if not is_last:
            aliases[at + 1] = 2
        out, u, lg, spread = carried
        operands += [in_vmem(x) for x in (spread, lg, out, u)]
        in_specs = in_specs + resident * 4
    out_shape = [pltpu.VMEM(q_rows.shape, bf16), pltpu.VMEM((2, half, kv_heads * HD), bf16)]
    scratch = []
    if is_last:
        out_shape += [pltpu.VMEM((2 * rank, tok), bf16)] * n_blocks
        scratch = [pltpu.VMEM((span, width), f32)]
    else:
        out_shape.append(pltpu.VMEM((span, width), f32))
    if carried is None:
        out_shape.append(pltpu.VMEM((span, width), bf16))
    work = heads * group * tok * (span - tok + sub) * HD * 2 * 6
    result = pl.pallas_call(
        partial(
            attention_kernel,
            n_blocks=n_blocks,
            first_head=first_head,
            heads=heads,
            tok=tok,
            group=group,
            sub=sub,
            rank=rank,
            chained=carried is not None,
            is_last=is_last,
        ),
        in_specs=in_specs,
        out_specs=resident * len(out_shape),
        out_shape=out_shape,
        scratch_shapes=scratch
        + [pltpu.VMEM((tok, heads * group * HD), bf16), pltpu.SemaphoreType.DMA(())],
        input_output_aliases=aliases,
        compiler_params=pltpu.CompilerParams(vmem_limit_bytes=28 << 20),
        cost_estimate=pl.CostEstimate(flops=work, transcendentals=0, bytes_accessed=heads * tok * HD * 20),
        name="attention",
    )(*operands)
    if is_last:
        return result
    return (*result[:3], result[3] if carried is None else spread)


def product_kernel(*refs, n_recv, lanes, up_cols):
    side_ref, own_ref = refs[:2]
    recv = refs[2 : 2 + n_recv]
    mask_ref, up_ref, handed_ref, hidden_hbm = refs[2 + n_recv : 6 + n_recv]
    keep_ref, send_ref, handed_out, hidden_ref, sems = refs[6 + n_recv :]
    loads = [
        pltpu.make_async_copy(hidden_hbm.at[:, cut], hidden_ref.at[:, cut], sems.at[k])
        for k, cut in enumerate(lanes)
    ]
    handing = pltpu.make_async_copy(handed_ref, handed_out, sems.at[len(loads)])
    for load in loads:
        load.start()
    handing.start()
    side = side_ref[0]
    total = own_ref[...].astype(f32)
    for r in recv:
        total = total + r[...].astype(f32)
    width = mask_ref.shape[0]
    half = width // 2
    cols = hidden_ref.shape[1] // HD
    total = lax.dot_general(
        picks(width, total.shape[0] // 2),
        total.astype(bf16),
        (((0,), (0,)), ((), ())),
        preferred_element_type=f32,
    )
    total = total * mask_ref[...]
    swapped = jnp.concatenate([total[half:], total[:half]], axis=0)
    total = jnp.where(side == 0, total, swapped).astype(bf16)
    per_row = cols + up_cols
    rows = half // SUB
    for h in range(up_cols):
        for r in range(rows):
            where = (slice(r * SUB, (r + 1) * SUB), slice(h * HD, (h + 1) * HD))
            keep_ref[r * per_row + cols + h] = up_ref[(side,) + where]
            send_ref[r * per_row + cols + h] = up_ref[(1 - side,) + where]
    used = rows * per_row
    if keep_ref.shape[0] > used:
        rest = keep_ref.shape[0] - used
        keep_ref[pl.ds(used, rest)] = jnp.zeros((rest, SUB, HD), bf16)
        send_ref[pl.ds(used, rest)] = jnp.zeros((rest, SUB, HD), bf16)
    step = 2 if cols % 2 == 0 else 1
    starts = [cut.start // HD for cut in lanes]
    for c in range(0, cols, step):
        if c in starts:
            loads[starts.index(c)].wait()
        w = jnp.dot(
            total, hidden_ref[:, c * HD : (c + step) * HD], preferred_element_type=f32
        ).astype(bf16)
        for j in range(step):
            for r in range(rows):
                tile = w[:, j * HD : (j + 1) * HD]
                keep_ref[r * per_row + c + j] = tile[r * SUB : (r + 1) * SUB]
                send_ref[r * per_row + c + j] = tile[half + r * SUB : half + (r + 1) * SUB]
    handing.wait()


def merge_kernel(keep_ref, recv_ref, out_ref):
    out_ref[...] = (keep_ref[...].astype(f32) + recv_ref[...].astype(f32)).astype(bf16)


def assemble_kernel(scalars_ref, tiles_ref, *refs, cols, rows, own):
    w_hbm, u_hbm, w_ref, u_ref, sems = refs[-5:]
    side, me = scalars_ref[0], scalars_ref[1]
    half = side if own else 1 - side
    units = tiles_ref.shape[1]
    up_cols = u_ref.shape[1] // HD
    per_row = cols + up_cols
    stores = []
    for r in range(rows):
        at = slice(r * SUB, (r + 1) * SUB)
        for c in range(per_row):
            t = r * per_row + c
            tile = tiles_ref[(t // units) ^ me, t % units].astype(f32)
            if c < cols:
                w_ref[at, c * HD : (c + 1) * HD] = tile
            else:
                u_ref[at, (c - cols) * HD : (c - cols + 1) * HD] = tile
        band = pl.ds(pl.multiple_of((half * rows + r) * SUB, SUB), SUB)
        for src, dst in ((w_ref, w_hbm), (u_ref, u_hbm)):
            stores.append(pltpu.make_async_copy(src.at[at], dst.at[band], sems.at[len(stores)]))
            stores[-1].start()
    for store in stores:
        store.wait()


def assemble(scalars, tiles, before, width, model_width, kv_width):
    rows = width // 2 // SUB
    hbm = pl.BlockSpec(memory_space=pltpu.HBM)
    carried = [] if before is None else [in_hbm(x) for x in before]
    shapes = [(width, model_width), (width, kv_width)]
    return pl.pallas_call(
        partial(assemble_kernel, cols=model_width // HD, rows=rows, own=before is None),
        in_specs=[
            pl.BlockSpec(memory_space=pltpu.SMEM),
            pl.BlockSpec(memory_space=pltpu.VMEM),
            *[hbm for _ in carried],
        ],
        out_specs=[hbm, hbm],
        out_shape=[jax.ShapeDtypeStruct(shape, f32) for shape in shapes],
        scratch_shapes=[
            pltpu.VMEM((width // 2, model_width), f32),
            pltpu.VMEM((width // 2, kv_width), f32),
            pltpu.SemaphoreType.DMA((2 * rows,)),
        ],
        input_output_aliases={2 + i: i for i in range(len(carried))},
        compiler_params=pltpu.CompilerParams(vmem_limit_bytes=16 << 20),
        name="assemble",
    )(scalars, in_vmem(tiles), *carried)


def axis_bits(axis):
    bits, bit = [], 1
    while bit < lax.axis_size(axis):
        bits.append((axis, bit))
        bit *= 2
    return bits


def bit_of(stage):
    axis, bit = stage
    return ((lax.axis_index(axis) & bit) != 0).astype(jnp.int32)


def permute_masked(value, masks):
    axes = tuple(masks)
    sizes = [lax.axis_size(axis) for axis in axes]
    pairs = []
    for i in range(int(np.prod(sizes))):
        index = np.unravel_index(i, sizes)
        pairs.append((i, int(np.ravel_multi_index([k ^ masks[x] for k, x in zip(index, axes)], sizes))))
    return lax.ppermute(value, axes if len(axes) > 1 else axes[0], pairs)


def direct_peers(stages):
    masks = [{axis: 0 for axis, _ in stages}]
    for axis, bit in stages:
        masks = masks + [{**m, axis: m[axis] | bit} for m in masks]
    me = jnp.int32(0)
    for stage in reversed(stages):
        me = me * 2 + bit_of(stage)
    return masks, me


def direct_scatter(tiles, stages):
    masks, me = direct_peers(stages)
    total = lax.dynamic_index_in_dim(tiles, me, 0, keepdims=False).astype(f32)
    for j in range(1, len(masks)):
        part = lax.dynamic_index_in_dim(tiles, me ^ j, 0, keepdims=False)
        total = total + permute_masked(part, masks[j]).astype(f32)
    return total.astype(bf16)


def direct_gather(tiles, stages):
    masks, _ = direct_peers(stages)
    return jnp.stack([tiles] + [permute_masked(tiles, m) for m in masks[1:]])


def step(
    hidden,
    frozen_query_rows,
    frozen_key_rows,
    frozen_value_rows,
    next_output_gradient,
    document_lengths,
    document_adapter,
    adapter_down_maps,
    adapter_up_maps,
):
    tok, model_width = hidden.shape[1:]
    kv_width = frozen_key_rows.shape[2]
    kv_heads = kv_width // HD
    _, adapters, rank, _ = adapter_up_maps.shape
    width = 2 * adapters * rank
    half = width // 2
    ctx_index, ctx_size = lax.axis_index("ctx"), lax.axis_size("ctx")
    longest = tok * ctx_size // 4
    reach = min(-(-(min(WINDOW, longest) - 1) // tok), ctx_size - 1)
    steps = (reach + 1) // 2

    pieces = PIECES if sum(PIECES) == kv_heads else (kv_heads,)
    down = adapter_down_maps.reshape(model_width, width).T
    place = jnp.stack([ctx_index % 2, (ctx_index - 2 * steps) * tok]).astype(jnp.int32)
    messages, place = pack(place, hidden[0], down, frozen_key_rows[0], frozen_value_rows[0], pieces)
    parts = [window_blocks(m, steps, place)[::-1] + [m] for m in messages]
    returned = permute_cyclic(next_output_gradient, "section", -1)

    span = (2 * steps + 1) * tok
    mask, own_mask, bias, cos, sin = tables(
        place, document_lengths, document_adapter, span, tok, adapters, rank
    )
    up_rows = adapter_up_maps.reshape(2, half, kv_width)
    carried = None
    for i, heads in enumerate(pieces):
        carried = attention(
            parts[i],
            sum(pieces[:i]),
            heads,
            carried,
            i == len(pieces) - 1,
            mask,
            frozen_query_rows[0],
            returned[0],
            up_rows,
            bias,
            cos,
            sin,
            rank,
        )
    out, ups = carried[:2]
    lows = carried[2:]
    received = [permute_by(low, "ctx", j - 2 * steps) for j, low in enumerate(lows[:-1])]
    handed = permute_cyclic(out, "section", 1)[None]

    rest = axis_bits("ctx")[1:]
    rounds = [axis_bits("ctx")[:1] + axis_bits("dp")]
    rounds += [rest[k : k + 2] for k in range(0, len(rest), 2)]
    group = lax.axis_size("ctx") * lax.axis_size("dp")
    cols, up_cols, rows = model_width // HD, kv_heads, half // SUB
    units = -(-(rows * (cols + up_cols)) // group)
    side = lax.axis_index("section").astype(jnp.int32)
    smem = pl.BlockSpec(memory_space=pltpu.SMEM)
    vmem = pl.BlockSpec(memory_space=pltpu.VMEM)
    any_space = pl.BlockSpec(memory_space=pl.ANY)
    lanes = chunks_of(cols, 3)
    tile_shape = (units * group, SUB, HD)
    keep, send, handed = pl.pallas_call(
        partial(product_kernel, n_recv=len(received), lanes=lanes, up_cols=up_cols),
        in_specs=[smem] + [vmem] * (4 + len(received)) + [pl.BlockSpec(memory_space=pltpu.HBM)],
        out_specs=[vmem, vmem, any_space],
        out_shape=[
            pltpu.VMEM(tile_shape, bf16),
            pltpu.VMEM(tile_shape, bf16),
            jax.ShapeDtypeStruct(handed.shape, bf16),
        ],
        scratch_shapes=[
            pltpu.VMEM((tok, model_width), bf16),
            pltpu.SemaphoreType.DMA((len(lanes) + 1,)),
        ],
        compiler_params=pltpu.CompilerParams(vmem_limit_bytes=16 << 20),
        name="product",
    )(
        side[None],
        *[in_vmem(x) for x in (lows[-1], *received, own_mask, ups, handed)],
        in_hbm(hidden[0]),
    )
    recv = permute_cyclic(send, "section", 1)
    tiles = pl.pallas_call(
        merge_kernel,
        in_specs=[vmem, vmem],
        out_specs=vmem,
        out_shape=pltpu.VMEM(tile_shape, bf16),
        compiler_params=pltpu.CompilerParams(vmem_limit_bytes=8 << 20),
        name="merge",
    )(in_vmem(keep), in_vmem(recv))
    me = jnp.int32(0)
    for stages in rounds:
        tiles = direct_scatter(tiles.reshape(2 ** len(stages), -1, SUB, HD), stages)
        me = me * 2 ** len(stages) + direct_peers(stages)[1]
    for stages in reversed(rounds):
        tiles = direct_gather(tiles, stages).reshape(-1, SUB, HD)
    theirs = permute_cyclic(tiles, "section", 1)
    scalars = jnp.stack([side, me])
    outs = None
    for part in (tiles, theirs):
        part = part.reshape(group, units, SUB, HD)
        outs = assemble(scalars, part, outs, width, model_width, kv_width)
    w, u = outs
    down_map_gradient = w.T.reshape(model_width, 2, adapters, rank)
    up_map_gradient = u.reshape(2, adapters, rank, kv_width)
    return (handed, down_map_gradient, up_map_gradient)


def solution(mesh):
    return jax.shard_map(
        step,
        mesh=mesh,
        in_specs=(
            P(("section", "dp"), "ctx", None),
            P(("section", "dp"), "ctx", None),
            P(("section", "dp"), "ctx", None),
            P(("section", "dp"), "ctx", None),
            P(("section", "dp"), "ctx", None),
            P(("section", "dp"), None),
            P(("section", "dp"), None),
            P(),
            P(),
        ),
        out_specs=(P(("section", "dp"), "ctx", None), P(), P()),
        check_vma=False,
    )
```

```python
from functools import partial

import jax
import jax.numpy as jnp
import numpy as np
from jax import lax
from jax.experimental import pallas as pl
from jax.experimental.pallas import tpu as pltpu
from jax.sharding import PartitionSpec as P

HD = 128
WINDOW = 1024
SUB = 16
PIECES = (2, 2, 2, 2)

query_scale = 168.0 ** (-0.5)
adapter_scale = 0.5
log2e = 1.4426950408889634
rope_base = 10000.0
masked_score = -1e30
f32 = jnp.float32
bf16 = jnp.bfloat16


def permute_by(value, axis, steps):
    count = lax.axis_size(axis)
    first, last = max(0, -steps), min(count, count - steps)
    return lax.ppermute(value, axis, [(i, i + steps) for i in range(first, last)])


def permute_cyclic(value, axis, by):
    count = lax.axis_size(axis)
    return lax.ppermute(value, axis, [(i, (i + by) % count) for i in range(count)])


def permute_xor(value, axis, bit):
    count = lax.axis_size(axis)
    return lax.ppermute(value, axis, [(i, i ^ bit) for i in range(count)])


def window_blocks(own, steps, odd):
    chain = [own]
    for _ in range(steps):
        chain.append(permute_by(chain[-1], "ctx", 2))
    blocks = []
    for i in range(steps):
        payload = chosen(odd, chain[i], chain[i + 1])
        blocks.append(permute_xor(payload, "ctx", 1))
        blocks.append(chain[i + 1])
    return blocks


def choose_kernel(second_ref, a_ref, b_ref, out_ref):
    out_ref[...] = jnp.where(second_ref[0] == 0, a_ref[...], b_ref[...])


def chosen(second, a, b):
    resident = pl.BlockSpec(memory_space=pltpu.VMEM)
    return pl.pallas_call(
        choose_kernel,
        in_specs=[pl.BlockSpec(memory_space=pltpu.SMEM), resident, resident],
        out_specs=resident,
        out_shape=pltpu.VMEM(a.shape, a.dtype),
        compiler_params=pltpu.CompilerParams(vmem_limit_bytes=4 << 20),
        name="choose",
    )(second, in_vmem(a), in_vmem(b))


def tables_kernel(
    place_ref, lengths_ref, adapter_ref, freq_ref,
    mask_ref, own_mask_ref, bias_ref, cos_ref, sin_ref, *, adapters, rank,
):
    span, width = mask_ref.shape
    tok = bias_ref.shape[1]
    first = place_ref[1]

    def labels(position):
        label = jnp.full(position.shape, adapter_ref[0, 0], jnp.int32)
        end = jnp.int32(0)
        for i in range(lengths_ref.shape[1] - 1):
            end = end + lengths_ref[0, i]
            label = jnp.where(end <= position, 64 * (i + 1) + adapter_ref[0, i + 1], label)
        return label

    key_pos = first + lax.broadcasted_iota(jnp.int32, (span, HD), 0)
    key_label = labels(key_pos)
    lane = lax.broadcasted_iota(jnp.int32, (1, HD), 1)
    mask_ref[...] = ((lane // rank) % adapters == (key_label & 63)).astype(f32).astype(bf16)
    pos = first + (span - tok) + lax.broadcasted_iota(jnp.int32, (SUB, tok), 1)
    label = labels(pos)[:1]
    row = lax.broadcasted_iota(jnp.int32, (width, tok), 0)
    own_mask_ref[...] = ((row // rank) % adapters == (label & 63)).astype(f32)
    for c in range(0, tok, HD):
        lanes = slice(c, c + HD)
        gap = pos[:1, lanes] - key_pos
        allowed = (key_label == label[:, lanes]) & (gap >= 0) & (gap < WINDOW) & (key_pos >= 0)
        bias_ref[:, lanes] = jnp.where(allowed, 0.0, masked_score)
    size = next(n for n in (32, 16, 8, 1) if span % n == 0)
    groups = span // size
    padded = -(-groups // 8) * 8
    freq = freq_ref[...]
    outer = (first + size * lax.broadcasted_iota(jnp.int32, (padded, HD), 0)).astype(f32) * freq
    inner = lax.broadcasted_iota(jnp.int32, (size, HD), 0).astype(f32) * freq
    cos_o, sin_o, cos_i, sin_i = jnp.cos(outer), jnp.sin(outer), jnp.cos(inner), jnp.sin(inner)
    sign = jnp.where(lane < HD // 2, -1.0, 1.0)
    for k in range(groups):
        rows = slice(k * size, (k + 1) * size)
        c, s = cos_o[k : k + 1], sin_o[k : k + 1]
        cos_ref[rows] = c * cos_i - s * sin_i
        sin_ref[rows] = (sign * s) * cos_i + (sign * c) * sin_i


def tables(place, lengths, adapter, span, tok, adapters, rank):
    width = 2 * adapters * rank
    half = np.arange(HD // 2, dtype=np.float64) * 2.0 / HD
    freq = np.tile((rope_base ** -half).astype(np.float32), 2)[None]
    smem = pl.BlockSpec(memory_space=pltpu.SMEM)
    resident = pl.BlockSpec(memory_space=pltpu.VMEM)
    return pl.pallas_call(
        partial(tables_kernel, adapters=adapters, rank=rank),
        in_specs=[smem, smem, smem, resident],
        out_specs=[resident] * 5,
        out_shape=[
            pltpu.VMEM((span, width), bf16),
            pltpu.VMEM((width, tok), f32),
            pltpu.VMEM((span, tok), f32),
            pltpu.VMEM((span, HD), f32),
            pltpu.VMEM((span, HD), f32),
        ],
        compiler_params=pltpu.CompilerParams(vmem_limit_bytes=8 << 20),
        name="tables",
    )(place, lengths, adapter, jnp.asarray(freq))


def in_hbm(value):
    return pltpu.with_memory_space_constraint(value, pltpu.HBM)


def chunks_of(cols, parts):
    chunk = -(-cols // parts)
    chunk += chunk % 2
    return [slice(c * HD, min(c + chunk, cols) * HD) for c in range(0, cols, chunk)]


def pack_kernel(place_ref, hidden_hbm, down_hbm, key_hbm, val_hbm, *refs, pieces, lanes):
    messages = refs[: len(pieces)]
    place_out, hidden_ref, down_ref, sems = refs[len(pieces) :]
    place_out[0] = place_ref[0]
    place_out[1] = place_ref[1]
    loads, packs = [], []
    for k, cut in enumerate(lanes):
        loads.append(
            [
                pltpu.make_async_copy(hidden_hbm.at[:, cut], hidden_ref.at[:, cut], sems.at[2 * k]),
                pltpu.make_async_copy(down_hbm.at[:, cut], down_ref.at[:, cut], sems.at[2 * k + 1]),
            ]
        )
    at = 2 * len(lanes)
    begin = 0
    for heads, message in zip(pieces, messages):
        cut = slice(begin * HD, (begin + heads) * HD)
        begin += heads
        for j, rows in enumerate((key_hbm, val_hbm)):
            target = message.at[:, j * heads * HD : (j + 1) * heads * HD]
            packs.append(pltpu.make_async_copy(rows.at[:, cut], target, sems.at[at]))
            at += 1
    for pair in loads:
        for load in pair:
            load.start()
    for pack in packs:
        pack.start()
    low = None
    for pair, cut in zip(loads, lanes):
        for load in pair:
            load.wait()
        part = lax.dot_general(
            hidden_ref[:, cut],
            down_ref[:, cut],
            (((1,), (1,)), ((), ())),
            preferred_element_type=f32,
        )
        low = part if low is None else low + part
    messages[0][:, 2 * pieces[0] * HD :] = low.astype(bf16)
    for pack in packs:
        pack.wait()


def pack(place, hidden, down, keys, vals, pieces):
    tok, model_width = hidden.shape
    width = down.shape[0]
    lanes = chunks_of(model_width // HD, 6)
    *messages, place = pl.pallas_call(
        partial(pack_kernel, pieces=pieces, lanes=lanes),
        in_specs=[pl.BlockSpec(memory_space=pltpu.SMEM)] + [pl.BlockSpec(memory_space=pltpu.HBM)] * 4,
        out_specs=[pl.BlockSpec(memory_space=pltpu.VMEM)] * len(pieces)
        + [pl.BlockSpec(memory_space=pltpu.SMEM)],
        out_shape=[
            pltpu.VMEM((tok, 2 * heads * HD + (width if i == 0 else 0)), bf16)
            for i, heads in enumerate(pieces)
        ]
        + [pltpu.SMEM((2,), jnp.int32)],
        scratch_shapes=[
            pltpu.VMEM((tok, model_width), bf16),
            pltpu.VMEM((width, model_width), bf16),
            pltpu.SemaphoreType.DMA((2 * len(lanes) + 2 * len(pieces),)),
        ],
        compiler_params=pltpu.CompilerParams(vmem_limit_bytes=16 << 20),
        name="pack",
    )(place, in_hbm(hidden), in_hbm(down), in_hbm(keys), in_hbm(vals))
    return messages, place


def in_vmem(value):
    return pltpu.with_memory_space_constraint(value, pltpu.VMEM)


def attention_kernel(*refs, n_blocks, first_head, heads, tok, group, sub, rank, chained, is_last):
    m_refs = refs[:n_blocks]
    q_ref, up_ref, bias_ref, cos_ref, sin_ref, mask_ref, g_hbm = refs[n_blocks : n_blocks + 7]
    at = n_blocks + 7
    if chained:
        spread_ref, lg_in_ref = refs[at : at + 2]
        at += 4
    out_ref, u_ref = refs[at : at + 2]
    at += 2
    if not is_last:
        lg_ref = refs[at]
        at += 1
    else:
        low_refs = refs[at : at + n_blocks]
        at += n_blocks
    if not chained:
        spread_ref = refs[at]
        at += 1
    if is_last:
        lg_ref = refs[at]
        at += 1
    g_ref, g_sem = refs[at:]
    g_lanes = slice(first_head * group * HD, (first_head + heads) * group * HD)
    g_load = pltpu.make_async_copy(g_hbm.at[:, g_lanes], g_ref, g_sem)
    g_load.start()
    if not chained:
        low_lanes = slice(2 * heads * HD, None)
        low = jnp.concatenate([r[:, low_lanes] for r in m_refs], axis=0).astype(f32)
        spread_ref[...] = (low * mask_ref[...].astype(f32)).astype(bf16)
    spread = spread_ref[...]
    span = spread.shape[0]
    half = spread.shape[1] // 2
    cos, sin = cos_ref[...], sin_ref[...]
    dot = partial(lax.dot_general, preferred_element_type=f32)
    last, first = (((1,), (1,)), ((), ())), (((0,), (0,)), ((), ()))
    length = span - tok + sub
    subs = tok // sub

    def lanes_of(query_head):
        at = first_head * group + query_head
        return slice(at * HD, (at + 1) * HD)

    def up_of(h):
        lanes = slice((first_head + h) * HD, (first_head + h + 1) * HD)
        zero = jnp.zeros((up_ref.shape[1], HD), bf16)
        keys = jnp.concatenate([up_ref[0, :, lanes], zero], axis=1)
        vals = jnp.concatenate([zero, up_ref[1, :, lanes]], axis=1)
        return jnp.concatenate([keys, vals], axis=0)

    def prepare(h):
        shift = adapter_scale * jnp.dot(spread, up_of(h), preferred_element_type=f32)
        kc, vc = slice(h * HD, (h + 1) * HD), slice((heads + h) * HD, (heads + h + 1) * HD)
        key = jnp.concatenate([r[:, kc] for r in m_refs], axis=0).astype(f32) + shift[:, :HD]
        key = (key * cos + pltpu.roll(key, HD // 2, 1) * sin).astype(bf16)
        val = jnp.concatenate([r[:, vc] for r in m_refs], axis=0).astype(f32) + shift[:, HD:]
        return key, val.astype(bf16)

    def scored(h, i, key):
        cut = slice(i * sub, (i + 1) * sub)
        rows = slice(i * sub, i * sub + length)
        cq, sq = cos[span - tok + i * sub : span - tok + (i + 1) * sub], sin[span - tok + i * sub : span - tok + (i + 1) * sub]
        queries = []
        for j in range(group):
            q = q_ref[cut, lanes_of(h * group + j)].astype(f32)
            q = q * cq + pltpu.roll(q, HD // 2, 1) * sq
            queries.append((q * (query_scale * log2e)).astype(bf16))
        q = jnp.concatenate(queries, axis=0)
        bias = jnp.concatenate([bias_ref[rows, cut]] * group, axis=1)
        return q, dot(key[rows], q, last) + bias

    def forward(h, i, scores, val):
        cut = slice(i * sub, (i + 1) * sub)
        rows = slice(i * sub, i * sub + length)
        top = jnp.max(scores, axis=0, keepdims=True)
        probs = jnp.exp2(scores - top)
        scale = 1.0 / jnp.sum(probs, axis=0, keepdims=True)
        low_probs = probs.astype(bf16)
        out_t = (dot(val[rows], low_probs, first) * scale).astype(bf16)
        out = out_t.T
        gs = []
        for j in range(group):
            lanes = lanes_of(h * group + j)
            out_ref[cut, lanes] = out[j * sub : (j + 1) * sub]
            gs.append(g_ref[cut, (h * group + j) * HD : (h * group + j + 1) * HD])
        g_t = (jnp.concatenate(gs, axis=0).T.astype(f32) * scale).astype(bf16)
        drift = jnp.sum(out_t.astype(f32) * g_t.astype(f32), axis=0, keepdims=True)
        dprob = jnp.dot(val[rows], g_t, preferred_element_type=f32)
        return probs, low_probs, g_t, drift, dprob

    def backward(q, state):
        probs, low_probs, g_t, drift, dprob = state
        dscore = (probs * (dprob - drift)).astype(bf16)
        return jnp.dot(dscore, q, preferred_element_type=f32), dot(low_probs, g_t, last)

    def overlapped(parts):
        rows = []
        for j in range(span // sub):
            here = [p[(j - i) * sub : (j - i + 1) * sub] for i, p in enumerate(parts) if 0 <= j - i < length // sub]
            rows.append(sum(here[1:], here[0]))
        return jnp.concatenate(rows, axis=0)

    def finish(h, parts):
        dkey = (1.0 / log2e) * overlapped([p[0] for p in parts])
        dval = overlapped([p[1] for p in parts])
        dkey = dkey * cos - pltpu.roll(dkey, HD // 2, 1) * sin
        both = jnp.concatenate([dkey.astype(bf16), dval.astype(bf16)], axis=1)
        lg = dot(both, up_of(h), last)
        if h > 0:
            lg_ref[...] += lg
        else:
            lg_ref[...] = lg_in_ref[...] + lg if chained else lg
        u = adapter_scale * dot(spread, both, first)
        head_lanes = slice((first_head + h) * HD, (first_head + h + 1) * HD)
        u_ref[0, :, head_lanes] = u[:half, :HD].astype(bf16)
        u_ref[1, :, head_lanes] = u[half:, HD:].astype(bf16)

    units = [(h, i) for h in range(heads) for i in range(subs)]
    prepared, scores, states, grads = {}, {}, {}, {}
    for t in range(len(units) + 2):
        if t < len(units):
            h, i = units[t]
            if i == 0:
                prepared[h] = prepare(h)
            scores[h, i] = scored(h, i, prepared[h][0])
        if t == 1:
            g_load.wait()
        if 0 <= t - 1 < len(units):
            h, i = units[t - 1]
            states[h, i] = forward(h, i, scores[h, i][1], prepared[h][1])
        if 0 <= t - 2 < len(units):
            h, i = units[t - 2]
            grads.setdefault(h, []).append(backward(scores[h, i][0], states[h, i]))
            if i == subs - 1:
                finish(h, grads[h])
    if is_last:
        masked = (adapter_scale * lg_ref[...] * mask_ref[...].astype(f32)).astype(bf16)
        compact = dot(picks(2 * half, rank), masked, last)
        for j, ref in enumerate(low_refs):
            ref[...] = compact[:, j * tok : (j + 1) * tok].astype(bf16)


def picks(width, rank):
    row = lax.broadcasted_iota(jnp.int32, (2 * rank, width), 0)
    col = lax.broadcasted_iota(jnp.int32, (2 * rank, width), 1)
    hit = (row // rank == col // (width // 2)) & (row % rank == col % rank)
    return hit.astype(f32).astype(bf16)


def attention(blocks, first_head, heads, carried, is_last, mask, q_rows, g_rows, ups, bias, cos, sin, rank):
    tok = q_rows.shape[0]
    _, half, kv_width = ups.shape
    kv_heads, width = kv_width // HD, 2 * half
    group = q_rows.shape[1] // (kv_heads * HD)
    n_blocks = len(blocks)
    span = bias.shape[0]
    sub = HD if tok % HD == 0 else tok
    operands = [in_vmem(x) for x in (*blocks, q_rows, ups, bias, cos, sin, mask)]
    operands.append(in_hbm(g_rows))
    aliases = {}
    resident = [pl.BlockSpec(memory_space=pltpu.VMEM)]
    in_specs = resident * (len(operands) - 1) + [pl.BlockSpec(memory_space=pltpu.HBM)]
    if carried is not None:
        at = len(operands)
        aliases = {at + 2: 0, at + 3: 1}
        if not is_last:
            aliases[at + 1] = 2
        out, u, lg, spread = carried
        operands += [in_vmem(x) for x in (spread, lg, out, u)]
        in_specs = in_specs + resident * 4
    out_shape = [pltpu.VMEM(q_rows.shape, bf16), pltpu.VMEM((2, half, kv_heads * HD), bf16)]
    scratch = []
    if is_last:
        out_shape += [pltpu.VMEM((2 * rank, tok), bf16)] * n_blocks
        scratch = [pltpu.VMEM((span, width), f32)]
    else:
        out_shape.append(pltpu.VMEM((span, width), f32))
    if carried is None:
        out_shape.append(pltpu.VMEM((span, width), bf16))
    work = heads * group * tok * (span - tok + sub) * HD * 2 * 6
    result = pl.pallas_call(
        partial(
            attention_kernel,
            n_blocks=n_blocks,
            first_head=first_head,
            heads=heads,
            tok=tok,
            group=group,
            sub=sub,
            rank=rank,
            chained=carried is not None,
            is_last=is_last,
        ),
        in_specs=in_specs,
        out_specs=resident * len(out_shape),
        out_shape=out_shape,
        scratch_shapes=scratch
        + [pltpu.VMEM((tok, heads * group * HD), bf16), pltpu.SemaphoreType.DMA(())],
        input_output_aliases=aliases,
        compiler_params=pltpu.CompilerParams(vmem_limit_bytes=28 << 20),
        cost_estimate=pl.CostEstimate(flops=work, transcendentals=0, bytes_accessed=heads * tok * HD * 20),
        name="attention",
    )(*operands)
    if is_last:
        return result
    return (*result[:3], result[3] if carried is None else spread)


def product_kernel(*refs, n_recv, lanes, up_cols):
    side_ref, own_ref = refs[:2]
    recv = refs[2 : 2 + n_recv]
    mask_ref, up_ref, handed_ref, hidden_hbm = refs[2 + n_recv : 6 + n_recv]
    keep_ref, send_ref, handed_out, hidden_ref, sems = refs[6 + n_recv :]
    loads = [
        pltpu.make_async_copy(hidden_hbm.at[:, cut], hidden_ref.at[:, cut], sems.at[k])
        for k, cut in enumerate(lanes)
    ]
    handing = pltpu.make_async_copy(handed_ref, handed_out, sems.at[len(loads)])
    for load in loads:
        load.start()
    handing.start()
    side = side_ref[0]
    total = own_ref[...].astype(f32)
    for r in recv:
        total = total + r[...].astype(f32)
    width = mask_ref.shape[0]
    half = width // 2
    cols = hidden_ref.shape[1] // HD
    total = lax.dot_general(
        picks(width, total.shape[0] // 2),
        total.astype(bf16),
        (((0,), (0,)), ((), ())),
        preferred_element_type=f32,
    )
    total = total * mask_ref[...]
    swapped = jnp.concatenate([total[half:], total[:half]], axis=0)
    total = jnp.where(side == 0, total, swapped).astype(bf16)
    per_row = cols + up_cols
    rows = half // SUB
    for h in range(up_cols):
        for r in range(rows):
            where = (slice(r * SUB, (r + 1) * SUB), slice(h * HD, (h + 1) * HD))
            keep_ref[r * per_row + cols + h] = up_ref[(side,) + where]
            send_ref[r * per_row + cols + h] = up_ref[(1 - side,) + where]
    used = rows * per_row
    if keep_ref.shape[0] > used:
        rest = keep_ref.shape[0] - used
        keep_ref[pl.ds(used, rest)] = jnp.zeros((rest, SUB, HD), bf16)
        send_ref[pl.ds(used, rest)] = jnp.zeros((rest, SUB, HD), bf16)
    step = 2 if cols % 2 == 0 else 1
    starts = [cut.start // HD for cut in lanes]
    for c in range(0, cols, step):
        if c in starts:
            loads[starts.index(c)].wait()
        w = jnp.dot(
            total, hidden_ref[:, c * HD : (c + step) * HD], preferred_element_type=f32
        ).astype(bf16)
        for j in range(step):
            for r in range(rows):
                tile = w[:, j * HD : (j + 1) * HD]
                keep_ref[r * per_row + c + j] = tile[r * SUB : (r + 1) * SUB]
                send_ref[r * per_row + c + j] = tile[half + r * SUB : half + (r + 1) * SUB]
    handing.wait()


def merge_kernel(keep_ref, recv_ref, out_ref):
    out_ref[...] = (keep_ref[...].astype(f32) + recv_ref[...].astype(f32)).astype(bf16)


def assemble_kernel(scalars_ref, tiles_ref, *refs, cols, rows, own):
    w_hbm, u_hbm, w_ref, u_ref, sems = refs[-5:]
    side, me = scalars_ref[0], scalars_ref[1]
    half = side if own else 1 - side
    units = tiles_ref.shape[1]
    up_cols = u_ref.shape[1] // HD
    per_row = cols + up_cols
    stores = []
    for r in range(rows):
        at = slice(r * SUB, (r + 1) * SUB)
        for c in range(per_row):
            t = r * per_row + c
            tile = tiles_ref[(t // units) ^ me, t % units].astype(f32)
            if c < cols:
                w_ref[at, c * HD : (c + 1) * HD] = tile
            else:
                u_ref[at, (c - cols) * HD : (c - cols + 1) * HD] = tile
        band = pl.ds(pl.multiple_of((half * rows + r) * SUB, SUB), SUB)
        for src, dst in ((w_ref, w_hbm), (u_ref, u_hbm)):
            stores.append(pltpu.make_async_copy(src.at[at], dst.at[band], sems.at[len(stores)]))
            stores[-1].start()
    for store in stores:
        store.wait()


def assemble(scalars, tiles, before, width, model_width, kv_width):
    rows = width // 2 // SUB
    hbm = pl.BlockSpec(memory_space=pltpu.HBM)
    carried = [] if before is None else [in_hbm(x) for x in before]
    shapes = [(width, model_width), (width, kv_width)]
    return pl.pallas_call(
        partial(assemble_kernel, cols=model_width // HD, rows=rows, own=before is None),
        in_specs=[
            pl.BlockSpec(memory_space=pltpu.SMEM),
            pl.BlockSpec(memory_space=pltpu.VMEM),
            *[hbm for _ in carried],
        ],
        out_specs=[hbm, hbm],
        out_shape=[jax.ShapeDtypeStruct(shape, f32) for shape in shapes],
        scratch_shapes=[
            pltpu.VMEM((width // 2, model_width), f32),
            pltpu.VMEM((width // 2, kv_width), f32),
            pltpu.SemaphoreType.DMA((2 * rows,)),
        ],
        input_output_aliases={2 + i: i for i in range(len(carried))},
        compiler_params=pltpu.CompilerParams(vmem_limit_bytes=16 << 20),
        name="assemble",
    )(scalars, in_vmem(tiles), *carried)


def axis_bits(axis):
    bits, bit = [], 1
    while bit < lax.axis_size(axis):
        bits.append((axis, bit))
        bit *= 2
    return bits


def bit_of(stage):
    axis, bit = stage
    return ((lax.axis_index(axis) & bit) != 0).astype(jnp.int32)


def permute_masked(value, masks):
    axes = tuple(masks)
    sizes = [lax.axis_size(axis) for axis in axes]
    pairs = []
    for i in range(int(np.prod(sizes))):
        index = np.unravel_index(i, sizes)
        pairs.append((i, int(np.ravel_multi_index([k ^ masks[x] for k, x in zip(index, axes)], sizes))))
    return lax.ppermute(value, axes if len(axes) > 1 else axes[0], pairs)


def direct_peers(stages):
    masks = [{axis: 0 for axis, _ in stages}]
    for axis, bit in stages:
        masks = masks + [{**m, axis: m[axis] | bit} for m in masks]
    me = jnp.int32(0)
    for stage in reversed(stages):
        me = me * 2 + bit_of(stage)
    return masks, me


def direct_scatter(tiles, stages):
    masks, me = direct_peers(stages)
    total = lax.dynamic_index_in_dim(tiles, me, 0, keepdims=False).astype(f32)
    for j in range(1, len(masks)):
        part = lax.dynamic_index_in_dim(tiles, me ^ j, 0, keepdims=False)
        total = total + permute_masked(part, masks[j]).astype(f32)
    return total.astype(bf16)


def direct_gather(tiles, stages):
    masks, _ = direct_peers(stages)
    return jnp.stack([tiles] + [permute_masked(tiles, m) for m in masks[1:]])


def step(
    hidden,
    frozen_query_rows,
    frozen_key_rows,
    frozen_value_rows,
    next_output_gradient,
    document_lengths,
    document_adapter,
    adapter_down_maps,
    adapter_up_maps,
):
    tok, model_width = hidden.shape[1:]
    kv_width = frozen_key_rows.shape[2]
    kv_heads = kv_width // HD
    _, adapters, rank, _ = adapter_up_maps.shape
    width = 2 * adapters * rank
    half = width // 2
    ctx_index, ctx_size = lax.axis_index("ctx"), lax.axis_size("ctx")
    longest = tok * ctx_size // 4
    reach = min(-(-(min(WINDOW, longest) - 1) // tok), ctx_size - 1)
    steps = (reach + 1) // 2

    pieces = PIECES if sum(PIECES) == kv_heads else (kv_heads,)
    down = adapter_down_maps.reshape(model_width, width).T
    place = jnp.stack([ctx_index % 2, (ctx_index - 2 * steps) * tok]).astype(jnp.int32)
    messages, place = pack(place, hidden[0], down, frozen_key_rows[0], frozen_value_rows[0], pieces)
    parts = [window_blocks(m, steps, place)[::-1] + [m] for m in messages]
    returned = permute_cyclic(next_output_gradient, "section", -1)

    span = (2 * steps + 1) * tok
    mask, own_mask, bias, cos, sin = tables(
        place, document_lengths, document_adapter, span, tok, adapters, rank
    )
    up_rows = adapter_up_maps.reshape(2, half, kv_width)
    carried = None
    for i, heads in enumerate(pieces):
        carried = attention(
            parts[i],
            sum(pieces[:i]),
            heads,
            carried,
            i == len(pieces) - 1,
            mask,
            frozen_query_rows[0],
            returned[0],
            up_rows,
            bias,
            cos,
            sin,
            rank,
        )
    out, ups = carried[:2]
    lows = carried[2:]
    received = [permute_by(low, "ctx", j - 2 * steps) for j, low in enumerate(lows[:-1])]
    handed = permute_cyclic(out, "section", 1)[None]

    rest = axis_bits("ctx")[1:]
    rounds = [axis_bits("ctx")[:1] + axis_bits("dp")]
    rounds += [rest[k : k + 2] for k in range(0, len(rest), 2)]
    group = lax.axis_size("ctx") * lax.axis_size("dp")
    cols, up_cols, rows = model_width // HD, kv_heads, half // SUB
    units = -(-(rows * (cols + up_cols)) // group)
    side = lax.axis_index("section").astype(jnp.int32)
    smem = pl.BlockSpec(memory_space=pltpu.SMEM)
    vmem = pl.BlockSpec(memory_space=pltpu.VMEM)
    any_space = pl.BlockSpec(memory_space=pl.ANY)
    lanes = chunks_of(cols, 3)
    tile_shape = (units * group, SUB, HD)
    keep, send, handed = pl.pallas_call(
        partial(product_kernel, n_recv=len(received), lanes=lanes, up_cols=up_cols),
        in_specs=[smem] + [vmem] * (4 + len(received)) + [pl.BlockSpec(memory_space=pltpu.HBM)],
        out_specs=[vmem, vmem, any_space],
        out_shape=[
            pltpu.VMEM(tile_shape, bf16),
            pltpu.VMEM(tile_shape, bf16),
            jax.ShapeDtypeStruct(handed.shape, bf16),
        ],
        scratch_shapes=[
            pltpu.VMEM((tok, model_width), bf16),
            pltpu.SemaphoreType.DMA((len(lanes) + 1,)),
        ],
        compiler_params=pltpu.CompilerParams(vmem_limit_bytes=16 << 20),
        name="product",
    )(
        side[None],
        *[in_vmem(x) for x in (lows[-1], *received, own_mask, ups, handed)],
        in_hbm(hidden[0]),
    )
    recv = permute_cyclic(send, "section", 1)
    tiles = pl.pallas_call(
        merge_kernel,
        in_specs=[vmem, vmem],
        out_specs=vmem,
        out_shape=pltpu.VMEM(tile_shape, bf16),
        compiler_params=pltpu.CompilerParams(vmem_limit_bytes=8 << 20),
        name="merge",
    )(in_vmem(keep), in_vmem(recv))
    me = jnp.int32(0)
    for stages in rounds:
        tiles = direct_scatter(tiles.reshape(2 ** len(stages), -1, SUB, HD), stages)
        me = me * 2 ** len(stages) + direct_peers(stages)[1]
    for stages in reversed(rounds):
        tiles = direct_gather(tiles, stages).reshape(-1, SUB, HD)
    theirs = permute_cyclic(tiles, "section", 1)
    scalars = jnp.stack([side, me])
    outs = None
    for part in (tiles, theirs):
        part = part.reshape(group, units, SUB, HD)
        outs = assemble(scalars, part, outs, width, model_width, kv_width)
    w, u = outs
    down_map_gradient = w.T.reshape(model_width, 2, adapters, rank)
    up_map_gradient = u.reshape(2, adapters, rank, kv_width)
    return (handed, down_map_gradient, up_map_gradient)


def solution(mesh):
    return jax.shard_map(
        step,
        mesh=mesh,
        in_specs=(
            P(("section", "dp"), "ctx", None),
            P(("section", "dp"), "ctx", None),
            P(("section", "dp"), "ctx", None),
            P(("section", "dp"), "ctx", None),
            P(("section", "dp"), "ctx", None),
            P(("section", "dp"), None),
            P(("section", "dp"), None),
            P(),
            P(),
        ),
        out_specs=(P(("section", "dp"), "ctx", None), P(), P()),
        check_vma=False,
    )
```
